128 devices in a mesh: coil: 32 (over x, y, z_lo), kz: 4 (over z_hi, core).
Axes of the slice: x: 4, y: 4, z: 4 (z_hi: 2, z_lo: 2; z = z_hi * 2 + z_lo), core: 2. Of those that a mesh axis runs over, the one named last changes fastest.
Arguments:
- kdata: bfloat16 [2, 64, 32, 256, 512], P(None, 'kz', 'coil'), may hold values from -6 to 6
- spoke_angle: int32 [256], replicated, may hold values from 0 to 63
- spoke_count: int32 [64], P('kz'), may hold values from 128 to 256
- block_index: int32 [64, 4], replicated, may hold values from 0 to 511
- interp: bfloat16 [64, 4, 128, 128], replicated, may hold values from -0.5 to 0.5
- sens_maps: bfloat16 [2, 32, 256, 256], P(None, 'coil'), may hold values from -2.5 to 2.5
Outputs:
- image: float32 [2, 64, 256, 256], P(None, 'kz', 'coil')
The draws below stay inside these ranges and needn't reach their ends.
Inputs may be any that keep to these rules, and one draw needn't show every extreme that they name: Partition p uses its first spoke_count[p] spokes. `block_index`: several segments may hit the same grid block.
All inputs are finite; a program needn't handle non-finite values.
Results may differ from the reference program's by a relative error of at most 0.0059.
Values sent between devices are 32-bit elements; how exact they have to be, the bound alone decides.
A program may use at most 128 MiB of HBM per device.

```python
import jax
import jax.numpy as jnp
from jax import lax

N = 256
SAMPLES = 512
SEG_LEN = 128
SEGS = 4
BLOCKS = 512
SPOKES = 256
ANGLES = 64
KZ = 64
COILS = 32


def place_ends(values, key, smallest, largest):
    spot = [jax.random.randint(jax.random.fold_in(key, axis), (), 0, length) for axis, length in enumerate(values.shape)]
    main_axis = values.shape.index(max(values.shape))
    next_to = spot[:main_axis] + [(spot[main_axis] + 1) % values.shape[main_axis]] + spot[main_axis + 1:]
    return values.at[tuple(spot)].set(smallest).at[tuple(next_to)].set(largest)


def level_of(stream_key, dims, cuts, smallest, largest):
    def one(dim, blocks):
        steps = jax.random.uniform(jax.random.fold_in(jax.random.fold_in(stream_key, 6), dim), (blocks,), jnp.float32, smallest / len(cuts), largest / len(cuts))
        return jnp.repeat(jnp.exp(steps), dims[dim] // blocks).reshape((-1,) + (1,) * (len(dims) - dim - 1))

    factor_of = one(*cuts[0])
    for cut in cuts[1:]:
        factor_of = factor_of * one(*cut)
    return factor_of


def centred(rng, shape, width, limit, cuts=(), kind=jnp.bfloat16):
    values = width * jax.random.normal(rng, shape, jnp.float32)
    if cuts:
        values = values * level_of(rng, shape, cuts, -0.22, 0.18)
    return jnp.clip(values, -limit, limit).astype(kind)


def setup_inputs(seed: int = 0) -> dict:
    arg_keys = jax.random.split(jax.random.key(seed), 7)
    return {
        "kdata": centred(arg_keys[0], (2, KZ, COILS, SPOKES, SAMPLES), 1.0, 6.0, ((1, 4), (2, 32))),
        "spoke_angle": place_ends(jax.random.randint(arg_keys[1], (SPOKES,), 0, ANGLES), jax.random.fold_in(arg_keys[1], 1), 0, ANGLES - 1).astype(jnp.int32),
        "spoke_count": place_ends(jax.random.randint(arg_keys[2], (KZ,), SPOKES // 2, SPOKES + 1), jax.random.fold_in(arg_keys[2], 1), SPOKES // 2, SPOKES).astype(jnp.int32),
        "block_index": place_ends(jax.random.randint(arg_keys[3], (ANGLES, SEGS), 0, BLOCKS), jax.random.fold_in(arg_keys[3], 1), 0, BLOCKS - 1).astype(jnp.int32),
        "interp": centred(arg_keys[4], (ANGLES, SEGS, SEG_LEN, SEG_LEN), SEG_LEN ** -0.5, 0.5),
        "sens_maps": centred(arg_keys[5], (2, COILS, N, N), (COILS ** -0.5), 2.5, ((1, 32),)),
    }


def dft_tables(length, dtype):
    index = jnp.arange(length, dtype=jnp.int32)
    product = index[:, None] * index[None, :] % length
    phase = product.astype(jnp.float32) * (2.0 * jnp.pi / length)
    scale = 1.0 / jnp.sqrt(jnp.float32(length))
    return ((jnp.cos(phase) * scale).astype(dtype), (jnp.sin(phase) * scale).astype(dtype))

def spoke_weights(spoke_count, spoke_angle, angles, spokes):
    position = jnp.arange(spokes, dtype=jnp.int32)
    used = position[None, :] < spoke_count[:, None]
    match = spoke_angle[:, None] == jnp.arange(angles, dtype=jnp.int32)[None, :]
    return (used[:, :, None] & match[None, :, :]).astype(jnp.bfloat16)

def coil_image(data, weights, interp, block_index, cos_t, sin_t):
    f32 = jnp.float32
    binned = jnp.einsum('rpsn,psa->rpan', data.astype(f32), weights.astype(f32)).astype(jnp.bfloat16)
    rdim, pdim, adim, mdim = binned.shape
    seg = interp.shape[2]
    gdim = mdim // seg
    side = cos_t.shape[0]
    pieces = binned.reshape(rdim, pdim, adim, gdim, seg)
    contrib = jnp.einsum('rpagj,agjt->rpagt', pieces.astype(f32), interp.astype(f32))
    flat = jnp.zeros((rdim, pdim, side * side // seg, seg), f32)
    flat = flat.at[:, :, block_index.reshape(-1)].add(contrib.reshape(rdim, pdim, adim * gdim, seg))
    grid = flat.reshape(rdim, pdim, side, side).astype(jnp.bfloat16)
    cosf = cos_t.astype(f32)
    sinf = sin_t.astype(f32)
    grid_re = grid[0].astype(f32)
    grid_im = grid[1].astype(f32)
    half_re = jnp.einsum('ky,pyx->pkx', cosf, grid_re) + jnp.einsum('ky,pyx->pkx', sinf, grid_im)
    half_im = jnp.einsum('ky,pyx->pkx', cosf, grid_im) - jnp.einsum('ky,pyx->pkx', sinf, grid_re)
    half_re = half_re.astype(jnp.bfloat16).astype(f32)
    half_im = half_im.astype(jnp.bfloat16).astype(f32)
    out_re = jnp.einsum('pkx,mx->pkm', half_re, cosf) + jnp.einsum('pkx,mx->pkm', half_im, sinf)
    out_im = jnp.einsum('pkx,mx->pkm', half_im, cosf) - jnp.einsum('pkx,mx->pkm', half_re, sinf)
    return jnp.stack([out_re, out_im])

def conj_product(sens, image):
    real_part = sens[0] * image[0] + sens[1] * image[1]
    imag_part = sens[0] * image[1] - sens[1] * image[0]
    return jnp.stack([real_part, imag_part])

def reference(kdata, spoke_angle, spoke_count, block_index, interp, sens_maps):
    cos_t, sin_t = dft_tables(N, jnp.bfloat16)
    weights = spoke_weights(spoke_count, spoke_angle, ANGLES, SPOKES)

    def per_coil(total, coil_id):
        data = lax.dynamic_index_in_dim(kdata, coil_id, 2, keepdims=False)
        image_c = coil_image(data, weights, interp, block_index, cos_t, sin_t)
        sens = lax.dynamic_index_in_dim(sens_maps, coil_id, 1, keepdims=False).astype(jnp.float32)
        return (total + conj_product(sens[:, None], image_c), None)
    start = jnp.zeros((2, KZ, N, N), jnp.float32)
    combined, unused = lax.scan(per_coil, start, jnp.arange(COILS, dtype=jnp.int32))
    cos_z, sin_z = dft_tables(KZ, jnp.float32)
    high = lax.Precision.HIGHEST
    image_re = jnp.einsum('zk,kyx->zyx', cos_z, combined[0], precision=high) + jnp.einsum('zk,kyx->zyx', sin_z, combined[1], precision=high)
    image_im = jnp.einsum('zk,kyx->zyx', cos_z, combined[1], precision=high) - jnp.einsum('zk,kyx->zyx', sin_z, combined[0], precision=high)
    return jnp.stack([image_re, image_im])
```

```python
import jax
import jax.numpy as jnp
from jax import lax
from jax.sharding import PartitionSpec as P


def split_up(shard, dim, length):
    shape = shard.shape
    tiles = shard.reshape(*shape[:dim], length, shape[dim] // length, *shape[dim + 1 :])
    return jnp.moveaxis(tiles, dim, 0)


def sum_at_owner(shard, axis, dim):
    tiles = split_up(shard, dim, lax.axis_size(axis))
    arrived = lax.all_to_all(tiles, axis, split_axis=0, concat_axis=0, tiled=True)
    return arrived.sum(axis=0)


def in_order(tiles, dim):
    shape = list(tiles.shape[1:])
    shape[dim] *= tiles.shape[0]
    return jnp.moveaxis(tiles, 0, dim).reshape(shape)


def from_everyone(shard, axis):
    copies = jnp.broadcast_to(shard, (lax.axis_size(axis), *shard.shape))
    return lax.all_to_all(copies, axis, split_axis=0, concat_axis=0, tiled=True)


def collect(shard, axis, dim):
    return in_order(from_everyone(shard, axis), dim)


def dft_tables(length, dtype):
    index = jnp.arange(length, dtype=jnp.int32)
    product = index[:, None] * index[None, :] % length
    phase = product.astype(jnp.float32) * (2.0 * jnp.pi / length)
    scale = 1.0 / jnp.sqrt(jnp.float32(length))
    return ((jnp.cos(phase) * scale).astype(dtype), (jnp.sin(phase) * scale).astype(dtype))


def kz_block(z_first, z_count, k_count, length):
    z_index = z_first + jnp.arange(z_count, dtype=jnp.int32)
    k_index = jnp.arange(k_count, dtype=jnp.int32)
    product = z_index[:, None] * k_index[None, :] % length
    phase = product.astype(jnp.float32) * (2.0 * jnp.pi / length)
    scale = 1.0 / jnp.sqrt(jnp.float32(length))
    return (jnp.cos(phase) * scale, jnp.sin(phase) * scale)


def kz_apply(cos_z, sin_z, slab):
    high = lax.Precision.HIGHEST
    real_part = jnp.einsum("zk,kyx->zyx", cos_z, slab[0], precision=high) + jnp.einsum(
        "zk,kyx->zyx", sin_z, slab[1], precision=high
    )
    imag_part = jnp.einsum("zk,kyx->zyx", cos_z, slab[1], precision=high) - jnp.einsum(
        "zk,kyx->zyx", sin_z, slab[0], precision=high
    )
    return jnp.stack([real_part, imag_part])


def coil_image(data, weights, interp, block_index, cos_t, sin_t):
    f32 = jnp.float32
    binned = jnp.einsum("rpsn,psa->rpan", data, weights, preferred_element_type=f32).astype(
        jnp.bfloat16
    )
    rdim, pdim, adim, mdim = binned.shape
    seg = interp.shape[2]
    gdim = mdim // seg
    side = cos_t.shape[0]
    pieces = binned.reshape(rdim, pdim, adim, gdim, seg)
    contrib = jnp.einsum("rpagj,agjt->agrpt", pieces, interp, preferred_element_type=f32).astype(jnp.bfloat16)
    contrib = contrib.reshape(adim * gdim, rdim, pdim, seg)
    xdim = side // seg
    blocks = block_index.reshape(-1)
    spread = (blocks[None, :] == jnp.arange(side * xdim, dtype=jnp.int32)[:, None]).astype(jnp.bfloat16)
    spread = spread.reshape(side, xdim, adim * gdim)
    cos_g = jnp.einsum("ky,yhq->hkq", cos_t, spread, preferred_element_type=f32).astype(jnp.bfloat16)
    sin_g = jnp.einsum("ky,yhq->hkq", sin_t, spread, preferred_element_type=f32).astype(jnp.bfloat16)
    half_re = jnp.einsum("hkq,qpt->pkht", cos_g, contrib[:, 0], preferred_element_type=f32) + jnp.einsum(
        "hkq,qpt->pkht", sin_g, contrib[:, 1], preferred_element_type=f32
    )
    half_im = jnp.einsum("hkq,qpt->pkht", cos_g, contrib[:, 1], preferred_element_type=f32) - jnp.einsum(
        "hkq,qpt->pkht", sin_g, contrib[:, 0], preferred_element_type=f32
    )
    half_re = half_re.astype(jnp.bfloat16).reshape(pdim, side, side)
    half_im = half_im.astype(jnp.bfloat16).reshape(pdim, side, side)
    out_re = jnp.einsum("pkx,mx->pkm", half_re, cos_t, preferred_element_type=f32) + jnp.einsum(
        "pkx,mx->pkm", half_im, sin_t, preferred_element_type=f32
    )
    out_im = jnp.einsum("pkx,mx->pkm", half_im, cos_t, preferred_element_type=f32) - jnp.einsum(
        "pkx,mx->pkm", half_re, sin_t, preferred_element_type=f32
    )
    return jnp.stack([out_re, out_im])


def conj_product(sens, image):
    real_part = sens[0] * image[0] + sens[1] * image[1]
    imag_part = sens[0] * image[1] - sens[1] * image[0]
    return jnp.stack([real_part, imag_part])


def per_device(kdata, spoke_angle, spoke_count, block_index, interp, sens_maps):
    side = sens_maps.shape[2]
    parts_here = kdata.shape[1]
    spokes = kdata.shape[3]
    angles = interp.shape[0]
    cos_t, sin_t = dft_tables(side, jnp.bfloat16)
    position = jnp.arange(spokes, dtype=jnp.int32)
    used = position[None, :] < spoke_count[:, None]
    match = spoke_angle[:, None] == jnp.arange(angles, dtype=jnp.int32)[None, :]
    weights = (used[:, :, None] & match[None, :, :]).astype(jnp.bfloat16)
    data = kdata[:, :, 0]
    image_c = coil_image(data, weights, interp, block_index, cos_t, sin_t)
    sens_here = sens_maps.astype(jnp.float32)
    weighted = conj_product(sens_here[:, 0][:, None], image_c)
    combined = lax.psum_scatter(weighted, "coil", scatter_dimension=2, tiled=True)
    groups = lax.axis_size("kz")
    kz_total = parts_here * groups
    my_first = lax.axis_index("kz") * parts_here
    piece = collect(combined, "kz", 1)
    cos_z, sin_z = kz_block(my_first, parts_here, piece.shape[1], kz_total)
    return kz_apply(cos_z, sin_z, piece)


def solution(mesh):
    placed = (
        P(None, "kz", "coil", None, None),
        P(),
        P("kz"),
        P(),
        P(),
        P(None, "coil", None, None),
    )
    return jax.shard_map(
        per_device,
        mesh=mesh,
        in_specs=placed,
        out_specs=P(None, "kz", "coil", None),
        check_vma=False,
    )
```

```python
import functools

import jax
import jax.numpy as jnp
import numpy as np
from jax import lax
from jax.experimental import pallas as pl
from jax.experimental.pallas import tpu as pltpu
from jax.sharding import PartitionSpec as P

F32 = jnp.float32
BF16 = jnp.bfloat16
MESH = pl.DeviceIdType.MESH

PPC = 2
BPAD = 40
LAGS = (0, 2, 4, 6, 8, 10)

STREAMS = ((True, 1), (True, 3), (False, 1), (False, 3))


def dft_np(rows, cols, length):
    product = (rows[:, None] * cols[None, :]) % length
    phase = product.astype(np.float64) * (2.0 * np.pi / length)
    return np.cos(phase) / np.sqrt(length), np.sin(phase) / np.sqrt(length)


def plane_table(side):
    index = np.arange(side)
    cos_t, sin_t = dft_np(index, index, side)
    table = np.block([[cos_t, -sin_t], [sin_t, cos_t]])
    return jnp.asarray(table, dtype=BF16)


def kz_table(groups, parts):
    total = groups * parts
    index = np.arange(total)
    cos_z, sin_z = dft_np(index, index, total)
    blocks = []
    for g in range(groups):
        c = cos_z[g * parts : (g + 1) * parts].reshape(parts, groups, 1, parts)
        s = sin_z[g * parts : (g + 1) * parts].reshape(parts, groups, 1, parts)
        real = np.concatenate([c, s], axis=2).reshape(parts, -1)
        imag = np.concatenate([-s, c], axis=2).reshape(parts, -1)
        blocks.append(np.concatenate([real, imag], axis=0))
    return jnp.asarray(np.stack(blocks), dtype=F32)


def flip(i, pairing):
    return i + 1 - 2 * (i % 2) if pairing == 1 else 3 - i


def kernel(
    parts, angles, spokes, side,
    count_ref, angle_ref, block_ref, ztab_ref,
    kdata_hbm, interp_hbm, sens_hbm, plane_hbm,
    out_ref,
    kd, itp, sens_v, plane, tab, sensp, binned, spread, half,
    img, r1x, r1y, r2, r3, r4, r5, gath, kzout,
    load_sem, send_sem, recv_sem, kz_send, kz_recv,
):
    chunks = parts // PPC
    segs = 4
    seg = 128
    hits = angles * segs
    xpad = hits + 8
    coil = lax.axis_index("coil")
    group = lax.axis_index("kz")
    x, y, z = coil // 8, (coil // 2) % 4, coil % 2

    def dev(axis_x, pairing):
        if axis_x:
            return ((flip(x, pairing) * 4 + y) * 2 + z, group)
        return ((x * 4 + flip(y, pairing)) * 2 + z, group)

    zdev = ((x * 4 + y) * 2 + 1 - z, group)
    kzdevs = [(coil, (group + d) % 4) for d in range(1, 4)]

    loads = [
        pltpu.make_async_copy(plane_hbm, plane, load_sem.at[0]),
        pltpu.make_async_copy(sens_hbm, sens_v, load_sem.at[1]),
    ]
    kloads = [
        pltpu.make_async_copy(
            kdata_hbm.at[:, pl.ds(q * (parts // 4), parts // 4)],
            kd.at[:, pl.ds(q * (parts // 4), parts // 4)],
            load_sem.at[2 + q],
        )
        for q in range(4)
    ]
    iloads = [
        pltpu.make_async_copy(
            interp_hbm.at[pl.ds(q * (angles // 4), angles // 4)],
            itp.at[pl.ds(q * (angles // 4), angles // 4)],
            load_sem.at[6 + q],
        )
        for q in range(4)
    ]
    for copy in loads + kloads + iloads:
        copy.start()

    barrier = pltpu.get_barrier_semaphore()
    peers = [dev(a, p) for a in (True, False) for p in (1, 3)] + [zdev] + kzdevs
    for peer in peers:
        pl.semaphore_signal(barrier, inc=1, device_id=peer, device_id_type=MESH)

    for copy in loads:
        copy.wait()
    row = lax.broadcasted_iota(jnp.int32, (side, side), 0)
    col = lax.broadcasted_iota(jnp.int32, (side, side), 1)
    perm = jnp.where(jnp.bitwise_xor(row, col) == coil * 8, 1.0, 0.0).astype(BF16)
    cos_p = jnp.dot(perm, plane[0:side, 0:side], preferred_element_type=F32).astype(BF16)
    sin_p = jnp.dot(perm, plane[side : 2 * side, 0:side], preferred_element_type=F32).astype(BF16)
    blocks = jnp.broadcast_to(block_ref[0:1, :], (side, hits))
    yrow = lax.broadcasted_iota(jnp.int32, (side, hits), 0)
    for h in range(2):
        onto = jnp.where(blocks == yrow * 2 + h, 1.0, 0.0).astype(BF16)
        cos_g = jnp.dot(cos_p, onto, preferred_element_type=F32)
        sin_g = jnp.dot(sin_p, onto, preferred_element_type=F32)
        tab[h, 0:side, 0:hits] = cos_g.astype(BF16)
        tab[h, side : 2 * side, hits : 2 * hits] = cos_g.astype(BF16)
        tab[h, 0:side, hits : 2 * hits] = sin_g.astype(BF16)
        tab[h, side : 2 * side, 0:hits] = (-sin_g).astype(BF16)
    for r in range(2):
        sensp[r] = jnp.dot(perm, sens_v[r], preferred_element_type=F32)

    arow = lax.broadcasted_iota(jnp.int32, (angles, spokes), 0)
    scol = lax.broadcasted_iota(jnp.int32, (angles, spokes), 1)
    match = jnp.broadcast_to(angle_ref[0:1, :], (angles, spokes)) == arow
    for q in range(4):
        kloads[q].wait()

        def bin_one(i, carry):
            p = q * (parts // 4) + i
            used = jnp.logical_and(match, scol < count_ref[p])
            weights = jnp.where(used, 1.0, 0.0).astype(BF16)
            for r in range(2):
                summed = jnp.dot(weights, kd[r, p], preferred_element_type=F32)
                for g in range(segs):
                    start = g * angles * BPAD + r * parts + p
                    binned[pl.ds(start, angles, stride=BPAD), :] = summed[:, g * seg : (g + 1) * seg]
            return carry

        lax.fori_loop(0, parts // 4, bin_one, 0)

    batch = 4
    for q in range(4):
        iloads[q].wait()

        def spread_some(i, carry):
            for k in range(batch):
                a = q * (angles // 4) + i * batch + k
                for g in range(segs):
                    start = pl.multiple_of(g * angles * BPAD + a * BPAD, 8)
                    piece = binned[pl.ds(start, 2 * parts), :].astype(BF16)
                    got = jnp.dot(piece, itp[a, g], preferred_element_type=F32)
                    spread[pl.ds(a * segs + g, 2 * parts, stride=xpad), :] = got
            return carry

        lax.fori_loop(0, angles // 4 // batch, spread_some, 0)

    pl.semaphore_wait(barrier, len(peers))

    def make(c):
        ps = [c * PPC + k for k in range(PPC)]
        rows = []
        for r in range(2):
            pieces = [
                spread[pl.ds(pl.multiple_of((r * parts + p) * xpad, 8), hits), :].astype(BF16) for p in ps
            ]
            rows.append(jnp.concatenate(pieces, axis=1))
        stacked = jnp.concatenate(rows, axis=0)
        for h in range(2):
            got = jnp.dot(tab[h], stacked, preferred_element_type=F32).astype(BF16)
            for k in range(PPC):
                for r in range(2):
                    half[k, :, r * side + h * seg : r * side + (h + 1) * seg] = got[
                        r * side : (r + 1) * side, k * seg : (k + 1) * seg
                    ]
        for k in range(PPC):
            full = jnp.dot(half[k], plane[...], preferred_element_type=F32)
            s_re, s_im = sensp[0], sensp[1]
            o_re, o_im = full[:, 0:side], full[:, side : 2 * side]
            w_re = s_re * o_re + s_im * o_im
            w_im = s_re * o_im - s_im * o_re
            for h in range(2):
                cols = slice(h * seg, (h + 1) * seg)
                img[h, ps[k]] = w_re[:, cols].reshape(4, 4, 16, seg)
                img[2 + h, ps[k]] = w_im[:, cols].reshape(4, 4, 16, seg)

    def slots(pairing):
        return (1, 0, 1, 3) if pairing == 1 else (2, 1, 0, 1)

    def copies(s, stage, ps):
        first_x, pairing = STREAMS[s]
        sent, keep, onward, quarter = slots(pairing)
        if stage == 1:
            peer = dev(first_x, pairing)
            if first_x:
                src, dst = img.at[s, ps, pl.ds(sent, 2)], r1x.at[s, ps]
            else:
                src, dst = img.at[s, ps, :, pl.ds(sent, 2)], r1y.at[s - 2, ps]
        elif stage == 2:
            peer = dev(first_x, 4 - pairing)
            src = r1x.at[s, ps, onward] if first_x else r1y.at[s - 2, ps, :, onward]
            dst = r2.at[s, ps]
        elif stage == 3:
            peer = dev(not first_x, pairing)
            src, dst = r2.at[s, ps, pl.ds(sent, 2)], r3.at[s, ps]
        elif stage == 4:
            peer = dev(not first_x, 4 - pairing)
            src, dst = r3.at[s, ps, onward], r4.at[s, ps]
        else:
            peer = zdev
            src, dst = r4.at[s, ps, pl.ds(8, 8)], r5.at[s, ps]
        return src, dst, peer

    def remote(s, stage, c):
        src, dst, peer = copies(s, stage, pl.ds(c * PPC, PPC))
        return pltpu.make_async_remote_copy(
            src_ref=src, dst_ref=dst,
            send_sem=send_sem.at[stage - 1, s], recv_sem=recv_sem.at[stage - 1, s, c],
            device_id=peer, device_id_type=MESH,
        )

    def held(s, ps, quarters, rows=slice(None)):
        first_x, pairing = STREAMS[s]
        keep = slots(pairing)[1]
        if first_x:
            return img[s, ps, 0, quarters, rows] + r1x[s, ps, keep, quarters, rows] + r2[s, ps, quarters, rows]
        return img[s, ps, quarters, 0, rows] + r1y[s - 2, ps, quarters, keep, rows] + r2[s, ps, quarters, rows]

    def step(stage, c):
        ps = pl.ds(c * PPC, PPC)
        for s in range(4):
            first_x, pairing = STREAMS[s]
            sent, keep, onward, quarter = slots(pairing)
            if stage > 1:
                remote(s, stage - 1, c).wait_recv()
            if stage == 2:
                if first_x:
                    r1x[s, ps, onward] += img[s, ps, quarter]
                else:
                    r1y[s - 2, ps, :, onward] += img[s, ps, :, quarter]
            elif stage == 3:
                r2[s, ps, sent : sent + 2] = held(s, ps, slice(sent, sent + 2))
            elif stage == 4:
                r3[s, ps, onward] += held(s, ps, quarter)
            elif stage == 5:
                rows = slice(8, 16)
                r4[s, ps, rows] += held(s, ps, 0, rows) + r3[s, ps, keep, rows]
            elif stage == 6:
                rows = slice(0, 8)
                gath[group, s, ps] = held(s, ps, 0, rows) + r3[s, ps, keep, rows] + r4[s, ps, rows] + r5[s, ps]
            if stage < 6:
                remote(s, stage, c).start()

    def kz_remote(d, c, slot):
        ps = pl.ds(c * PPC, PPC)
        return pltpu.make_async_remote_copy(
            src_ref=gath.at[slot, :, ps], dst_ref=gath.at[slot, :, ps],
            send_sem=kz_send.at[d], recv_sem=kz_recv.at[slot, c],
            device_id=kzdevs[d], device_id_type=MESH,
        )

    def pipeline(i, carry):
        @pl.when(i < chunks)
        def _():
            make(i)
            step(1, i)

        for stage in range(2, 7):
            c = i - LAGS[stage - 1]

            @pl.when(jnp.logical_and(c >= 0, c < chunks))
            def _():
                step(stage, c)
                if stage == 6:
                    for d in range(3):
                        kz_remote(d, c, group).start()

        return carry

    lax.fori_loop(0, chunks + LAGS[5], pipeline, 0)

    for d in range(3):
        for c in range(chunks):
            kz_remote(d, c, (group + d + 1) % 4).wait_recv()

    for mh in range(2):
        for yy in range(8):
            pieces = []
            for g in range(4):
                for r in range(2):
                    pieces.append(gath[g, r * 2 + mh, :, yy, :])
            stacked = jnp.concatenate(pieces, axis=0)
            got = jnp.dot(ztab_ref[group], stacked, preferred_element_type=F32, precision=lax.Precision.HIGHEST)
            kzout[mh, pl.ds(yy, 2 * parts, stride=8), :] = got
        out_ref[:, :, :, mh * seg : (mh + 1) * seg] = kzout[mh].reshape(2, parts, 8, seg)

    everything = pl.ds(0, parts)
    for s in range(4):
        for stage in range(1, 6):
            src, dst, peer = copies(s, stage, everything)
            pltpu.make_async_remote_copy(
                src_ref=src, dst_ref=dst, send_sem=send_sem.at[stage - 1, s],
                recv_sem=recv_sem.at[stage - 1, s, 0], device_id=peer, device_id_type=MESH,
            ).wait_send()
    for d in range(3):
        pltpu.make_async_remote_copy(
            src_ref=gath.at[group], dst_ref=gath.at[group], send_sem=kz_send.at[d],
            recv_sem=kz_recv.at[group, 0], device_id=kzdevs[d], device_id_type=MESH,
        ).wait_send()


def per_device(kdata, spoke_angle, spoke_count, block_index, interp, sens_maps):
    side = sens_maps.shape[2]
    parts = kdata.shape[1]
    spokes, samples = kdata.shape[3], kdata.shape[4]
    angles, segs, seg = interp.shape[0], interp.shape[1], interp.shape[2]
    hits = angles * segs
    chunks = parts // PPC
    any_spec = pl.BlockSpec(memory_space=pl.ANY)
    vmem_spec = pl.BlockSpec(memory_space=pltpu.VMEM)
    return pl.pallas_call(
        functools.partial(kernel, parts, angles, spokes, side),
        out_shape=jax.ShapeDtypeStruct((2, parts, 8, side), F32),
        in_specs=[pl.BlockSpec(memory_space=pltpu.SMEM)] + [vmem_spec] * 3 + [any_spec] * 4,
        out_specs=vmem_spec,
        scratch_shapes=[
            pltpu.VMEM((2, parts, spokes, samples), BF16),
            pltpu.VMEM((angles, segs, seg, seg), BF16),
            pltpu.VMEM((2, side, side), BF16),
            pltpu.VMEM((2 * side, 2 * side), BF16),
            pltpu.VMEM((2, 2 * side, 2 * hits), BF16),
            pltpu.VMEM((2, side, side), F32),
            pltpu.VMEM((segs * angles * BPAD, seg), F32),
            pltpu.VMEM((2 * parts * (hits + 8), seg), F32),
            pltpu.VMEM((PPC, side, 2 * side), BF16),
            pltpu.VMEM((4, parts, 4, 4, 16, seg), F32),
            pltpu.VMEM((2, parts, 2, 4, 16, seg), F32),
            pltpu.VMEM((2, parts, 4, 2, 16, seg), F32),
            pltpu.VMEM((4, parts, 4, 16, seg), F32),
            pltpu.VMEM((4, parts, 2, 16, seg), F32),
            pltpu.VMEM((4, parts, 16, seg), F32),
            pltpu.VMEM((4, parts, 8, seg), F32),
            pltpu.VMEM((4, 4, parts, 8, seg), F32),
            pltpu.VMEM((2, 2 * parts * 8, seg), F32),
            pltpu.SemaphoreType.DMA((10,)),
            pltpu.SemaphoreType.DMA((5, 4)),
            pltpu.SemaphoreType.DMA((5, 4, chunks)),
            pltpu.SemaphoreType.DMA((3,)),
            pltpu.SemaphoreType.DMA((4, chunks)),
        ],
        compiler_params=pltpu.CompilerParams(
            collective_id=0, has_side_effects=True, vmem_limit_bytes=63 << 20
        ),
    )(
        spoke_count,
        spoke_angle.reshape(1, spokes),
        block_index.reshape(1, hits),
        kz_table(4, parts),
        kdata[:, :, 0],
        interp,
        sens_maps[:, 0],
        plane_table(side),
    )


def solution(mesh):
    placed = (
        P(None, "kz", "coil", None, None),
        P(),
        P("kz"),
        P(),
        P(),
        P(None, "coil", None, None),
    )
    return jax.shard_map(
        per_device,
        mesh=mesh,
        in_specs=placed,
        out_specs=P(None, "kz", "coil", None),
        check_vma=False,
    )
```

```python
import functools

import jax
import jax.numpy as jnp
import numpy as np
from jax import lax
from jax.experimental import pallas as pl
from jax.experimental.pallas import tpu as pltpu
from jax.sharding import PartitionSpec as P

F32 = jnp.float32
BF16 = jnp.bfloat16
MESH = pl.DeviceIdType.MESH

BPAD = 40

STREAMS = ((True, 1), (True, 3), (False, 1), (False, 3))


def dft_np(rows, cols, length):
    product = (rows[:, None] * cols[None, :]) % length
    phase = product.astype(np.float64) * (2.0 * np.pi / length)
    return np.cos(phase) / np.sqrt(length), np.sin(phase) / np.sqrt(length)


def plane_table(side):
    index = np.arange(side)
    cos_t, sin_t = dft_np(index, index, side)
    table = np.block([[cos_t, -sin_t], [sin_t, cos_t]])
    return jnp.asarray(table, dtype=BF16)


def kz_table(groups, parts):
    total = groups * parts
    index = np.arange(total)
    cos_z, sin_z = dft_np(index, index, total)
    blocks = []
    for g in range(groups):
        c = cos_z[g * parts : (g + 1) * parts].reshape(parts, groups, 1, parts)
        s = sin_z[g * parts : (g + 1) * parts].reshape(parts, groups, 1, parts)
        real = np.concatenate([c, s], axis=2).reshape(parts, -1)
        imag = np.concatenate([-s, c], axis=2).reshape(parts, -1)
        blocks.append(np.concatenate([real, imag], axis=0))
    return jnp.asarray(np.stack(blocks), dtype=F32)


def flip(i, pairing):
    return i + 1 - 2 * (i % 2) if pairing == 1 else 3 - i


def kernel(
    parts, angles, spokes, side,
    count_ref, angle_ref, block_ref, ztab_ref,
    kdata_hbm, interp_hbm, sens_hbm, plane_hbm,
    out_ref,
    kd, itp, sens_v, plane, tab, sensp, senso, binned, spread, other, half,
    img, r2x, r2y, r3, r4, r5, gath, kzout,
    load_sem, sens_send, sens_recv, send_sem, seg_recv, recv_sem, own_send, own_recv, kz_send, kz_recv,
):
    segs = 4
    seg = 128
    hits = angles * segs
    xpad = hits + 8
    coil = lax.axis_index("coil")
    group = lax.axis_index("kz")
    core = group % 2
    x, y, z = coil // 8, (coil // 2) % 4, coil % 2

    def dev(axis_x, pairing, over_z=False):
        zz = 1 - z if over_z else z
        if axis_x:
            return ((flip(x, pairing) * 4 + y) * 2 + zz, group)
        return ((x * 4 + flip(y, pairing)) * 2 + zz, group)

    zdev = ((x * 4 + y) * 2 + 1 - z, group)
    kzdevs = [(coil, (group + d) % 4) for d in range(1, 4)]
    sibling = (coil, group + 1 - 2 * core)

    def side_of(s):
        first_x, pairing = STREAMS[s]
        i = x if first_x else y
        return ((i + 1) // 2) % 2 if pairing == 1 else i // 2

    def part_of(s, k, mine):
        return k * 8 + s * 2 + (side_of(s) if mine else 1 - side_of(s))

    loads = [
        pltpu.make_async_copy(plane_hbm, plane, load_sem.at[0]),
        pltpu.make_async_copy(sens_hbm, sens_v, load_sem.at[1]),
    ]
    kloads = [
        pltpu.make_async_copy(
            kdata_hbm.at[:, pl.ds(q * (parts // 4), parts // 4)],
            kd.at[:, pl.ds(q * (parts // 4), parts // 4)],
            load_sem.at[2 + q],
        )
        for q in range(4)
    ]
    iloads = [
        pltpu.make_async_copy(
            interp_hbm.at[pl.ds(q * (angles // 4), angles // 4)],
            itp.at[pl.ds(q * (angles // 4), angles // 4)],
            load_sem.at[6 + q],
        )
        for q in range(4)
    ]
    for copy in loads + kloads + iloads:
        copy.start()

    barrier = pltpu.get_barrier_semaphore()
    peers = [dev(*stream, over_z) for stream in STREAMS for over_z in (False, True)] + [zdev] + kzdevs
    for peer in peers:
        pl.semaphore_signal(barrier, inc=1, device_id=peer, device_id_type=MESH)

    for copy in loads:
        copy.wait()
    row = lax.broadcasted_iota(jnp.int32, (side, side), 0)
    col = lax.broadcasted_iota(jnp.int32, (side, side), 1)
    perm = jnp.where(jnp.bitwise_xor(row, col) == coil * 8, 1.0, 0.0).astype(BF16)
    for r in range(2):
        sensp[r] = jnp.dot(perm, sens_v[r], preferred_element_type=F32)

    pl.semaphore_wait(barrier, len(peers))

    def sens_copy(s):
        return pltpu.make_async_remote_copy(
            src_ref=sensp.at[core], dst_ref=senso.at[s, core],
            send_sem=sens_send.at[0, s], recv_sem=sens_recv.at[0, s],
            device_id=dev(*STREAMS[s]), device_id_type=MESH,
        )

    def sens_pass(s, r):
        return pltpu.make_async_remote_copy(
            src_ref=senso.at[s, r], dst_ref=senso.at[s, r],
            send_sem=sens_send.at[1, s], recv_sem=sens_recv.at[1, s],
            device_id=sibling, device_id_type=MESH,
        )

    for s in range(4):
        sens_copy(s).start()

    cos_p = jnp.dot(perm, plane[0:side, 0:side], preferred_element_type=F32).astype(BF16)
    sin_p = jnp.dot(perm, plane[side : 2 * side, 0:side], preferred_element_type=F32).astype(BF16)
    blocks = jnp.broadcast_to(block_ref[0:1, :], (side, hits))
    yrow = lax.broadcasted_iota(jnp.int32, (side, hits), 0)
    for h in range(2):
        onto = jnp.where(blocks == yrow * 2 + h, 1.0, 0.0).astype(BF16)
        cos_g = jnp.dot(cos_p, onto, preferred_element_type=F32)
        sin_g = jnp.dot(sin_p, onto, preferred_element_type=F32)
        tab[h, 0:side, 0:hits] = cos_g.astype(BF16)
        tab[h, side : 2 * side, hits : 2 * hits] = cos_g.astype(BF16)
        tab[h, 0:side, hits : 2 * hits] = sin_g.astype(BF16)
        tab[h, side : 2 * side, 0:hits] = (-sin_g).astype(BF16)

    arow = lax.broadcasted_iota(jnp.int32, (angles, spokes), 0)
    scol = lax.broadcasted_iota(jnp.int32, (angles, spokes), 1)
    match = jnp.broadcast_to(angle_ref[0:1, :], (angles, spokes)) == arow
    for q in range(4):
        kloads[q].wait()

        def bin_one(i, carry):
            p = q * (parts // 4) + i
            used = jnp.logical_and(match, scol < count_ref[p])
            weights = jnp.where(used, 1.0, 0.0).astype(BF16)
            for r in range(2):
                summed = jnp.dot(weights, kd[r, p], preferred_element_type=F32)
                for g in range(segs):
                    start = g * angles * BPAD + r * parts + p
                    binned[pl.ds(start, angles, stride=BPAD), :] = summed[:, g * seg : (g + 1) * seg]
            return carry

        lax.fori_loop(0, parts // 4, bin_one, 0)

    batch = 4
    for q in range(4):
        iloads[q].wait()

        def spread_some(i, carry):
            for k in range(batch):
                a = q * (angles // 4) + i * batch + k
                for g in range(segs):
                    start = pl.multiple_of(g * angles * BPAD + a * BPAD, 8)
                    piece = binned[pl.ds(start, 2 * parts), :].astype(BF16)
                    got = jnp.dot(piece, itp[a, g], preferred_element_type=F32)
                    spread[pl.ds(a * segs + g, 2 * parts, stride=xpad), :] = got
            return carry

        lax.fori_loop(0, angles // 4 // batch, spread_some, 0)

    def seg_rows(p, r):
        return pl.ds(pl.multiple_of((r * parts + p) * xpad, 8), hits)

    def seg_copy(s, k, r):
        return pltpu.make_async_remote_copy(
            src_ref=spread.at[seg_rows(part_of(s, k, False), r)], dst_ref=other.at[s, k, r],
            send_sem=send_sem.at[0, s], recv_sem=seg_recv.at[s, k, r],
            device_id=dev(*STREAMS[s]), device_id_type=MESH,
        )

    for k in range(2):
        for s in range(4):
            for r in range(2):
                seg_copy(s, k, r).start()
    for s in range(4):
        sens_copy(s).wait_recv()
        sens_pass(s, core).start()
    for s in range(4):
        sens_pass(s, 1 - core).wait_recv()

    def slots(pairing):
        return (1, 0, 1, 3) if pairing == 1 else (2, 1, 0, 1)

    def lay(s):
        first_x, pairing = STREAMS[s]
        return (first_x, 3, 2, 1, 0) if pairing == 1 else (first_x, 1, 1, 0, 1)

    def make(s, k):
        first_x, pairing = STREAMS[s]
        for r in range(2):
            seg_copy(s, k, r).wait_recv()
        p = part_of(s, k, True)
        rows = []
        for r in range(2):
            own = spread[seg_rows(p, r), :].astype(BF16)
            rows.append(jnp.concatenate([own, other[s, k, r].astype(BF16)], axis=1))
        stacked = jnp.concatenate(rows, axis=0)
        for h in range(2):
            got = jnp.dot(tab[h], stacked, preferred_element_type=F32).astype(BF16)
            for n in range(2):
                for r in range(2):
                    half[n, :, r * side + h * seg : r * side + (h + 1) * seg] = got[
                        r * side : (r + 1) * side, n * seg : (n + 1) * seg
                    ]
        mine = jnp.dot(half[0], plane[...], preferred_element_type=F32)
        theirs = jnp.dot(half[1], plane[...], preferred_element_type=F32)
        for jx in range(4):
            for jy in range(4):
                here = slice((jx * 4 + jy) * 16, (jx * 4 + jy + 1) * 16)
                there = (jx ^ pairing) * 4 + jy if first_x else jx * 4 + (jy ^ pairing)
                that = slice(there * 16, (there + 1) * 16)
                a_re, a_im = sensp[0, here, :], sensp[1, here, :]
                b_re, b_im = senso[s, 0, that, :], senso[s, 1, that, :]
                o_re, o_im = mine[here, 0:side], mine[here, side : 2 * side]
                t_re, t_im = theirs[here, 0:side], theirs[here, side : 2 * side]
                img[s, k, 0, jx, jy] = (a_re * o_re + a_im * o_im) + (b_re * t_re + b_im * t_im)
                img[s, k, 1, jx, jy] = (a_re * o_im - a_im * o_re) + (b_re * t_im - b_im * t_re)

    def copies(s, stage, k, r):
        first_x, second, sent2, slot0, slot_t = lay(s)
        pairing = STREAMS[s][1]
        sent, keep, onward, quarter = slots(pairing)
        if stage == 2:
            if first_x:
                return img.at[s, k, r, pl.ds(sent2, 2)], r2x.at[s, k, r], dev(True, second)
            return img.at[s, k, r, :, pl.ds(sent2, 2)], r2y.at[s - 2, k, r], dev(False, second)
        if stage == 3:
            if first_x:
                return r2x.at[s, k, r, :, pl.ds(sent, 2)], r3.at[s, k, r], dev(False, pairing)
            return r2y.at[s - 2, k, r, pl.ds(sent, 2)], r3.at[s, k, r], dev(True, pairing)
        src = r3.at[s, k, r, :, onward] if first_x else r3.at[s, k, r, onward]
        return src, r4.at[s, k, r], dev(not first_x, second)

    def remote(s, stage, k, r):
        src, dst, peer = copies(s, stage, k, r)
        return pltpu.make_async_remote_copy(
            src_ref=src, dst_ref=dst,
            send_sem=send_sem.at[stage - 1, s], recv_sem=recv_sem.at[stage - 2, s, k, r],
            device_id=peer, device_id_type=MESH,
        )

    def held(s, k, r, pair, quarter):
        first_x, second, sent2, slot0, slot_t = lay(s)
        j = STREAMS[s][1] if pair else 0
        slot = slot_t if pair else slot0
        if first_x:
            return img[s, k, r, j, quarter] + r2x[s, k, r, slot, quarter]
        return img[s, k, r, quarter, j] + r2y[s - 2, k, r, quarter, slot]

    def held3(s, k, r, pair, which, quarter):
        first_x, second, sent2, slot0, slot_t = lay(s)
        slot = slot_t if pair else slot0
        got = r3[s, k, r, slot, which] if first_x else r3[s, k, r, which, slot]
        return held(s, k, r, pair, quarter) + got

    def owner_copies(s, k, r):
        first_x, second, sent2, slot0, slot_t = lay(s)
        spots = ((slot_t, 0), (slot0, 8), (slot_t, 8))
        to = (dev(*STREAMS[s]), zdev, dev(*STREAMS[s], True))
        return [
            pltpu.make_async_remote_copy(
                src_ref=r4.at[s, k, r, slot, pl.ds(start, 8)], dst_ref=r5.at[s, k, r, n],
                send_sem=own_send.at[n, s], recv_sem=own_recv.at[n, s, k, r],
                device_id=to[n], device_id_type=MESH,
            )
            for n, (slot, start) in enumerate(spots)
        ]

    def step(stage, k, r):
        for s in range(4):
            first_x, second, sent2, slot0, slot_t = lay(s)
            sent, keep, onward, quarter = slots(STREAMS[s][1])
            if 3 <= stage <= 5:
                remote(s, stage - 1, k, r).wait_recv()
            if stage == 3:
                for pair in (False, True):
                    slot = slot_t if pair else slot0
                    for q in (sent, sent + 1):
                        value = held(s, k, r, pair, q)
                        if first_x:
                            r2x[s, k, r, slot, q] = value
                        else:
                            r2y[s - 2, k, r, q, slot] = value
            elif stage == 4:
                for pair in (False, True):
                    slot = slot_t if pair else slot0
                    value = held3(s, k, r, pair, onward, quarter)
                    if first_x:
                        r3[s, k, r, slot, onward] = value
                    else:
                        r3[s, k, r, onward, slot] = value
            elif stage == 5:
                for pair in (False, True):
                    slot = slot_t if pair else slot0
                    r4[s, k, r, slot] += held3(s, k, r, pair, keep, 0)
                for copy in owner_copies(s, k, r):
                    copy.start()
            elif stage == 6:
                for copy in owner_copies(s, k, r):
                    copy.wait_recv()
                first = r4[s, k, r, slot0, 0:8, :] + r5[s, k, r, 1]
                second_sum = r5[s, k, r, 0] + r5[s, k, r, 2]
                for h in range(2):
                    cols = slice(h * seg, (h + 1) * seg)
                    gath[group, r, h, part_of(s, k, True)] = first[:, cols]
                    gath[group, r, h, part_of(s, k, False)] = second_sum[:, cols]
            if stage < 5:
                remote(s, stage, k, r).start()

    def kz_remote(d, k, r, slot):
        where = gath.at[slot, r, :, pl.ds(k * 8, 8)]
        return pltpu.make_async_remote_copy(
            src_ref=where, dst_ref=where,
            send_sem=kz_send.at[d], recv_sem=kz_recv.at[slot, k, r],
            device_id=kzdevs[d], device_id_type=MESH,
        )

    def images(k, carry):
        for s in range(4):
            make(s, k)
            for r in range(2):
                remote(s, 2, k, r).start()
        return carry

    lax.fori_loop(0, 2, images, 0)

    def pipeline(i, carry):
        for stage in range(3, 7):
            c = i - (stage - 3)

            @pl.when(jnp.logical_and(c >= 0, c < 4))
            def _():
                k, r = c // 2, c % 2
                step(stage, k, r)
                if stage == 6:
                    for d in range(3):
                        kz_remote(d, k, r, group).start()

        return carry

    lax.fori_loop(0, 7, pipeline, 0)

    for c in range(4):
        for d in range(3):
            kz_remote(d, c // 2, c % 2, (group + d + 1) % 4).wait_recv()

    for mh in range(2):
        for yy in range(8):
            pieces = []
            for g in range(4):
                for r in range(2):
                    pieces.append(gath[g, r, mh, :, yy, :])
            stacked = jnp.concatenate(pieces, axis=0)
            got = jnp.dot(ztab_ref[group], stacked, preferred_element_type=F32, precision=lax.Precision.HIGHEST)
            kzout[mh, pl.ds(yy, 2 * parts, stride=8), :] = got
        out_ref[:, :, :, mh * seg : (mh + 1) * seg] = kzout[mh].reshape(2, parts, 8, seg)

    def sent_all(ref, sem, unused, peer):
        pltpu.make_async_remote_copy(
            src_ref=ref, dst_ref=ref, send_sem=sem, recv_sem=unused, device_id=peer, device_id_type=MESH
        ).wait_send()

    both = pl.ds(0, 2)
    for s in range(4):
        sens_copy(s).wait_send()
        sens_pass(s, core).wait_send()
        sent_all(other.at[s], send_sem.at[0, s], seg_recv.at[s, 0, 0], zdev)
        for stage in range(2, 5):
            src, dst, peer = copies(s, stage, both, both)
            sent_all(src, send_sem.at[stage - 1, s], recv_sem.at[stage - 2, s, 0, 0], peer)
        for n in range(3):
            sent_all(r5.at[s, :, :, n], own_send.at[n, s], own_recv.at[n, s, 0, 0], zdev)
    for d in range(3):
        sent_all(gath.at[group], kz_send.at[d], kz_recv.at[group, 0, 0], kzdevs[d])


def per_device(kdata, spoke_angle, spoke_count, block_index, interp, sens_maps):
    side = sens_maps.shape[2]
    parts = kdata.shape[1]
    spokes, samples = kdata.shape[3], kdata.shape[4]
    angles, segs, seg = interp.shape[0], interp.shape[1], interp.shape[2]
    hits = angles * segs
    any_spec = pl.BlockSpec(memory_space=pl.ANY)
    vmem_spec = pl.BlockSpec(memory_space=pltpu.VMEM)
    return pl.pallas_call(
        functools.partial(kernel, parts, angles, spokes, side),
        out_shape=jax.ShapeDtypeStruct((2, parts, 8, side), F32),
        in_specs=[pl.BlockSpec(memory_space=pltpu.SMEM)] + [vmem_spec] * 3 + [any_spec] * 4,
        out_specs=vmem_spec,
        scratch_shapes=[
            pltpu.VMEM((2, parts, spokes, samples), BF16),
            pltpu.VMEM((angles, segs, seg, seg), BF16),
            pltpu.VMEM((2, side, side), BF16),
            pltpu.VMEM((2 * side, 2 * side), BF16),
            pltpu.VMEM((2, 2 * side, 2 * hits), BF16),
            pltpu.VMEM((2, side, side), F32),
            pltpu.VMEM((4, 2, side, side), F32),
            pltpu.VMEM((segs * angles * BPAD, seg), F32),
            pltpu.VMEM((2 * parts * (hits + 8), seg), F32),
            pltpu.VMEM((4, 2, 2, hits, seg), F32),
            pltpu.VMEM((2, side, 2 * side), BF16),
            pltpu.VMEM((4, 2, 2, 4, 4, 16, side), F32),
            pltpu.VMEM((2, 2, 2, 2, 4, 16, side), F32),
            pltpu.VMEM((2, 2, 2, 4, 2, 16, side), F32),
            pltpu.VMEM((4, 2, 2, 2, 2, 16, side), F32),
            pltpu.VMEM((4, 2, 2, 2, 16, side), F32),
            pltpu.VMEM((4, 2, 2, 3, 8, side), F32),
            pltpu.VMEM((4, 2, 2, parts, 8, seg), F32),
            pltpu.VMEM((2, 2 * parts * 8, seg), F32),
            pltpu.SemaphoreType.DMA((10,)),
            pltpu.SemaphoreType.DMA((2, 4)),
            pltpu.SemaphoreType.DMA((2, 4)),
            pltpu.SemaphoreType.DMA((4, 4)),
            pltpu.SemaphoreType.DMA((4, 2, 2)),
            pltpu.SemaphoreType.DMA((3, 4, 2, 2)),
            pltpu.SemaphoreType.DMA((3, 4)),
            pltpu.SemaphoreType.DMA((3, 4, 2, 2)),
            pltpu.SemaphoreType.DMA((3,)),
            pltpu.SemaphoreType.DMA((4, 2, 2)),
        ],
        compiler_params=pltpu.CompilerParams(
            collective_id=0, has_side_effects=True, vmem_limit_bytes=63 << 20
        ),
    )(
        spoke_count,
        spoke_angle.reshape(1, spokes),
        block_index.reshape(1, hits),
        kz_table(4, parts),
        kdata[:, :, 0],
        interp,
        sens_maps[:, 0],
        plane_table(side),
    )


def solution(mesh):
    placed = (
        P(None, "kz", "coil", None, None),
        P(),
        P("kz"),
        P(),
        P(),
        P(None, "coil", None, None),
    )
    return jax.shard_map(
        per_device,
        mesh=mesh,
        in_specs=placed,
        out_specs=P(None, "kz", "coil", None),
        check_vma=False,
    )
```

```python
import functools

import jax
import jax.numpy as jnp
import numpy as np
from jax import lax
from jax.experimental import pallas as pl
from jax.experimental.pallas import tpu as pltpu
from jax.sharding import PartitionSpec as P

F32 = jnp.float32
BF16 = jnp.bfloat16
MESH = pl.DeviceIdType.MESH

BPAD = 40

STREAMS = ((True, 1), (True, 3), (False, 1), (False, 3))


def dft_np(rows, cols, length):
    product = (rows[:, None] * cols[None, :]) % length
    phase = product.astype(np.float64) * (2.0 * np.pi / length)
    return np.cos(phase) / np.sqrt(length), np.sin(phase) / np.sqrt(length)


def plane_table(side):
    index = np.arange(side)
    cos_t, sin_t = dft_np(index, index, side)
    table = np.block([[cos_t, -sin_t], [sin_t, cos_t]])
    return jnp.asarray(table, dtype=BF16)


def kz_table(groups, parts):
    total = groups * parts
    index = np.arange(total)
    cos_z, sin_z = dft_np(index, index, total)
    blocks = []
    for g in range(groups):
        c = cos_z[g * parts : (g + 1) * parts].reshape(parts, groups, 1, parts)
        s = sin_z[g * parts : (g + 1) * parts].reshape(parts, groups, 1, parts)
        real = np.concatenate([c, s], axis=2).reshape(parts, -1)
        imag = np.concatenate([-s, c], axis=2).reshape(parts, -1)
        blocks.append(np.concatenate([real, imag], axis=0))
    return jnp.asarray(np.stack(blocks), dtype=F32)


def flip(i, pairing):
    return i + 1 - 2 * (i % 2) if pairing == 1 else 3 - i


def kernel(
    parts, angles, spokes, side,
    count_ref, angle_ref, block_ref, ztab_ref,
    kdata_hbm, interp_hbm, sens_hbm, plane_hbm,
    out_ref,
    kd, itp, sens_v, plane, tab, sensp, senso, binned, spread, other, half,
    img, r2x, r2y, r3, r4, r5, gath, kzout,
    load_sem, sens_send, sens_recv, send_sem, seg_recv, recv_sem, own_send, own_recv, kz_send, kz_recv,
):
    segs = 4
    seg = 128
    hits = angles * segs
    xpad = hits + 8
    coil = lax.axis_index("coil")
    group = lax.axis_index("kz")
    core = group % 2
    x, y, z = coil // 8, (coil // 2) % 4, coil % 2

    def dev(axis_x, pairing, over_z=False):
        zz = 1 - z if over_z else z
        if axis_x:
            return ((flip(x, pairing) * 4 + y) * 2 + zz, group)
        return ((x * 4 + flip(y, pairing)) * 2 + zz, group)

    zdev = ((x * 4 + y) * 2 + 1 - z, group)
    beside = group + 1 - 2 * core
    sibling = (coil, beside)
    across = (coil, (group + 2) % 4)

    def side_of(s):
        first_x, pairing = STREAMS[s]
        i = x if first_x else y
        return ((i + 1) // 2) % 2 if pairing == 1 else i // 2

    def part_of(s, k, mine):
        return k * 8 + s * 2 + (side_of(s) if mine else 1 - side_of(s))

    loads = [
        pltpu.make_async_copy(plane_hbm, plane, load_sem.at[0]),
        pltpu.make_async_copy(sens_hbm, sens_v, load_sem.at[1]),
    ]

    def kload(q):
        rows = pl.ds(q * (parts // 4), parts // 4)
        return pltpu.make_async_copy(kdata_hbm.at[:, rows], kd.at[:, rows], load_sem.at[2 + q])

    def iload(q):
        rows = pl.ds(q * (angles // 4), angles // 4)
        return pltpu.make_async_copy(interp_hbm.at[rows], itp.at[rows], load_sem.at[6 + q])

    for copy in loads + [kload(q) for q in range(4)] + [iload(q) for q in range(4)]:
        copy.start()

    barrier = pltpu.get_barrier_semaphore()
    peers = [dev(*stream, over_z) for stream in STREAMS for over_z in (False, True)] + [zdev, sibling, across]
    for peer in peers:
        pl.semaphore_signal(barrier, inc=1, device_id=peer, device_id_type=MESH)

    for copy in loads:
        copy.wait()
    row = lax.broadcasted_iota(jnp.int32, (side, side), 0)
    col = lax.broadcasted_iota(jnp.int32, (side, side), 1)
    perm = jnp.where(jnp.bitwise_xor(row, col) == coil * 8, 1.0, 0.0).astype(BF16)
    for r in range(2):
        sensp[r] = jnp.dot(perm, sens_v[r], preferred_element_type=F32)

    def sens_copy(s):
        return pltpu.make_async_remote_copy(
            src_ref=sensp.at[core], dst_ref=senso.at[s, core],
            send_sem=sens_send.at[0, s], recv_sem=sens_recv.at[0, s],
            device_id=dev(*STREAMS[s]), device_id_type=MESH,
        )

    def sens_pass(s, r):
        return pltpu.make_async_remote_copy(
            src_ref=senso.at[s, r], dst_ref=senso.at[s, r],
            send_sem=sens_send.at[1, s], recv_sem=sens_recv.at[1, s],
            device_id=sibling, device_id_type=MESH,
        )

    cos_p = jnp.dot(perm, plane[0:side, 0:side], preferred_element_type=F32).astype(BF16)
    sin_p = jnp.dot(perm, plane[side : 2 * side, 0:side], preferred_element_type=F32).astype(BF16)
    blocks = jnp.concatenate([block_ref[g : g + 1, :] for g in range(segs)], axis=1)
    blocks = jnp.broadcast_to(blocks, (side, hits))
    yrow = lax.broadcasted_iota(jnp.int32, (side, hits), 0)
    for h in range(2):
        onto = jnp.where(blocks == yrow * 2 + h, 1.0, 0.0).astype(BF16)
        cos_g = jnp.dot(cos_p, onto, preferred_element_type=F32)
        sin_g = jnp.dot(sin_p, onto, preferred_element_type=F32)
        tab[h, 0:side, 0:hits] = cos_g.astype(BF16)
        tab[h, side : 2 * side, hits : 2 * hits] = cos_g.astype(BF16)
        tab[h, 0:side, hits : 2 * hits] = sin_g.astype(BF16)
        tab[h, side : 2 * side, 0:hits] = (-sin_g).astype(BF16)

    arow = lax.broadcasted_iota(jnp.int32, (angles, spokes), 0)
    scol = lax.broadcasted_iota(jnp.int32, (angles, spokes), 1)
    match = jnp.broadcast_to(angle_ref[0:1, :], (angles, spokes)) == arow
    def bin_some(q, carry):
        kload(q).wait()
        for i in range(parts // 4):
            p = q * (parts // 4) + i
            used = jnp.logical_and(match, scol < count_ref[p])
            weights = jnp.where(used, 1.0, 0.0).astype(BF16)
            for r in range(2):
                summed = jnp.dot(weights, kd[r, p], preferred_element_type=F32)
                for g in range(segs):
                    start = g * angles * BPAD + r * parts + p
                    binned[pl.ds(start, angles, stride=BPAD), :] = summed[:, g * seg : (g + 1) * seg]
        return carry

    lax.fori_loop(0, 4, bin_some, 0)

    pl.semaphore_wait(barrier, len(peers))

    for s in range(4):
        sens_copy(s).start()

    def spread_some(q, carry):
        iload(q).wait()
        for k in range(angles // 4):
            a = q * (angles // 4) + k
            for g in range(segs):
                start = pl.multiple_of(g * angles * BPAD + a * BPAD, 8)
                piece = binned[pl.ds(start, 2 * parts), :].astype(BF16)
                got = jnp.dot(piece, itp[a, g], preferred_element_type=F32)
                spread[pl.ds(g * angles + a, 2 * parts, stride=xpad), :] = got
        return carry

    lax.fori_loop(0, 4, spread_some, 0)

    def seg_rows(p, r):
        return pl.ds(pl.multiple_of((r * parts + p) * xpad, 8), hits)

    def seg_copy(s, k, r):
        return pltpu.make_async_remote_copy(
            src_ref=spread.at[seg_rows(part_of(s, k, False), r)], dst_ref=other.at[s, k, r],
            send_sem=send_sem.at[0, s], recv_sem=seg_recv.at[s, k, r],
            device_id=dev(*STREAMS[s]), device_id_type=MESH,
        )

    for k in range(2):
        for s in range(4):
            for r in range(2):
                seg_copy(s, k, r).start()
    for s in range(4):
        sens_copy(s).wait_recv()
        sens_pass(s, core).start()
    for s in range(4):
        sens_pass(s, 1 - core).wait_recv()

    def slots(pairing):
        return (1, 0, 1, 3) if pairing == 1 else (2, 1, 0, 1)

    def lay(s):
        first_x, pairing = STREAMS[s]
        return (first_x, 3, 2, 1, 0) if pairing == 1 else (first_x, 1, 1, 0, 1)

    def make(s, k):
        first_x, pairing = STREAMS[s]
        for r in range(2):
            seg_copy(s, k, r).wait_recv()
        p = part_of(s, k, True)
        rows = []
        for r in range(2):
            own = spread[seg_rows(p, r), :].astype(BF16)
            rows.append(jnp.concatenate([own, other[s, k, r].astype(BF16)], axis=1))
        stacked = jnp.concatenate(rows, axis=0)
        for h in range(2):
            got = jnp.dot(tab[h], stacked, preferred_element_type=F32).astype(BF16)
            for n in range(2):
                for r in range(2):
                    half[n, :, r * side + h * seg : r * side + (h + 1) * seg] = got[
                        r * side : (r + 1) * side, n * seg : (n + 1) * seg
                    ]
        mine = jnp.dot(half[0], plane[...], preferred_element_type=F32)
        theirs = jnp.dot(half[1], plane[...], preferred_element_type=F32)
        for jx in range(4):
            for jy in range(4):
                here = slice((jx * 4 + jy) * 16, (jx * 4 + jy + 1) * 16)
                there = (jx ^ pairing) * 4 + jy if first_x else jx * 4 + (jy ^ pairing)
                that = slice(there * 16, (there + 1) * 16)
                a_re, a_im = sensp[0, here, :], sensp[1, here, :]
                b_re, b_im = senso[s, 0, that, :], senso[s, 1, that, :]
                o_re, o_im = mine[here, 0:side], mine[here, side : 2 * side]
                t_re, t_im = theirs[here, 0:side], theirs[here, side : 2 * side]
                img[s, k, 0, jx, jy] = (a_re * o_re + a_im * o_im) + (b_re * t_re + b_im * t_im)
                img[s, k, 1, jx, jy] = (a_re * o_im - a_im * o_re) + (b_re * t_im - b_im * t_re)

    def copies(s, stage, k, r):
        first_x, second, sent2, slot0, slot_t = lay(s)
        pairing = STREAMS[s][1]
        sent, keep, onward, quarter = slots(pairing)
        if stage == 2:
            if first_x:
                return img.at[s, k, r, pl.ds(sent2, 2)], r2x.at[s, k, r], dev(True, second)
            return img.at[s, k, r, :, pl.ds(sent2, 2)], r2y.at[s - 2, k, r], dev(False, second)
        if stage == 3:
            if first_x:
                return r2x.at[s, k, r, :, pl.ds(sent, 2)], r3.at[s, k, r], dev(False, pairing)
            return r2y.at[s - 2, k, r, pl.ds(sent, 2)], r3.at[s, k, r], dev(True, pairing)
        src = r3.at[s, k, r, :, onward] if first_x else r3.at[s, k, r, onward]
        return src, r4.at[s, k, r], dev(not first_x, second)

    def remote(s, stage, k, r):
        src, dst, peer = copies(s, stage, k, r)
        return pltpu.make_async_remote_copy(
            src_ref=src, dst_ref=dst,
            send_sem=send_sem.at[stage - 1, s], recv_sem=recv_sem.at[stage - 2, s, k, r],
            device_id=peer, device_id_type=MESH,
        )

    def held(s, k, r, pair, quarter):
        first_x, second, sent2, slot0, slot_t = lay(s)
        j = STREAMS[s][1] if pair else 0
        slot = slot_t if pair else slot0
        if first_x:
            return img[s, k, r, j, quarter] + r2x[s, k, r, slot, quarter]
        return img[s, k, r, quarter, j] + r2y[s - 2, k, r, quarter, slot]

    def held3(s, k, r, pair, which, quarter):
        first_x, second, sent2, slot0, slot_t = lay(s)
        slot = slot_t if pair else slot0
        got = r3[s, k, r, slot, which] if first_x else r3[s, k, r, which, slot]
        return held(s, k, r, pair, quarter) + got

    def owner_copies(s, k, r):
        first_x, second, sent2, slot0, slot_t = lay(s)
        spots = ((slot_t, 0), (slot0, 8), (slot_t, 8))
        to = (dev(*STREAMS[s]), zdev, dev(*STREAMS[s], True))
        return [
            pltpu.make_async_remote_copy(
                src_ref=r4.at[s, k, r, slot, pl.ds(start, 8)], dst_ref=r5.at[s, k, r, n],
                send_sem=own_send.at[n, s], recv_sem=own_recv.at[n, s, k, r],
                device_id=to[n], device_id_type=MESH,
            )
            for n, (slot, start) in enumerate(spots)
        ]

    def step(stage, k, r):
        for s in range(4):
            first_x, second, sent2, slot0, slot_t = lay(s)
            sent, keep, onward, quarter = slots(STREAMS[s][1])
            if 3 <= stage <= 5:
                remote(s, stage - 1, k, r).wait_recv()
            if stage == 3:
                for pair in (False, True):
                    slot = slot_t if pair else slot0
                    for q in (sent, sent + 1):
                        value = held(s, k, r, pair, q)
                        if first_x:
                            r2x[s, k, r, slot, q] = value
                        else:
                            r2y[s - 2, k, r, q, slot] = value
            elif stage == 4:
                for pair in (False, True):
                    slot = slot_t if pair else slot0
                    value = held3(s, k, r, pair, onward, quarter)
                    if first_x:
                        r3[s, k, r, slot, onward] = value
                    else:
                        r3[s, k, r, onward, slot] = value
            elif stage == 5:
                for pair in (False, True):
                    slot = slot_t if pair else slot0
                    r4[s, k, r, slot] += held3(s, k, r, pair, keep, 0)
                for copy in owner_copies(s, k, r):
                    copy.start()
            elif stage == 6:
                for copy in owner_copies(s, k, r):
                    copy.wait_recv()
                first = r4[s, k, r, slot0, 0:8, :] + r5[s, k, r, 1]
                second_sum = r5[s, k, r, 0] + r5[s, k, r, 2]
                for h in range(2):
                    cols = slice(h * seg, (h + 1) * seg)
                    gath[group, r, h, part_of(s, k, True)] = first[:, cols]
                    gath[group, r, h, part_of(s, k, False)] = second_sum[:, cols]
            if stage < 5:
                remote(s, stage, k, r).start()

    def kz_remote(n, k, r, slot, peer):
        where = gath.at[slot, r, :, pl.ds(k * 8, 8)]
        return pltpu.make_async_remote_copy(
            src_ref=where, dst_ref=where,
            send_sem=kz_send.at[n], recv_sem=kz_recv.at[slot, k, r],
            device_id=peer, device_id_type=MESH,
        )

    def images(k, carry):
        for s in range(4):
            make(s, k)
            for r in range(2):
                remote(s, 2, k, r).start()
        return carry

    lax.fori_loop(0, 2, images, 0)

    for stage in range(3, 7):

        def stage_items(c, carry):
            k, r = c // 2, c % 2
            step(stage, k, r)
            if stage == 6:
                kz_remote(0, k, r, group, across).start()
                kz_remote(1, k, r, group, sibling).start()
            return carry

        lax.fori_loop(0, 4, stage_items, 0)

    far = (group + 2) % 4
    for c in range(4):
        k, r = c // 2, c % 2
        kz_remote(0, k, r, far, across).wait_recv()
        kz_remote(2, k, r, far, sibling).start()
    for c in range(4):
        k, r = c // 2, c % 2
        kz_remote(1, k, r, beside, sibling).wait_recv()
        kz_remote(2, k, r, (beside + 2) % 4, sibling).wait_recv()

    for mh in range(2):
        for yy in range(8):
            pieces = []
            for g in range(4):
                for r in range(2):
                    pieces.append(gath[g, r, mh, :, yy, :])
            stacked = jnp.concatenate(pieces, axis=0)
            got = jnp.dot(ztab_ref[group], stacked, preferred_element_type=F32, precision=lax.Precision.HIGHEST)
            kzout[mh, pl.ds(yy, 2 * parts, stride=8), :] = got
        out_ref[:, :, :, mh * seg : (mh + 1) * seg] = kzout[mh].reshape(2, parts, 8, seg)

    def sent_all(ref, sem, unused, peer):
        pltpu.make_async_remote_copy(
            src_ref=ref, dst_ref=ref, send_sem=sem, recv_sem=unused, device_id=peer, device_id_type=MESH
        ).wait_send()

    both = pl.ds(0, 2)
    for s in range(4):
        sens_copy(s).wait_send()
        sens_pass(s, core).wait_send()
        sent_all(other.at[s], send_sem.at[0, s], seg_recv.at[s, 0, 0], zdev)
        for stage in range(2, 5):
            src, dst, peer = copies(s, stage, both, both)
            sent_all(src, send_sem.at[stage - 1, s], recv_sem.at[stage - 2, s, 0, 0], peer)
        for n in range(3):
            sent_all(r5.at[s, :, :, n], own_send.at[n, s], own_recv.at[n, s, 0, 0], zdev)
    for n in range(3):
        sent_all(gath.at[group], kz_send.at[n], kz_recv.at[group, 0, 0], sibling)


def per_device(kdata, spoke_angle, spoke_count, block_index, interp, sens_maps):
    side = sens_maps.shape[2]
    parts = kdata.shape[1]
    spokes, samples = kdata.shape[3], kdata.shape[4]
    angles, segs, seg = interp.shape[0], interp.shape[1], interp.shape[2]
    hits = angles * segs
    any_spec = pl.BlockSpec(memory_space=pl.ANY)
    vmem_spec = pl.BlockSpec(memory_space=pltpu.VMEM)
    return pl.pallas_call(
        functools.partial(kernel, parts, angles, spokes, side),
        out_shape=jax.ShapeDtypeStruct((2, parts, 8, side), F32),
        in_specs=[pl.BlockSpec(memory_space=pltpu.SMEM)] + [vmem_spec] * 3 + [any_spec] * 4,
        out_specs=vmem_spec,
        scratch_shapes=[
            pltpu.VMEM((2, parts, spokes, samples), BF16),
            pltpu.VMEM((angles, segs, seg, seg), BF16),
            pltpu.VMEM((2, side, side), BF16),
            pltpu.VMEM((2 * side, 2 * side), BF16),
            pltpu.VMEM((2, 2 * side, 2 * hits), BF16),
            pltpu.VMEM((2, side, side), F32),
            pltpu.VMEM((4, 2, side, side), F32),
            pltpu.VMEM((segs * angles * BPAD, seg), F32),
            pltpu.VMEM((2 * parts * (hits + 8), seg), F32),
            pltpu.VMEM((4, 2, 2, hits, seg), F32),
            pltpu.VMEM((2, side, 2 * side), BF16),
            pltpu.VMEM((4, 2, 2, 4, 4, 16, side), F32),
            pltpu.VMEM((2, 2, 2, 2, 4, 16, side), F32),
            pltpu.VMEM((2, 2, 2, 4, 2, 16, side), F32),
            pltpu.VMEM((4, 2, 2, 2, 2, 16, side), F32),
            pltpu.VMEM((4, 2, 2, 2, 16, side), F32),
            pltpu.VMEM((4, 2, 2, 3, 8, side), F32),
            pltpu.VMEM((4, 2, 2, parts, 8, seg), F32),
            pltpu.VMEM((2, 2 * parts * 8, seg), F32),
            pltpu.SemaphoreType.DMA((10,)),
            pltpu.SemaphoreType.DMA((2, 4)),
            pltpu.SemaphoreType.DMA((2, 4)),
            pltpu.SemaphoreType.DMA((4, 4)),
            pltpu.SemaphoreType.DMA((4, 2, 2)),
            pltpu.SemaphoreType.DMA((3, 4, 2, 2)),
            pltpu.SemaphoreType.DMA((3, 4)),
            pltpu.SemaphoreType.DMA((3, 4, 2, 2)),
            pltpu.SemaphoreType.DMA((3,)),
            pltpu.SemaphoreType.DMA((4, 2, 2)),
        ],
        compiler_params=pltpu.CompilerParams(
            collective_id=0, has_side_effects=True, vmem_limit_bytes=63 << 20
        ),
    )(
        spoke_count,
        spoke_angle.reshape(1, spokes),
        block_index.T,
        kz_table(4, parts),
        kdata[:, :, 0],
        interp,
        sens_maps[:, 0],
        plane_table(side),
    )


def solution(mesh):
    placed = (
        P(None, "kz", "coil", None, None),
        P(),
        P("kz"),
        P(),
        P(),
        P(None, "coil", None, None),
    )
    return jax.shard_map(
        per_device,
        mesh=mesh,
        in_specs=placed,
        out_specs=P(None, "kz", "coil", None),
        check_vma=False,
    )
```

```python
import functools

import jax
import jax.numpy as jnp
import numpy as np
from jax import lax
from jax.experimental import pallas as pl
from jax.experimental.pallas import tpu as pltpu
from jax.sharding import PartitionSpec as P

F32 = jnp.float32
BF16 = jnp.bfloat16
MESH = pl.DeviceIdType.MESH

EARLY = ((0, 1, 2, 3), (4, 5, 6, 7))
BETWEEN = (((), (), (), ()), ((), (), (), ()))
PLAN = [(w, c) for w in "34" for c in range(8)] + [(w, c) for w in "XF" for c in range(4)]
BARRIER_AT = 1
BPAD = 40

STREAMS = ((True, 1), (True, 3), (False, 1), (False, 3))


def dft_np(rows, cols, length):
    product = (rows[:, None] * cols[None, :]) % length
    phase = product.astype(np.float64) * (2.0 * np.pi / length)
    return np.cos(phase) / np.sqrt(length), np.sin(phase) / np.sqrt(length)


def plane_table(side):
    index = np.arange(side)
    cos_t, sin_t = dft_np(index, index, side)
    table = np.block([[cos_t, -sin_t], [sin_t, cos_t]])
    return jnp.asarray(table, dtype=BF16)


def kz_table(groups, parts):
    total = groups * parts
    index = np.arange(total)
    cos_z, sin_z = dft_np(index, index, total)
    blocks = []
    for g in range(groups):
        c = cos_z[g * parts : (g + 1) * parts].reshape(parts, groups, 1, parts)
        s = sin_z[g * parts : (g + 1) * parts].reshape(parts, groups, 1, parts)
        real = np.concatenate([c, s], axis=2).reshape(parts, -1)
        imag = np.concatenate([-s, c], axis=2).reshape(parts, -1)
        blocks.append(np.concatenate([real, imag], axis=0))
    return jnp.asarray(np.stack(blocks), dtype=F32)


def flip(i, pairing):
    return i + 1 - 2 * (i % 2) if pairing == 1 else 3 - i


def kernel(
    parts, angles, spokes, side,
    count_ref, angle_ref, block_ref,
    kdata_hbm, interp_hbm, sens_hbm, plane_hbm,
    gath,
    kd, itp, sens_v, plane, tab, sensp, senso, binned, spread, other, half,
    img, r2x, r2y, r3, r4, xbuf, rx,
    load_sem, sens_send, sens_recv, send_sem, seg_recv, recv_sem, own_send, own_recv, kz_send, kz_recv,
):
    segs = 4
    seg = 128
    hits = angles * segs
    xpad = hits + 8
    coil = lax.axis_index("coil")
    group = lax.axis_index("kz")
    core = group % 2
    x, y, z = coil // 8, (coil // 2) % 4, coil % 2

    beside = group + 1 - 2 * core
    far = (group + 2) % 4
    sibling = (coil, beside)

    def dev(axis_x, pairing, over_z=0, over_kz=0):
        zz = 1 - z if over_z else z
        there = far if over_kz else group
        if axis_x:
            return ((flip(x, pairing) * 4 + y) * 2 + zz, there)
        return ((x * 4 + flip(y, pairing)) * 2 + zz, there)

    def zdev(over_z, over_kz):
        return ((x * 4 + y) * 2 + (1 - z if over_z else z), far if over_kz else group)

    def side_of(s):
        first_x, pairing = STREAMS[s]
        i = x if first_x else y
        return ((i + 1) // 2) % 2 if pairing == 1 else i // 2

    def part_of(s, k, mine):
        return k * 8 + s * 2 + (side_of(s) if mine else 1 - side_of(s))

    loads = [
        pltpu.make_async_copy(plane_hbm, plane, load_sem.at[0]),
        pltpu.make_async_copy(sens_hbm, sens_v, load_sem.at[1]),
    ]

    def kload(q):
        rows = pl.ds(q * (parts // 4), parts // 4)
        return pltpu.make_async_copy(kdata_hbm.at[:, rows], kd.at[:, rows], load_sem.at[2 + q])

    def iload(q):
        rows = pl.ds(q * (angles // 4), angles // 4)
        return pltpu.make_async_copy(interp_hbm.at[rows], itp.at[rows], load_sem.at[6 + q])

    for copy in loads + [kload(q) for q in range(4)] + [iload(q) for q in range(4)]:
        copy.start()

    barrier = pltpu.get_barrier_semaphore()
    turns = [(0, 0), (0, 1), (1, 0), (1, 1)]
    peers = [dev(*stream, *turn) for stream in STREAMS for turn in turns]
    peers += [zdev(*turn) for turn in turns[1:]] + [sibling]
    for peer in peers:
        pl.semaphore_signal(barrier, inc=1, device_id=peer, device_id_type=MESH)

    for copy in loads:
        copy.wait()
    row = lax.broadcasted_iota(jnp.int32, (side, side), 0)
    col = lax.broadcasted_iota(jnp.int32, (side, side), 1)
    perm = jnp.where(jnp.bitwise_xor(row, col) == coil * 8, 1.0, 0.0).astype(BF16)
    for r in range(2):
        sensp[r] = jnp.dot(perm, sens_v[r], preferred_element_type=F32)

    def sens_copy(s):
        return pltpu.make_async_remote_copy(
            src_ref=sensp.at[core], dst_ref=senso.at[s, core],
            send_sem=sens_send.at[0, s], recv_sem=sens_recv.at[0, s],
            device_id=dev(*STREAMS[s]), device_id_type=MESH,
        )

    def sens_pass(s, r):
        return pltpu.make_async_remote_copy(
            src_ref=senso.at[s, r], dst_ref=senso.at[s, r],
            send_sem=sens_send.at[1, s], recv_sem=sens_recv.at[1, s],
            device_id=sibling, device_id_type=MESH,
        )

    cos_p = jnp.dot(perm, plane[0:side, 0:side], preferred_element_type=F32).astype(BF16)
    sin_p = jnp.dot(perm, plane[side : 2 * side, 0:side], preferred_element_type=F32).astype(BF16)
    blocks = jnp.concatenate([block_ref[g : g + 1, :] for g in range(segs)], axis=1)
    blocks = jnp.broadcast_to(blocks, (side, hits))
    yrow = lax.broadcasted_iota(jnp.int32, (side, hits), 0)
    for h in range(2):
        onto = jnp.where(blocks == yrow * 2 + h, 1.0, 0.0).astype(BF16)
        cos_g = jnp.dot(cos_p, onto, preferred_element_type=F32)
        sin_g = jnp.dot(sin_p, onto, preferred_element_type=F32)
        tab[h, 0:side, 0:hits] = cos_g.astype(BF16)
        tab[h, side : 2 * side, hits : 2 * hits] = cos_g.astype(BF16)
        tab[h, 0:side, hits : 2 * hits] = sin_g.astype(BF16)
        tab[h, side : 2 * side, 0:hits] = (-sin_g).astype(BF16)

    arow = lax.broadcasted_iota(jnp.int32, (angles, spokes), 0)
    scol = lax.broadcasted_iota(jnp.int32, (angles, spokes), 1)
    match = jnp.broadcast_to(angle_ref[0:1, :], (angles, spokes)) == arow
    def bin_some(q, carry):
        kload(q).wait()
        for i in range(parts // 4):
            p = q * (parts // 4) + i
            used = jnp.logical_and(match, scol < count_ref[p])
            weights = jnp.where(used, 1.0, 0.0).astype(BF16)
            for r in range(2):
                summed = jnp.dot(weights, kd[r, p], preferred_element_type=F32)
                for g in range(segs):
                    start = g * angles * BPAD + r * parts + p
                    binned[pl.ds(start, angles, stride=BPAD), :] = summed[:, g * seg : (g + 1) * seg]
        return carry

    lax.fori_loop(0, BARRIER_AT, bin_some, 0)
    pl.semaphore_wait(barrier, len(peers))
    for s in range(4):
        sens_copy(s).start()
    lax.fori_loop(BARRIER_AT, 4, bin_some, 0)

    def spread_some(q, carry):
        iload(q).wait()
        for k in range(angles // 4):
            a = q * (angles // 4) + k
            for g in range(segs):
                start = pl.multiple_of(g * angles * BPAD + a * BPAD, 8)
                piece = binned[pl.ds(start, 2 * parts), :].astype(BF16)
                got = jnp.dot(piece, itp[a, g], preferred_element_type=F32)
                spread[pl.ds(g * angles + a, 2 * parts, stride=xpad), :] = got
        return carry

    lax.fori_loop(0, 4, spread_some, 0)

    def seg_rows(p, r):
        return pl.ds(pl.multiple_of((r * parts + p) * xpad, 8), hits)

    def seg_copy(s, k, r):
        return pltpu.make_async_remote_copy(
            src_ref=spread.at[seg_rows(part_of(s, k, False), r)], dst_ref=other.at[s, k, r],
            send_sem=send_sem.at[0, s], recv_sem=seg_recv.at[s, k, r],
            device_id=dev(*STREAMS[s]), device_id_type=MESH,
        )

    for k in range(2):
        for s in range(4):
            for r in range(2):
                seg_copy(s, k, r).start()
    for s in range(4):
        sens_copy(s).wait_recv()
        sens_pass(s, core).start()
    for s in range(4):
        sens_pass(s, 1 - core).wait_recv()

    def slots(pairing):
        return (1, 0, 1, 3) if pairing == 1 else (2, 1, 0, 1)

    def lay(s):
        first_x, pairing = STREAMS[s]
        return (first_x, 3, 2, 1, 0) if pairing == 1 else (first_x, 1, 1, 0, 1)

    def make(s, k):
        first_x, pairing = STREAMS[s]
        for r in range(2):
            seg_copy(s, k, r).wait_recv()
        p = part_of(s, k, True)
        rows = []
        for r in range(2):
            own = spread[seg_rows(p, r), :].astype(BF16)
            rows.append(jnp.concatenate([own, other[s, k, r].astype(BF16)], axis=1))
        stacked = jnp.concatenate(rows, axis=0)
        for h in range(2):
            got = jnp.dot(tab[h], stacked, preferred_element_type=F32).astype(BF16)
            for n in range(2):
                for r in range(2):
                    half[n, :, r * side + h * seg : r * side + (h + 1) * seg] = got[
                        r * side : (r + 1) * side, n * seg : (n + 1) * seg
                    ]
        mine = jnp.dot(half[0], plane[...], preferred_element_type=F32)
        theirs = jnp.dot(half[1], plane[...], preferred_element_type=F32)
        for jx in range(4):
            for jy in range(4):
                here = slice((jx * 4 + jy) * 16, (jx * 4 + jy + 1) * 16)
                there = (jx ^ pairing) * 4 + jy if first_x else jx * 4 + (jy ^ pairing)
                that = slice(there * 16, (there + 1) * 16)
                a_re, a_im = sensp[0, here, :], sensp[1, here, :]
                b_re, b_im = senso[s, 0, that, :], senso[s, 1, that, :]
                o_re, o_im = mine[here, 0:side], mine[here, side : 2 * side]
                t_re, t_im = theirs[here, 0:side], theirs[here, side : 2 * side]
                parts_of = (
                    (a_re * o_re + a_im * o_im) + (b_re * t_re + b_im * t_im),
                    (a_re * o_im - a_im * o_re) + (b_re * t_im - b_im * t_re),
                )
                for r in range(2):
                    for h in range(2):
                        img[s, k * 4 + r * 2 + h, jx, jy] = parts_of[r][:, h * seg : (h + 1) * seg]

    def copies(s, stage, c):
        first_x, second, sent2, slot0, slot_t = lay(s)
        pairing = STREAMS[s][1]
        sent, keep, onward, quarter = slots(pairing)
        if stage == 2:
            if first_x:
                return img.at[s, c, pl.ds(sent2, 2)], r2x.at[s, c], dev(True, second)
            return img.at[s, c, :, pl.ds(sent2, 2)], r2y.at[s - 2, c], dev(False, second)
        if stage == 3:
            if first_x:
                return r2x.at[s, c, :, pl.ds(sent, 2)], r3.at[s, c], dev(False, pairing)
            return r2y.at[s - 2, c, pl.ds(sent, 2)], r3.at[s, c], dev(True, pairing)
        src = r3.at[s, c, :, onward] if first_x else r3.at[s, c, onward]
        return src, r4.at[s, c], dev(not first_x, second)

    def remote(s, stage, c):
        src, dst, peer = copies(s, stage, c)
        return pltpu.make_async_remote_copy(
            src_ref=src, dst_ref=dst,
            send_sem=send_sem.at[stage - 1, s], recv_sem=recv_sem.at[stage - 2, s, c],
            device_id=peer, device_id_type=MESH,
        )

    def held(s, c, pair, quarter):
        first_x, second, sent2, slot0, slot_t = lay(s)
        j = STREAMS[s][1] if pair else 0
        slot = slot_t if pair else slot0
        if first_x:
            return img[s, c, j, quarter] + r2x[s, c, slot, quarter]
        return img[s, c, quarter, j] + r2y[s - 2, c, quarter, slot]

    def held3(s, c, pair, which, quarter):
        first_x, second, sent2, slot0, slot_t = lay(s)
        slot = slot_t if pair else slot0
        got = r3[s, c, slot, which] if first_x else r3[s, c, which, slot]
        return held(s, c, pair, quarter) + got

    def step(stage, c):
        for s in range(4):
            first_x, second, sent2, slot0, slot_t = lay(s)
            sent, keep, onward, quarter = slots(STREAMS[s][1])
            remote(s, stage - 1, c).wait_recv()
            for pair in range(2):
                slot = slot_t if pair else slot0
                if stage == 3:
                    for q in (sent, sent + 1):
                        value = held(s, c, pair, q)
                        if first_x:
                            r2x[s, c, slot, q] = value
                        else:
                            r2y[s - 2, c, q, slot] = value
                else:
                    value = held3(s, c, pair, onward, quarter)
                    if first_x:
                        r3[s, c, slot, onward] = value
                    else:
                        r3[s, c, onward, slot] = value
            remote(s, stage, c).start()

    def last_copies(kr, pair, s):
        got = []
        for jz, jk in turns:
            n = pair * 4 + jz * 2 + jk
            if n == 0:
                continue
            if pair:
                src, dst, peer = xbuf.at[1, kr, jz, s], rx.at[n, kr, s], dev(*STREAMS[s], jz, jk)
            else:
                src, dst, peer = xbuf.at[0, kr, jz], rx.at[n, kr], zdev(jz, jk)
            got.append(
                pltpu.make_async_remote_copy(
                    src_ref=src, dst_ref=dst, send_sem=own_send.at[n], recv_sem=own_recv.at[n, kr],
                    device_id=peer, device_id_type=MESH,
                )
            )
        return got

    def last(kr):
        for s in range(4):
            first_x, second, sent2, slot0, slot_t = lay(s)
            keep = slots(STREAMS[s][1])[1]
            for h in range(2):
                c = kr * 2 + h
                remote(s, 4, c).wait_recv()
                for pair in range(2):
                    slot = slot_t if pair else slot0
                    value = r4[s, c, slot] + held3(s, c, pair, keep, 0)
                    for jz in range(2):
                        xbuf[pair, kr, jz, s, h] = value[jz * 8 : (jz + 1) * 8]
            for copy in last_copies(kr, 1, s):
                copy.start()
        for copy in last_copies(kr, 0, 0):
            copy.start()

    def arrived(n, kr):
        whole = rx.at[n, kr]
        return pltpu.make_async_remote_copy(
            src_ref=whole, dst_ref=whole, send_sem=own_send.at[n], recv_sem=own_recv.at[n, kr],
            device_id=sibling, device_id_type=MESH,
        )

    def kz_remote(n, kr):
        slot = far if n else group
        where = gath.at[slot, kr % 2, :, pl.ds(kr // 2 * 8, 8)]
        return pltpu.make_async_remote_copy(
            src_ref=where, dst_ref=where,
            send_sem=kz_send.at[n], recv_sem=kz_recv.at[n, kr],
            device_id=sibling, device_id_type=MESH,
        )

    def finish(kr):
        k, r = kr // 2, kr % 2
        for n in range(1, 8):
            arrived(n, kr).wait_recv()
        for s in range(4):
            for h in range(2):
                gath[group, r, h, part_of(s, k, True)] = xbuf[0, kr, 0, s, h] + rx[2, kr, s, h]
                gath[group, r, h, part_of(s, k, False)] = rx[4, kr, s, h] + rx[6, kr, s, h]
                gath[far, r, h, part_of(s, k, True)] = rx[1, kr, s, h] + rx[3, kr, s, h]
                gath[far, r, h, part_of(s, k, False)] = rx[5, kr, s, h] + rx[7, kr, s, h]
        for n in range(2):
            kz_remote(n, kr).start()

    def run(plan):
        for what, c in plan:
            if what == "2":
                for s in range(4):
                    remote(s, 2, c).start()
            elif what == "X":
                last(c)
            elif what == "F":
                finish(c)
            else:
                step(int(what), c)

    for k in range(2):
        for s in range(4):
            make(s, k)
            for c in EARLY[k]:
                remote(s, 2, c).start()
            run(BETWEEN[k][s])
    run(PLAN)

    for kr in range(4):
        for n in range(2):
            kz_remote(n, kr).wait_recv()

    def sent_all(ref, sem, unused, peer):
        pltpu.make_async_remote_copy(
            src_ref=ref, dst_ref=ref, send_sem=sem, recv_sem=unused, device_id=peer, device_id_type=MESH
        ).wait_send()

    everything = pl.ds(0, 8)
    for s in range(4):
        sens_copy(s).wait_send()
        sens_pass(s, core).wait_send()
        sent_all(other.at[s], send_sem.at[0, s], seg_recv.at[s, 0, 0], sibling)
        for stage in range(2, 5):
            src, dst, peer = copies(s, stage, everything)
            sent_all(src, send_sem.at[stage - 1, s], recv_sem.at[stage - 2, s, 0], peer)
    for n in range(1, 8):
        sent_all(rx.at[n], own_send.at[n], own_recv.at[n, 0], sibling)
    for n in range(2):
        sent_all(gath.at[group], kz_send.at[n], kz_recv.at[n, 0], sibling)


def kz_kernel(parts, ztab_ref, gath, out_ref, kzout):
    seg = 128
    group = lax.axis_index("kz")
    for mh in range(2):
        for yy in range(8):
            pieces = []
            for g in range(4):
                for r in range(2):
                    pieces.append(gath[g, r, mh, :, yy, :])
            stacked = jnp.concatenate(pieces, axis=0)
            got = jnp.dot(ztab_ref[group], stacked, preferred_element_type=F32, precision=lax.Precision.HIGHEST)
            kzout[mh, pl.ds(yy, 2 * parts, stride=8), :] = got
        out_ref[:, :, :, mh * seg : (mh + 1) * seg] = kzout[mh].reshape(2, parts, 8, seg)


def per_device(kdata, spoke_angle, spoke_count, block_index, interp, sens_maps):
    side = sens_maps.shape[2]
    parts = kdata.shape[1]
    spokes, samples = kdata.shape[3], kdata.shape[4]
    angles, segs, seg = interp.shape[0], interp.shape[1], interp.shape[2]
    hits = angles * segs
    any_spec = pl.BlockSpec(memory_space=pl.ANY)
    vmem_spec = pl.BlockSpec(memory_space=pltpu.VMEM)
    gathered = pl.pallas_call(
        functools.partial(kernel, parts, angles, spokes, side),
        out_shape=jax.ShapeDtypeStruct((4, 2, 2, parts, 8, seg), F32),
        in_specs=[pl.BlockSpec(memory_space=pltpu.SMEM)] + [vmem_spec] * 2 + [any_spec] * 4,
        out_specs=vmem_spec,
        scratch_shapes=[
            pltpu.VMEM((2, parts, spokes, samples), BF16),
            pltpu.VMEM((angles, segs, seg, seg), BF16),
            pltpu.VMEM((2, side, side), BF16),
            pltpu.VMEM((2 * side, 2 * side), BF16),
            pltpu.VMEM((2, 2 * side, 2 * hits), BF16),
            pltpu.VMEM((2, side, side), F32),
            pltpu.VMEM((4, 2, side, side), F32),
            pltpu.VMEM((segs * angles * BPAD, seg), F32),
            pltpu.VMEM((2 * parts * (hits + 8), seg), F32),
            pltpu.VMEM((4, 2, 2, hits, seg), F32),
            pltpu.VMEM((2, side, 2 * side), BF16),
            pltpu.VMEM((4, 8, 4, 4, 16, seg), F32),
            pltpu.VMEM((2, 8, 2, 4, 16, seg), F32),
            pltpu.VMEM((2, 8, 4, 2, 16, seg), F32),
            pltpu.VMEM((4, 8, 2, 2, 16, seg), F32),
            pltpu.VMEM((4, 8, 2, 16, seg), F32),
            pltpu.VMEM((2, 4, 2, 4, 2, 8, seg), F32),
            pltpu.VMEM((8, 4, 4, 2, 8, seg), F32),
            pltpu.SemaphoreType.DMA((10,)),
            pltpu.SemaphoreType.DMA((2, 4)),
            pltpu.SemaphoreType.DMA((2, 4)),
            pltpu.SemaphoreType.DMA((4, 4)),
            pltpu.SemaphoreType.DMA((4, 2, 2)),
            pltpu.SemaphoreType.DMA((3, 4, 8)),
            pltpu.SemaphoreType.DMA((8,)),
            pltpu.SemaphoreType.DMA((8, 4)),
            pltpu.SemaphoreType.DMA((2,)),
            pltpu.SemaphoreType.DMA((2, 4)),
        ],
        compiler_params=pltpu.CompilerParams(
            collective_id=0, has_side_effects=True, vmem_limit_bytes=56 << 20
        ),
    )(
        spoke_count,
        spoke_angle.reshape(1, spokes),
        block_index.T,
        kdata[:, :, 0],
        interp,
        sens_maps[:, 0],
        plane_table(side),
    )
    return pl.pallas_call(
        functools.partial(kz_kernel, parts),
        out_shape=jax.ShapeDtypeStruct((2, parts, 8, side), F32),
        in_specs=[vmem_spec, vmem_spec],
        out_specs=vmem_spec,
        scratch_shapes=[pltpu.VMEM((2, 2 * parts * 8, seg), F32)],
    )(kz_table(4, parts), gathered)


def solution(mesh):
    placed = (
        P(None, "kz", "coil", None, None),
        P(),
        P("kz"),
        P(),
        P(),
        P(None, "coil", None, None),
    )
    return jax.shard_map(
        per_device,
        mesh=mesh,
        in_specs=placed,
        out_specs=P(None, "kz", "coil", None),
        check_vma=False,
    )
```

```python
import functools

import jax
import jax.numpy as jnp
import numpy as np
from jax import lax
from jax.experimental import pallas as pl
from jax.experimental.pallas import tpu as pltpu
from jax.sharding import PartitionSpec as P

F32 = jnp.float32
BF16 = jnp.bfloat16
MESH = pl.DeviceIdType.MESH

PLAN = (('M', 0, 3), ('M', 0, 2), ('2', 3, 2), ('M', 0, 1), ('2', 3, 1), ('2', 3, 3), ('2', 1, 3), ('2', 2, 3), ('2', 0, 3), ('2', 0, 1), ('M', 0, 0), ('2', 2, 2), ('2', 3, 0), ('2', 0, 2), ('2', 2, 0), ('2', 1, 2), ('2', 0, 0), ('2', 2, 1), ('M', 1, 3), ('M', 1, 1), ('2', 6, 3), ('2', 1, 0), ('2', 1, 1), ('M', 1, 2), ('2', 7, 1), ('2', 7, 2), ('M', 1, 0), ('2', 7, 0), ('2', 4, 1), ('3', 3), ('2', 6, 2), ('3', 2), ('2', 6, 1), ('2', 5, 2), ('2', 7, 3), ('2', 5, 3), ('2', 6, 0), ('3', 1), ('3', 0), ('2', 5, 1), ('2', 4, 3), ('2', 5, 0), ('4', 2), ('4', 3), ('2', 4, 0), ('2', 4, 2), ('3', 7), ('3', 6), ('4', 1), ('4', 0), ('3', 5), ('X', 1), ('3', 4), ('4', 7), ('4', 6), ('X', 0), ('4', 5), ('4', 4), ('X', 3), ('F', 1), ('X', 2), ('F', 0), ('O', 1), ('F', 3), ('O', 0), ('F', 2), ('O', 3), ('O', 2))
BARRIER_AT = 1
BPAD = 40

STREAMS = ((True, 1), (True, 3), (False, 1), (False, 3))


def dft_np(rows, cols, length):
    product = (rows[:, None] * cols[None, :]) % length
    phase = product.astype(np.float64) * (2.0 * np.pi / length)
    return np.cos(phase) / np.sqrt(length), np.sin(phase) / np.sqrt(length)


def plane_table(side):
    index = np.arange(side)
    cos_t, sin_t = dft_np(index, index, side)
    table = np.block([[cos_t, -sin_t], [sin_t, cos_t]])
    return jnp.asarray(table, dtype=BF16)


def kz_table(groups, parts):
    total = groups * parts
    index = np.arange(total)
    cos_z, sin_z = dft_np(index, index, total)
    blocks = []
    for g in range(groups):
        c = cos_z[g * parts : (g + 1) * parts].reshape(parts, groups, 1, parts)
        s = sin_z[g * parts : (g + 1) * parts].reshape(parts, groups, 1, parts)
        real = np.concatenate([c, s], axis=2).reshape(parts, -1)
        imag = np.concatenate([-s, c], axis=2).reshape(parts, -1)
        blocks.append(np.concatenate([real, imag], axis=0))
    table = np.stack(blocks).astype(np.float32)
    high = table.astype(jnp.bfloat16)
    low = (table - high.astype(np.float32)).astype(jnp.bfloat16)
    return jnp.asarray(np.concatenate([high, low, high], axis=2))


def flip(i, pairing):
    return i + 1 - 2 * (i % 2) if pairing == 1 else 3 - i


def kernel(
    parts, angles, spokes, side,
    count_ref, angle_ref, block_ref,
    kdata_hbm, interp_hbm, sens_hbm, plane_hbm,
    out_hbm,
    kd, itp, sens_v, plane, tab, sensp, senso, binned, spread, other, half,
    img, r2x, r2y, r3, r4, xbuf, rx, gath,
    load_sem, sens_send, sens_recv, send_sem, seg_recv, recv_sem, own_send, own_recv, kz_send, kz_recv, out_sem,
):
    segs = 4
    seg = 128
    hits = angles * segs
    xpad = hits + 8
    coil = lax.axis_index("coil")
    group = lax.axis_index("kz")
    core = group % 2
    x, y, z = coil // 8, (coil // 2) % 4, coil % 2

    beside = group + 1 - 2 * core
    far = (group + 2) % 4
    sibling = (coil, beside)

    def dev(axis_x, pairing, over_z=0, over_kz=0):
        zz = 1 - z if over_z else z
        there = far if over_kz else group
        if axis_x:
            return ((flip(x, pairing) * 4 + y) * 2 + zz, there)
        return ((x * 4 + flip(y, pairing)) * 2 + zz, there)

    def zdev(over_z, over_kz):
        return ((x * 4 + y) * 2 + (1 - z if over_z else z), far if over_kz else group)

    def side_of(s):
        first_x, pairing = STREAMS[s]
        i = x if first_x else y
        return ((i + 1) // 2) % 2 if pairing == 1 else i // 2

    def part_of(s, k, mine):
        return k * 8 + s * 2 + (side_of(s) if mine else 1 - side_of(s))

    loads = [
        pltpu.make_async_copy(plane_hbm, plane, load_sem.at[0]),
        pltpu.make_async_copy(sens_hbm, sens_v, load_sem.at[1]),
    ]

    def kload(q):
        rows = pl.ds(q * (parts // 4), parts // 4)
        return pltpu.make_async_copy(kdata_hbm.at[:, rows], kd.at[:, rows], load_sem.at[2 + q])

    def iload(q):
        rows = pl.ds(q * (angles // 4), angles // 4)
        return pltpu.make_async_copy(interp_hbm.at[rows], itp.at[rows], load_sem.at[6 + q])

    for copy in loads + [kload(q) for q in range(4)] + [iload(q) for q in range(4)]:
        copy.start()

    barrier = pltpu.get_barrier_semaphore()
    turns = [(0, 0), (0, 1), (1, 0), (1, 1)]
    peers = [dev(*stream, *turn) for stream in STREAMS for turn in turns]
    peers += [zdev(*turn) for turn in turns[1:]] + [sibling]
    for peer in peers:
        pl.semaphore_signal(barrier, inc=1, device_id=peer, device_id_type=MESH)

    for copy in loads:
        copy.wait()
    row = lax.broadcasted_iota(jnp.int32, (side, side), 0)
    col = lax.broadcasted_iota(jnp.int32, (side, side), 1)
    perm = jnp.where(jnp.bitwise_xor(row, col) == coil * 8, 1.0, 0.0).astype(BF16)
    for r in range(2):
        sensp[r] = jnp.dot(perm, sens_v[r], preferred_element_type=F32)

    def sens_copy(s):
        return pltpu.make_async_remote_copy(
            src_ref=sensp.at[core], dst_ref=senso.at[s, core],
            send_sem=sens_send.at[0, s], recv_sem=sens_recv.at[0, s],
            device_id=dev(*STREAMS[s]), device_id_type=MESH,
        )

    def sens_pass(s, r):
        return pltpu.make_async_remote_copy(
            src_ref=senso.at[s, r], dst_ref=senso.at[s, r],
            send_sem=sens_send.at[1, s], recv_sem=sens_recv.at[1, s],
            device_id=sibling, device_id_type=MESH,
        )

    cos_p = jnp.dot(perm, plane[0:side, 0:side], preferred_element_type=F32).astype(BF16)
    sin_p = jnp.dot(perm, plane[side : 2 * side, 0:side], preferred_element_type=F32).astype(BF16)
    blocks = jnp.concatenate([block_ref[g : g + 1, :] for g in range(segs)], axis=1)
    blocks = jnp.broadcast_to(blocks, (side, hits))
    yrow = lax.broadcasted_iota(jnp.int32, (side, hits), 0)
    for h in range(2):
        onto = jnp.where(blocks == yrow * 2 + h, 1.0, 0.0).astype(BF16)
        cos_g = jnp.dot(cos_p, onto, preferred_element_type=F32)
        sin_g = jnp.dot(sin_p, onto, preferred_element_type=F32)
        tab[h, 0:side, 0:hits] = cos_g.astype(BF16)
        tab[h, side : 2 * side, hits : 2 * hits] = cos_g.astype(BF16)
        tab[h, 0:side, hits : 2 * hits] = sin_g.astype(BF16)
        tab[h, side : 2 * side, 0:hits] = (-sin_g).astype(BF16)

    arow = lax.broadcasted_iota(jnp.int32, (angles, spokes), 0)
    scol = lax.broadcasted_iota(jnp.int32, (angles, spokes), 1)
    match = jnp.broadcast_to(angle_ref[0:1, :], (angles, spokes)) == arow
    def bin_some(q, carry):
        kload(q).wait()
        for i in range(parts // 4):
            p = q * (parts // 4) + i
            used = jnp.logical_and(match, scol < count_ref[p])
            weights = jnp.where(used, 1.0, 0.0).astype(BF16)
            for r in range(2):
                summed = jnp.dot(weights, kd[r, p], preferred_element_type=F32)
                for g in range(segs):
                    start = g * angles * BPAD + r * parts + p
                    binned[pl.ds(start, angles, stride=BPAD), :] = summed[:, g * seg : (g + 1) * seg]
        return carry

    lax.fori_loop(0, BARRIER_AT, bin_some, 0)
    pl.semaphore_wait(barrier, len(peers))
    for s in range(4):
        sens_copy(s).start()
    lax.fori_loop(BARRIER_AT, 4, bin_some, 0)

    def spread_some(q, carry):
        iload(q).wait()
        for k in range(angles // 4):
            a = q * (angles // 4) + k
            for g in range(segs):
                start = pl.multiple_of(g * angles * BPAD + a * BPAD, 8)
                piece = binned[pl.ds(start, 2 * parts), :].astype(BF16)
                got = jnp.dot(piece, itp[a, g], preferred_element_type=F32)
                spread[pl.ds(g * angles + a, 2 * parts, stride=xpad), :] = got
        return carry

    lax.fori_loop(0, 4, spread_some, 0)

    def seg_rows(p, r):
        return pl.ds(pl.multiple_of((r * parts + p) * xpad, 8), hits)

    def seg_copy(s, k, r):
        return pltpu.make_async_remote_copy(
            src_ref=spread.at[seg_rows(part_of(s, k, False), r)], dst_ref=other.at[s, k, r],
            send_sem=send_sem.at[0, s], recv_sem=seg_recv.at[s, k, r],
            device_id=dev(*STREAMS[s]), device_id_type=MESH,
        )

    for k in range(2):
        for s in range(4):
            for r in range(2):
                seg_copy(s, k, r).start()
    for s in range(4):
        sens_copy(s).wait_recv()
        sens_pass(s, core).start()
    for s in range(4):
        sens_pass(s, 1 - core).wait_recv()

    def slots(pairing):
        return (1, 0, 1, 3) if pairing == 1 else (2, 1, 0, 1)

    def lay(s):
        first_x, pairing = STREAMS[s]
        return (first_x, 3, 2, 1, 0) if pairing == 1 else (first_x, 1, 1, 0, 1)

    def make(s, k):
        first_x, pairing = STREAMS[s]
        for r in range(2):
            seg_copy(s, k, r).wait_recv()
        p = part_of(s, k, True)
        rows = []
        for r in range(2):
            own = spread[seg_rows(p, r), :].astype(BF16)
            rows.append(jnp.concatenate([own, other[s, k, r].astype(BF16)], axis=1))
        stacked = jnp.concatenate(rows, axis=0)
        for h in range(2):
            got = jnp.dot(tab[h], stacked, preferred_element_type=F32).astype(BF16)
            for n in range(2):
                for r in range(2):
                    half[n, :, r * side + h * seg : r * side + (h + 1) * seg] = got[
                        r * side : (r + 1) * side, n * seg : (n + 1) * seg
                    ]
        mine = jnp.dot(half[0], plane[...], preferred_element_type=F32)
        theirs = jnp.dot(half[1], plane[...], preferred_element_type=F32)
        for jx in range(4):
            for jy in range(4):
                here = slice((jx * 4 + jy) * 16, (jx * 4 + jy + 1) * 16)
                there = (jx ^ pairing) * 4 + jy if first_x else jx * 4 + (jy ^ pairing)
                that = slice(there * 16, (there + 1) * 16)
                a_re, a_im = sensp[0, here, :], sensp[1, here, :]
                b_re, b_im = senso[s, 0, that, :], senso[s, 1, that, :]
                o_re, o_im = mine[here, 0:side], mine[here, side : 2 * side]
                t_re, t_im = theirs[here, 0:side], theirs[here, side : 2 * side]
                parts_of = (
                    (a_re * o_re + a_im * o_im) + (b_re * t_re + b_im * t_im),
                    (a_re * o_im - a_im * o_re) + (b_re * t_im - b_im * t_re),
                )
                for r in range(2):
                    for h in range(2):
                        img[s, k * 4 + r * 2 + h, jx, jy] = parts_of[r][:, h * seg : (h + 1) * seg]

    def copies(s, stage, c):
        first_x, second, sent2, slot0, slot_t = lay(s)
        pairing = STREAMS[s][1]
        sent, keep, onward, quarter = slots(pairing)
        if stage == 2:
            if first_x:
                return img.at[s, c, pl.ds(sent2, 2)], r2x.at[s, c], dev(True, second)
            return img.at[s, c, :, pl.ds(sent2, 2)], r2y.at[s - 2, c], dev(False, second)
        if stage == 3:
            if first_x:
                return r2x.at[s, c, :, pl.ds(sent, 2)], r3.at[s, c], dev(False, pairing)
            return r2y.at[s - 2, c, pl.ds(sent, 2)], r3.at[s, c], dev(True, pairing)
        src = r3.at[s, c, :, onward] if first_x else r3.at[s, c, onward]
        return src, r4.at[s, c], dev(not first_x, second)

    def remote(s, stage, c):
        src, dst, peer = copies(s, stage, c)
        return pltpu.make_async_remote_copy(
            src_ref=src, dst_ref=dst,
            send_sem=send_sem.at[stage - 1, s], recv_sem=recv_sem.at[stage - 2, s, c],
            device_id=peer, device_id_type=MESH,
        )

    def held(s, c, pair, quarter):
        first_x, second, sent2, slot0, slot_t = lay(s)
        j = STREAMS[s][1] if pair else 0
        slot = slot_t if pair else slot0
        if first_x:
            return img[s, c, j, quarter] + r2x[s, c, slot, quarter]
        return img[s, c, quarter, j] + r2y[s - 2, c, quarter, slot]

    def held3(s, c, pair, which, quarter):
        first_x, second, sent2, slot0, slot_t = lay(s)
        slot = slot_t if pair else slot0
        got = r3[s, c, slot, which] if first_x else r3[s, c, which, slot]
        return held(s, c, pair, quarter) + got

    def step(stage, c):
        for s in range(4):
            first_x, second, sent2, slot0, slot_t = lay(s)
            sent, keep, onward, quarter = slots(STREAMS[s][1])
            remote(s, stage - 1, c).wait_recv()
            for pair in range(2):
                slot = slot_t if pair else slot0
                if stage == 3:
                    for q in (sent, sent + 1):
                        value = held(s, c, pair, q)
                        if first_x:
                            r2x[s, c, slot, q] = value
                        else:
                            r2y[s - 2, c, q, slot] = value
                else:
                    value = held3(s, c, pair, onward, quarter)
                    if first_x:
                        r3[s, c, slot, onward] = value
                    else:
                        r3[s, c, onward, slot] = value
            remote(s, stage, c).start()

    def last_copies(kr, pair, s):
        got = []
        for jz, jk in turns:
            n = pair * 4 + jz * 2 + jk
            if n == 0:
                continue
            if pair:
                src, dst, peer = xbuf.at[1, kr, jz, s], rx.at[n, kr, s], dev(*STREAMS[s], jz, jk)
            else:
                src, dst, peer = xbuf.at[0, kr, jz], rx.at[n, kr], zdev(jz, jk)
            got.append(
                pltpu.make_async_remote_copy(
                    src_ref=src, dst_ref=dst, send_sem=own_send.at[n], recv_sem=own_recv.at[n, kr],
                    device_id=peer, device_id_type=MESH,
                )
            )
        return got

    def last(kr):
        for s in range(4):
            first_x, second, sent2, slot0, slot_t = lay(s)
            keep = slots(STREAMS[s][1])[1]
            for h in range(2):
                c = kr * 2 + h
                remote(s, 4, c).wait_recv()
                for pair in range(2):
                    slot = slot_t if pair else slot0
                    value = r4[s, c, slot] + held3(s, c, pair, keep, 0)
                    for jz in range(2):
                        xbuf[pair, kr, jz, s, h] = value[jz * 8 : (jz + 1) * 8]
            for copy in last_copies(kr, 1, s):
                copy.start()
        for copy in last_copies(kr, 0, 0):
            copy.start()

    def arrived(n, kr):
        whole = rx.at[n, kr]
        return pltpu.make_async_remote_copy(
            src_ref=whole, dst_ref=whole, send_sem=own_send.at[n], recv_sem=own_recv.at[n, kr],
            device_id=sibling, device_id_type=MESH,
        )

    def kz_remote(n, kr):
        slot = far if n else group
        where = gath.at[slot, kr % 2, :, pl.ds(kr // 2 * 8, 8)]
        return pltpu.make_async_remote_copy(
            src_ref=where, dst_ref=where,
            send_sem=kz_send.at[n], recv_sem=kz_recv.at[n, kr],
            device_id=sibling, device_id_type=MESH,
        )

    def finish(kr):
        k, r = kr // 2, kr % 2
        for n in range(1, 8):
            arrived(n, kr).wait_recv()
        for s in range(4):
            for h in range(2):
                gath[group, r, h, part_of(s, k, True)] = xbuf[0, kr, 0, s, h] + rx[2, kr, s, h]
                gath[group, r, h, part_of(s, k, False)] = rx[4, kr, s, h] + rx[6, kr, s, h]
                gath[far, r, h, part_of(s, k, True)] = rx[1, kr, s, h] + rx[3, kr, s, h]
                gath[far, r, h, part_of(s, k, False)] = rx[5, kr, s, h] + rx[7, kr, s, h]
        for n in range(2):
            kz_remote(n, kr).start()

    def out_copy(kr):
        rows = (slice(None), kr % 2, slice(None), pl.ds(kr // 2 * 8, 8))
        return pltpu.make_async_copy(gath.at[rows], out_hbm.at[rows], out_sem.at[kr])

    def put(kr):
        for n in range(2):
            kz_remote(n, kr).wait_recv()
        out_copy(kr).start()

    for what, *where in PLAN:
        if what == "M":
            make(where[1], where[0])
        elif what == "2":
            remote(where[1], 2, where[0]).start()
        elif what == "X":
            last(*where)
        elif what == "F":
            finish(*where)
        elif what == "O":
            put(*where)
        else:
            step(int(what), *where)

    def sent_all(ref, sem, unused, peer):
        pltpu.make_async_remote_copy(
            src_ref=ref, dst_ref=ref, send_sem=sem, recv_sem=unused, device_id=peer, device_id_type=MESH
        ).wait_send()

    everything = pl.ds(0, 8)
    for s in range(4):
        sens_copy(s).wait_send()
        sens_pass(s, core).wait_send()
        sent_all(other.at[s], send_sem.at[0, s], seg_recv.at[s, 0, 0], sibling)
        for stage in range(2, 5):
            src, dst, peer = copies(s, stage, everything)
            sent_all(src, send_sem.at[stage - 1, s], recv_sem.at[stage - 2, s, 0], peer)
    for n in range(1, 8):
        sent_all(rx.at[n], own_send.at[n], own_recv.at[n, 0], sibling)
    for n in range(2):
        sent_all(gath.at[group], kz_send.at[n], kz_recv.at[n, 0], sibling)
    for kr in range(4):
        out_copy(kr).wait()


def kz_kernel(parts, ztab_ref, gath, out_ref, kzout):
    group = lax.axis_index("kz")
    for yy in range(8):
        pieces = [gath[g, r, 0, :, yy, :] for g in range(4) for r in range(2)]
        stacked = jnp.concatenate(pieces, axis=0)
        high = stacked.astype(BF16)
        low = (stacked - high.astype(F32)).astype(BF16)
        got = jnp.dot(
            ztab_ref[group], jnp.concatenate([high, high, low], axis=0), preferred_element_type=F32
        )
        kzout[pl.ds(yy, 2 * parts, stride=8), :] = got
    out_ref[...] = kzout[...].reshape(2, parts, 8, kzout.shape[1])


def per_device(kdata, spoke_angle, spoke_count, block_index, interp, sens_maps):
    side = sens_maps.shape[2]
    parts = kdata.shape[1]
    spokes, samples = kdata.shape[3], kdata.shape[4]
    angles, segs, seg = interp.shape[0], interp.shape[1], interp.shape[2]
    hits = angles * segs
    any_spec = pl.BlockSpec(memory_space=pl.ANY)
    vmem_spec = pl.BlockSpec(memory_space=pltpu.VMEM)
    gathered = pl.pallas_call(
        functools.partial(kernel, parts, angles, spokes, side),
        out_shape=jax.ShapeDtypeStruct((4, 2, 2, parts, 8, seg), F32),
        in_specs=[pl.BlockSpec(memory_space=pltpu.SMEM)] + [vmem_spec] * 2 + [any_spec] * 4,
        out_specs=any_spec,
        scratch_shapes=[
            pltpu.VMEM((2, parts, spokes, samples), BF16),
            pltpu.VMEM((angles, segs, seg, seg), BF16),
            pltpu.VMEM((2, side, side), BF16),
            pltpu.VMEM((2 * side, 2 * side), BF16),
            pltpu.VMEM((2, 2 * side, 2 * hits), BF16),
            pltpu.VMEM((2, side, side), F32),
            pltpu.VMEM((4, 2, side, side), F32),
            pltpu.VMEM((segs * angles * BPAD, seg), F32),
            pltpu.VMEM((2 * parts * (hits + 8), seg), F32),
            pltpu.VMEM((4, 2, 2, hits, seg), F32),
            pltpu.VMEM((2, side, 2 * side), BF16),
            pltpu.VMEM((4, 8, 4, 4, 16, seg), F32),
            pltpu.VMEM((2, 8, 2, 4, 16, seg), F32),
            pltpu.VMEM((2, 8, 4, 2, 16, seg), F32),
            pltpu.VMEM((4, 8, 2, 2, 16, seg), F32),
            pltpu.VMEM((4, 8, 2, 16, seg), F32),
            pltpu.VMEM((2, 4, 2, 4, 2, 8, seg), F32),
            pltpu.VMEM((8, 4, 4, 2, 8, seg), F32),
            pltpu.VMEM((4, 2, 2, parts, 8, seg), F32),
            pltpu.SemaphoreType.DMA((10,)),
            pltpu.SemaphoreType.DMA((2, 4)),
            pltpu.SemaphoreType.DMA((2, 4)),
            pltpu.SemaphoreType.DMA((4, 4)),
            pltpu.SemaphoreType.DMA((4, 2, 2)),
            pltpu.SemaphoreType.DMA((3, 4, 8)),
            pltpu.SemaphoreType.DMA((8,)),
            pltpu.SemaphoreType.DMA((8, 4)),
            pltpu.SemaphoreType.DMA((2,)),
            pltpu.SemaphoreType.DMA((2, 4)),
            pltpu.SemaphoreType.DMA((4,)),
        ],
        compiler_params=pltpu.CompilerParams(
            collective_id=0, has_side_effects=True, vmem_limit_bytes=56 << 20
        ),
    )(
        spoke_count,
        spoke_angle.reshape(1, spokes),
        block_index.T,
        kdata[:, :, 0],
        interp,
        sens_maps[:, 0],
        plane_table(side),
    )
    return pl.pallas_call(
        functools.partial(kz_kernel, parts),
        grid=(2,),
        out_shape=jax.ShapeDtypeStruct((2, parts, 8, side), F32),
        in_specs=[
            pl.BlockSpec((4, 2 * parts, 24 * parts), lambda h: (0, 0, 0)),
            pl.BlockSpec((4, 2, 1, parts, 8, seg), lambda h: (0, 0, h, 0, 0, 0)),
        ],
        out_specs=pl.BlockSpec((2, parts, 8, seg), lambda h: (0, 0, 0, h)),
        scratch_shapes=[pltpu.VMEM((2 * parts * 8, seg), F32)],
    )(kz_table(4, parts), gathered)


def solution(mesh):
    placed = (
        P(None, "kz", "coil", None, None),
        P(),
        P("kz"),
        P(),
        P(),
        P(None, "coil", None, None),
    )
    return jax.shard_map(
        per_device,
        mesh=mesh,
        in_specs=placed,
        out_specs=P(None, "kz", "coil", None),
        check_vma=False,
    )
```

```python
import functools

import jax
import jax.numpy as jnp
import numpy as np
from jax import lax
from jax.experimental import pallas as pl
from jax.experimental.pallas import tpu as pltpu
from jax.sharding import PartitionSpec as P

F32 = jnp.float32
BF16 = jnp.bfloat16
MESH = pl.DeviceIdType.MESH

PLAN = (('M', 0, 2), ('M', 0, 1), ('M', 0, 3), ('2', 1, 2), ('2', 0, 3), ('2', 0, 1), ('M', 0, 0), ('2', 1, 1), ('2', 3, 0), ('2', 1, 3), ('2', 2, 1), ('2', 0, 2), ('2', 3, 1), ('2', 2, 2), ('2', 2, 3), ('2', 0, 0), ('2', 3, 2), ('2', 1, 0), ('M', 1, 2), ('2', 7, 2), ('M', 1, 3), ('2', 2, 0), ('2', 4, 3), ('M', 1, 1), ('2', 3, 3), ('M', 1, 0), ('2', 5, 0), ('2', 6, 1), ('3', 0), ('2', 5, 2), ('2', 5, 3), ('3', 1), ('2', 4, 1), ('2', 4, 2), ('2', 5, 1), ('2', 4, 0), ('2', 6, 0), ('2', 6, 3), ('3', 2), ('3', 3), ('4', 0), ('2', 7, 3), ('2', 7, 0), ('2', 6, 2), ('4', 1), ('2', 7, 1), ('3', 5), ('3', 4), ('4', 3), ('4', 2), ('3', 6), ('X', 0), ('3', 7), ('4', 5), ('4', 4), ('X', 1), ('4', 6), ('4', 7), ('X', 2), ('X', 3), ('F', 0), ('F', 1), ('O', 0), ('F', 2), ('O', 1), ('F', 3), ('O', 2), ('O', 3))
BARRIER_AT = 1
BPAD = 40

STREAMS = ((True, 1), (True, 3), (False, 1), (False, 3))


def dft_np(rows, cols, length):
    product = (rows[:, None] * cols[None, :]) % length
    phase = product.astype(np.float64) * (2.0 * np.pi / length)
    return np.cos(phase) / np.sqrt(length), np.sin(phase) / np.sqrt(length)


def plane_table(side):
    index = np.arange(side)
    cos_t, sin_t = dft_np(index, index, side)
    table = np.block([[cos_t, -sin_t], [sin_t, cos_t]])
    return jnp.asarray(table, dtype=BF16)


def kz_table(groups, parts):
    total = groups * parts
    index = np.arange(total)
    cos_z, sin_z = dft_np(index, index, total)
    blocks = []
    for g in range(groups):
        c = cos_z[g * parts : (g + 1) * parts].reshape(parts, groups, 1, parts)
        s = sin_z[g * parts : (g + 1) * parts].reshape(parts, groups, 1, parts)
        real = np.concatenate([c, s], axis=2).reshape(parts, -1)
        imag = np.concatenate([-s, c], axis=2).reshape(parts, -1)
        blocks.append(np.concatenate([real, imag], axis=0))
    table = np.stack(blocks).astype(np.float32).reshape(groups, 2 * parts, groups, 2, 2, parts // 2)
    table = table.transpose(0, 4, 3, 1, 2, 5).reshape(groups, 4, 2 * parts, groups * (parts // 2))
    high = table.astype(jnp.bfloat16)
    low = (table - high.astype(np.float32)).astype(jnp.bfloat16)
    return jnp.asarray(np.concatenate([high, low, high], axis=3))


def flip(i, pairing):
    return i + 1 - 2 * (i % 2) if pairing == 1 else 3 - i


def kernel(
    parts, angles, spokes, side,
    count_ref, angle_ref, block_ref, ztab_ref,
    kdata_hbm, interp_hbm, sens_hbm, plane_hbm,
    out_ref,
    kd, itp, sens_v, plane, tab, sensp, senso, binned, spread, other, half,
    img, r2x, r2y, r3, r4, xbuf, rx, gath, total, kzout,
    load_sem, sens_send, sens_recv, send_sem, seg_recv, recv_sem, own_send, own_recv, kz_send, kz_recv,
):
    segs = 4
    seg = 128
    hits = angles * segs
    xpad = hits + 8
    coil = lax.axis_index("coil")
    group = lax.axis_index("kz")
    core = group % 2
    x, y, z = coil // 8, (coil // 2) % 4, coil % 2

    beside = group + 1 - 2 * core
    far = (group + 2) % 4
    sibling = (coil, beside)

    def dev(axis_x, pairing, over_z=0, over_kz=0):
        zz = 1 - z if over_z else z
        there = far if over_kz else group
        if axis_x:
            return ((flip(x, pairing) * 4 + y) * 2 + zz, there)
        return ((x * 4 + flip(y, pairing)) * 2 + zz, there)

    def zdev(over_z, over_kz):
        return ((x * 4 + y) * 2 + (1 - z if over_z else z), far if over_kz else group)

    def side_of(s):
        first_x, pairing = STREAMS[s]
        i = x if first_x else y
        return ((i + 1) // 2) % 2 if pairing == 1 else i // 2

    def part_of(s, k, mine):
        return k * 8 + s * 2 + (side_of(s) if mine else 1 - side_of(s))

    loads = [
        pltpu.make_async_copy(plane_hbm, plane, load_sem.at[0]),
        pltpu.make_async_copy(sens_hbm, sens_v, load_sem.at[1]),
    ]

    def kload(q):
        rows = pl.ds(q * (parts // 4), parts // 4)
        return pltpu.make_async_copy(kdata_hbm.at[:, rows], kd.at[:, rows], load_sem.at[2 + q])

    def iload(q):
        rows = pl.ds(q * (angles // 4), angles // 4)
        return pltpu.make_async_copy(interp_hbm.at[rows], itp.at[rows], load_sem.at[6 + q])

    for copy in loads + [kload(q) for q in range(4)] + [iload(q) for q in range(4)]:
        copy.start()

    barrier = pltpu.get_barrier_semaphore()
    turns = [(0, 0), (0, 1), (1, 0), (1, 1)]
    peers = [dev(*stream, *turn) for stream in STREAMS for turn in turns]
    peers += [zdev(*turn) for turn in turns[1:]] + [sibling]
    for peer in peers:
        pl.semaphore_signal(barrier, inc=1, device_id=peer, device_id_type=MESH)

    for copy in loads:
        copy.wait()
    row = lax.broadcasted_iota(jnp.int32, (side, side), 0)
    col = lax.broadcasted_iota(jnp.int32, (side, side), 1)
    perm = jnp.where(jnp.bitwise_xor(row, col) == coil * 8, 1.0, 0.0).astype(BF16)
    for r in range(2):
        sensp[r] = jnp.dot(perm, sens_v[r], preferred_element_type=F32)

    def sens_copy(s):
        return pltpu.make_async_remote_copy(
            src_ref=sensp.at[core], dst_ref=senso.at[s, core],
            send_sem=sens_send.at[0, s], recv_sem=sens_recv.at[0, s],
            device_id=dev(*STREAMS[s]), device_id_type=MESH,
        )

    def sens_pass(s, r):
        return pltpu.make_async_remote_copy(
            src_ref=senso.at[s, r], dst_ref=senso.at[s, r],
            send_sem=sens_send.at[1, s], recv_sem=sens_recv.at[1, s],
            device_id=sibling, device_id_type=MESH,
        )

    cos_p = jnp.dot(perm, plane[0:side, 0:side], preferred_element_type=F32).astype(BF16)
    sin_p = jnp.dot(perm, plane[side : 2 * side, 0:side], preferred_element_type=F32).astype(BF16)
    blocks = jnp.concatenate([block_ref[g : g + 1, :] for g in range(segs)], axis=1)
    blocks = jnp.broadcast_to(blocks, (side, hits))
    yrow = lax.broadcasted_iota(jnp.int32, (side, hits), 0)
    for h in range(2):
        onto = jnp.where(blocks == yrow * 2 + h, 1.0, 0.0).astype(BF16)
        cos_g = jnp.dot(cos_p, onto, preferred_element_type=F32)
        sin_g = jnp.dot(sin_p, onto, preferred_element_type=F32)
        tab[h, 0:side, 0:hits] = cos_g.astype(BF16)
        tab[h, side : 2 * side, hits : 2 * hits] = cos_g.astype(BF16)
        tab[h, 0:side, hits : 2 * hits] = sin_g.astype(BF16)
        tab[h, side : 2 * side, 0:hits] = (-sin_g).astype(BF16)

    arow = lax.broadcasted_iota(jnp.int32, (angles, spokes), 0)
    scol = lax.broadcasted_iota(jnp.int32, (angles, spokes), 1)
    match = jnp.broadcast_to(angle_ref[0:1, :], (angles, spokes)) == arow
    def bin_some(q, carry):
        kload(q).wait()
        for i in range(parts // 4):
            p = q * (parts // 4) + i
            used = jnp.logical_and(match, scol < count_ref[p])
            weights = jnp.where(used, 1.0, 0.0).astype(BF16)
            for r in range(2):
                summed = jnp.dot(weights, kd[r, p], preferred_element_type=F32)
                for g in range(segs):
                    start = g * angles * BPAD + r * parts + p
                    binned[pl.ds(start, angles, stride=BPAD), :] = summed[:, g * seg : (g + 1) * seg]
        return carry

    lax.fori_loop(0, BARRIER_AT, bin_some, 0)
    pl.semaphore_wait(barrier, len(peers))
    for s in range(4):
        sens_copy(s).start()
    lax.fori_loop(BARRIER_AT, 4, bin_some, 0)

    def spread_some(q, carry):
        iload(q).wait()
        for k in range(angles // 4):
            a = q * (angles // 4) + k
            for g in range(segs):
                start = pl.multiple_of(g * angles * BPAD + a * BPAD, 8)
                piece = binned[pl.ds(start, 2 * parts), :].astype(BF16)
                got = jnp.dot(piece, itp[a, g], preferred_element_type=F32)
                spread[pl.ds(g * angles + a, 2 * parts, stride=xpad), :] = got
        return carry

    lax.fori_loop(0, 4, spread_some, 0)

    def seg_rows(p, r):
        return pl.ds(pl.multiple_of((r * parts + p) * xpad, 8), hits)

    def seg_copy(s, k, r):
        return pltpu.make_async_remote_copy(
            src_ref=spread.at[seg_rows(part_of(s, k, False), r)], dst_ref=other.at[s, k, r],
            send_sem=send_sem.at[0, s], recv_sem=seg_recv.at[s, k, r],
            device_id=dev(*STREAMS[s]), device_id_type=MESH,
        )

    for k in range(2):
        for s in range(4):
            for r in range(2):
                seg_copy(s, k, r).start()
    for s in range(4):
        sens_copy(s).wait_recv()
        sens_pass(s, core).start()
    for s in range(4):
        sens_pass(s, 1 - core).wait_recv()

    def slots(pairing):
        return (1, 0, 1, 3) if pairing == 1 else (2, 1, 0, 1)

    def lay(s):
        first_x, pairing = STREAMS[s]
        return (first_x, 3, 2, 1, 0) if pairing == 1 else (first_x, 1, 1, 0, 1)

    def make(s, k):
        first_x, pairing = STREAMS[s]
        for r in range(2):
            seg_copy(s, k, r).wait_recv()
        p = part_of(s, k, True)
        rows = []
        for r in range(2):
            own = spread[seg_rows(p, r), :].astype(BF16)
            rows.append(jnp.concatenate([own, other[s, k, r].astype(BF16)], axis=1))
        stacked = jnp.concatenate(rows, axis=0)
        for h in range(2):
            got = jnp.dot(tab[h], stacked, preferred_element_type=F32).astype(BF16)
            for n in range(2):
                for r in range(2):
                    half[n, :, r * side + h * seg : r * side + (h + 1) * seg] = got[
                        r * side : (r + 1) * side, n * seg : (n + 1) * seg
                    ]
        mine = jnp.dot(half[0], plane[...], preferred_element_type=F32)
        theirs = jnp.dot(half[1], plane[...], preferred_element_type=F32)
        for jx in range(4):
            for jy in range(4):
                here = slice((jx * 4 + jy) * 16, (jx * 4 + jy + 1) * 16)
                there = (jx ^ pairing) * 4 + jy if first_x else jx * 4 + (jy ^ pairing)
                that = slice(there * 16, (there + 1) * 16)
                a_re, a_im = sensp[0, here, :], sensp[1, here, :]
                b_re, b_im = senso[s, 0, that, :], senso[s, 1, that, :]
                o_re, o_im = mine[here, 0:side], mine[here, side : 2 * side]
                t_re, t_im = theirs[here, 0:side], theirs[here, side : 2 * side]
                parts_of = (
                    (a_re * o_re + a_im * o_im) + (b_re * t_re + b_im * t_im),
                    (a_re * o_im - a_im * o_re) + (b_re * t_im - b_im * t_re),
                )
                for r in range(2):
                    for h in range(2):
                        img[s, k * 4 + r * 2 + h, jx, jy] = parts_of[r][:, h * seg : (h + 1) * seg]

    def copies(s, stage, c):
        first_x, second, sent2, slot0, slot_t = lay(s)
        pairing = STREAMS[s][1]
        sent, keep, onward, quarter = slots(pairing)
        if stage == 2:
            if first_x:
                return img.at[s, c, pl.ds(sent2, 2)], r2x.at[s, c], dev(True, second)
            return img.at[s, c, :, pl.ds(sent2, 2)], r2y.at[s - 2, c], dev(False, second)
        if stage == 3:
            if first_x:
                return r2x.at[s, c, :, pl.ds(sent, 2)], r3.at[s, c], dev(False, pairing)
            return r2y.at[s - 2, c, pl.ds(sent, 2)], r3.at[s, c], dev(True, pairing)
        src = r3.at[s, c, :, onward] if first_x else r3.at[s, c, onward]
        return src, r4.at[s, c], dev(not first_x, second)

    def remote(s, stage, c):
        src, dst, peer = copies(s, stage, c)
        return pltpu.make_async_remote_copy(
            src_ref=src, dst_ref=dst,
            send_sem=send_sem.at[stage - 1, s], recv_sem=recv_sem.at[stage - 2, s, c],
            device_id=peer, device_id_type=MESH,
        )

    def held(s, c, pair, quarter):
        first_x, second, sent2, slot0, slot_t = lay(s)
        j = STREAMS[s][1] if pair else 0
        slot = slot_t if pair else slot0
        if first_x:
            return img[s, c, j, quarter] + r2x[s, c, slot, quarter]
        return img[s, c, quarter, j] + r2y[s - 2, c, quarter, slot]

    def held3(s, c, pair, which, quarter):
        first_x, second, sent2, slot0, slot_t = lay(s)
        slot = slot_t if pair else slot0
        got = r3[s, c, slot, which] if first_x else r3[s, c, which, slot]
        return held(s, c, pair, quarter) + got

    def step(stage, c):
        for s in range(4):
            first_x, second, sent2, slot0, slot_t = lay(s)
            sent, keep, onward, quarter = slots(STREAMS[s][1])
            remote(s, stage - 1, c).wait_recv()
            for pair in range(2):
                slot = slot_t if pair else slot0
                if stage == 3:
                    for q in (sent, sent + 1):
                        value = held(s, c, pair, q)
                        if first_x:
                            r2x[s, c, slot, q] = value
                        else:
                            r2y[s - 2, c, q, slot] = value
                else:
                    value = held3(s, c, pair, onward, quarter)
                    if first_x:
                        r3[s, c, slot, onward] = value
                    else:
                        r3[s, c, onward, slot] = value
            remote(s, stage, c).start()

    def last_copies(kr, pair, s):
        got = []
        for jz, jk in turns:
            n = pair * 4 + jz * 2 + jk
            if n == 0:
                continue
            if pair:
                src, dst, peer = xbuf.at[1, kr, jz, s], rx.at[n, kr, s], dev(*STREAMS[s], jz, jk)
            else:
                src, dst, peer = xbuf.at[0, kr, jz], rx.at[n, kr], zdev(jz, jk)
            got.append(
                pltpu.make_async_remote_copy(
                    src_ref=src, dst_ref=dst, send_sem=own_send.at[n], recv_sem=own_recv.at[n, kr],
                    device_id=peer, device_id_type=MESH,
                )
            )
        return got

    def last(kr):
        for s in range(4):
            first_x, second, sent2, slot0, slot_t = lay(s)
            keep = slots(STREAMS[s][1])[1]
            for h in range(2):
                c = kr * 2 + h
                remote(s, 4, c).wait_recv()
                for pair in range(2):
                    slot = slot_t if pair else slot0
                    value = r4[s, c, slot] + held3(s, c, pair, keep, 0)
                    for jz in range(2):
                        xbuf[pair, kr, jz, s, h] = value[jz * 8 : (jz + 1) * 8]
            for copy in last_copies(kr, 1, s):
                copy.start()
        for copy in last_copies(kr, 0, 0):
            copy.start()

    def arrived(n, kr):
        whole = rx.at[n, kr]
        return pltpu.make_async_remote_copy(
            src_ref=whole, dst_ref=whole, send_sem=own_send.at[n], recv_sem=own_recv.at[n, kr],
            device_id=sibling, device_id_type=MESH,
        )

    def gath_rows(slot, kr):
        return pl.ds(pl.multiple_of((slot * 4 + kr) * 128, 128), 128)

    def kz_remote(n, kr):
        where = gath.at[gath_rows(far if n else group, kr)]
        return pltpu.make_async_remote_copy(
            src_ref=where, dst_ref=where,
            send_sem=kz_send.at[n], recv_sem=kz_recv.at[n, kr],
            device_id=sibling, device_id_type=MESH,
        )

    def finish(kr):
        for n in range(1, 8):
            arrived(n, kr).wait_recv()
        for s in range(4):
            for h in range(2):
                for slot, mine, value in (
                    (group, True, xbuf[0, kr, 0, s, h] + rx[2, kr, s, h]),
                    (group, False, rx[4, kr, s, h] + rx[6, kr, s, h]),
                    (far, True, rx[1, kr, s, h] + rx[3, kr, s, h]),
                    (far, False, rx[5, kr, s, h] + rx[7, kr, s, h]),
                ):
                    start = (slot * 4 + kr) * 128 + h * 64 + part_of(s, 0, mine)
                    gath[pl.ds(start, 8, stride=8), :] = value
        for n in range(2):
            kz_remote(n, kr).start()

    def put(kr, first, last_one):
        for n in range(2):
            kz_remote(n, kr).wait_recv()
        for h in range(2):
            rows = []
            for g in range(4):
                base = (g * 4 + kr) * 128 + h * 64
                rows.append(jnp.concatenate([gath[base + yy * 8 : base + yy * 8 + 8, :] for yy in range(8)], axis=1))
            stacked = jnp.concatenate(rows, axis=0)
            high = stacked.astype(BF16)
            low = (stacked - high.astype(F32)).astype(BF16)
            got = jnp.dot(
                ztab_ref[group, kr], jnp.concatenate([high, high, low], axis=0), preferred_element_type=F32
            )
            if not first:
                got = got + total[h]
            if not last_one:
                total[h] = got
                continue
            for yy in range(8):
                kzout[h, pl.ds(yy, 2 * parts, stride=8), :] = got[:, yy * seg : (yy + 1) * seg]
            out_ref[:, :, :, h * seg : (h + 1) * seg] = kzout[h].reshape(2, parts, 8, seg)

    begun = [what for what, *where in PLAN].index("O")
    for n, (what, *where) in enumerate(PLAN):
        if what == "M":
            make(where[1], where[0])
        elif what == "2":
            remote(where[1], 2, where[0]).start()
        elif what == "X":
            last(*where)
        elif what == "F":
            finish(*where)
        elif what == "O":
            put(*where, n == begun, n == len(PLAN) - 1)
        else:
            step(int(what), *where)

    def sent_all(ref, sem, unused, peer):
        pltpu.make_async_remote_copy(
            src_ref=ref, dst_ref=ref, send_sem=sem, recv_sem=unused, device_id=peer, device_id_type=MESH
        ).wait_send()

    everything = pl.ds(0, 8)
    for s in range(4):
        sens_copy(s).wait_send()
        sens_pass(s, core).wait_send()
        sent_all(other.at[s], send_sem.at[0, s], seg_recv.at[s, 0, 0], sibling)
        for stage in range(2, 5):
            src, dst, peer = copies(s, stage, everything)
            sent_all(src, send_sem.at[stage - 1, s], recv_sem.at[stage - 2, s, 0], peer)
    for n in range(1, 8):
        sent_all(rx.at[n], own_send.at[n], own_recv.at[n, 0], sibling)
    for n in range(2):
        sent_all(gath.at[pl.ds(0, 512)], kz_send.at[n], kz_recv.at[n, 0], sibling)


def per_device(kdata, spoke_angle, spoke_count, block_index, interp, sens_maps):
    side = sens_maps.shape[2]
    parts = kdata.shape[1]
    spokes, samples = kdata.shape[3], kdata.shape[4]
    angles, segs, seg = interp.shape[0], interp.shape[1], interp.shape[2]
    hits = angles * segs
    any_spec = pl.BlockSpec(memory_space=pl.ANY)
    vmem_spec = pl.BlockSpec(memory_space=pltpu.VMEM)
    return pl.pallas_call(
        functools.partial(kernel, parts, angles, spokes, side),
        out_shape=jax.ShapeDtypeStruct((2, parts, 8, side), F32),
        in_specs=[pl.BlockSpec(memory_space=pltpu.SMEM)] + [vmem_spec] * 3 + [any_spec] * 4,
        out_specs=vmem_spec,
        scratch_shapes=[
            pltpu.VMEM((2, parts, spokes, samples), BF16),
            pltpu.VMEM((angles, segs, seg, seg), BF16),
            pltpu.VMEM((2, side, side), BF16),
            pltpu.VMEM((2 * side, 2 * side), BF16),
            pltpu.VMEM((2, 2 * side, 2 * hits), BF16),
            pltpu.VMEM((2, side, side), F32),
            pltpu.VMEM((4, 2, side, side), F32),
            pltpu.VMEM((segs * angles * BPAD, seg), F32),
            pltpu.VMEM((2 * parts * (hits + 8), seg), F32),
            pltpu.VMEM((4, 2, 2, hits, seg), F32),
            pltpu.VMEM((2, side, 2 * side), BF16),
            pltpu.VMEM((4, 8, 4, 4, 16, seg), F32),
            pltpu.VMEM((2, 8, 2, 4, 16, seg), F32),
            pltpu.VMEM((2, 8, 4, 2, 16, seg), F32),
            pltpu.VMEM((4, 8, 2, 2, 16, seg), F32),
            pltpu.VMEM((4, 8, 2, 16, seg), F32),
            pltpu.VMEM((2, 4, 2, 4, 2, 8, seg), F32),
            pltpu.VMEM((8, 4, 4, 2, 8, seg), F32),
            pltpu.VMEM((4 * 4 * 128, seg), F32),
            pltpu.VMEM((2, 2 * parts, 8 * seg), F32),
            pltpu.VMEM((2, 2 * parts * 8, seg), F32),
            pltpu.SemaphoreType.DMA((10,)),
            pltpu.SemaphoreType.DMA((2, 4)),
            pltpu.SemaphoreType.DMA((2, 4)),
            pltpu.SemaphoreType.DMA((4, 4)),
            pltpu.SemaphoreType.DMA((4, 2, 2)),
            pltpu.SemaphoreType.DMA((3, 4, 8)),
            pltpu.SemaphoreType.DMA((8,)),
            pltpu.SemaphoreType.DMA((8, 4)),
            pltpu.SemaphoreType.DMA((2,)),
            pltpu.SemaphoreType.DMA((2, 4)),
        ],
        compiler_params=pltpu.CompilerParams(
            collective_id=0, has_side_effects=True, vmem_limit_bytes=56 << 20
        ),
    )(
        spoke_count,
        spoke_angle.reshape(1, spokes),
        block_index.T,
        kz_table(4, parts),
        kdata[:, :, 0],
        interp,
        sens_maps[:, 0],
        plane_table(side),
    )

def solution(mesh):
    placed = (
        P(None, "kz", "coil", None, None),
        P(),
        P("kz"),
        P(),
        P(),
        P(None, "coil", None, None),
    )
    return jax.shard_map(
        per_device,
        mesh=mesh,
        in_specs=placed,
        out_specs=P(None, "kz", "coil", None),
        check_vma=False,
    )
```

```python
import functools

import jax
import jax.numpy as jnp
import numpy as np
from jax import lax
from jax.experimental import pallas as pl
from jax.experimental.pallas import tpu as pltpu
from jax.sharding import PartitionSpec as P

F32 = jnp.float32
BF16 = jnp.bfloat16
MESH = pl.DeviceIdType.MESH

PLAN = (('M', 0, 2), ('M', 0, 1), ('M', 0, 3), ('2', 1, 2), ('2', 0, 3), ('2', 0, 1), ('M', 0, 0), ('2', 1, 1), ('2', 3, 0), ('2', 1, 3), ('2', 2, 1), ('2', 0, 2), ('2', 3, 1), ('2', 2, 2), ('2', 2, 3), ('2', 0, 0), ('2', 3, 2), ('2', 1, 0), ('M', 1, 2), ('2', 7, 2), ('M', 1, 3), ('2', 2, 0), ('2', 4, 3), ('M', 1, 1), ('2', 3, 3), ('M', 1, 0), ('2', 5, 0), ('2', 6, 1), ('3', 0), ('2', 5, 2), ('2', 5, 3), ('3', 1), ('2', 4, 1), ('2', 4, 2), ('2', 5, 1), ('2', 4, 0), ('2', 6, 0), ('2', 6, 3), ('3', 2), ('3', 3), ('4', 0), ('2', 7, 3), ('2', 7, 0), ('2', 6, 2), ('4', 1), ('2', 7, 1), ('3', 5), ('3', 4), ('4', 3), ('4', 2), ('3', 6), ('X', 0), ('3', 7), ('4', 5), ('4', 4), ('X', 1), ('4', 6), ('4', 7), ('X', 2), ('X', 3), ('F', 0), ('F', 1), ('O', 0), ('F', 2), ('O', 1), ('F', 3), ('O', 2), ('O', 3))
BARRIER_AT = 0
BPAD = 40

STREAMS = ((True, 1), (True, 3), (False, 1), (False, 3))


def dft_np(rows, cols, length):
    product = (rows[:, None] * cols[None, :]) % length
    phase = product.astype(np.float64) * (2.0 * np.pi / length)
    return np.cos(phase) / np.sqrt(length), np.sin(phase) / np.sqrt(length)


def plane_table(side):
    index = np.arange(side)
    cos_t, sin_t = dft_np(index, index, side)
    table = np.block([[cos_t, -sin_t], [sin_t, cos_t]])
    return jnp.asarray(table, dtype=BF16)


def kz_table(groups, parts):
    total = groups * parts
    index = np.arange(total)
    cos_z, sin_z = dft_np(index, index, total)
    blocks = []
    for g in range(groups):
        c = cos_z[g * parts : (g + 1) * parts].reshape(parts, groups, 1, parts)
        s = sin_z[g * parts : (g + 1) * parts].reshape(parts, groups, 1, parts)
        real = np.concatenate([c, s], axis=2).reshape(parts, -1)
        imag = np.concatenate([-s, c], axis=2).reshape(parts, -1)
        blocks.append(np.concatenate([real, imag], axis=0))
    table = np.stack(blocks).astype(np.float32).reshape(groups, 2 * parts, groups, 2, 2, parts // 2)
    table = table.transpose(0, 4, 3, 1, 2, 5).reshape(groups, 4, 2 * parts, groups * (parts // 2))
    high = table.astype(jnp.bfloat16)
    low = (table - high.astype(np.float32)).astype(jnp.bfloat16)
    return jnp.asarray(np.concatenate([high, low, high], axis=3))


def flip(i, pairing):
    return i + 1 - 2 * (i % 2) if pairing == 1 else 3 - i


def kernel(
    parts, angles, spokes, side,
    count_ref, angle_ref, block_ref, ztab_ref,
    kdata_hbm, interp_hbm, sens_hbm, plane_hbm,
    out_ref,
    kd, itp, sens_v, plane, tab, sensp, senso, binned, spread, other, half,
    img, r2x, r2y, r3, r4, xbuf, rx, gath, total, kzout,
    load_sem, sens_send, sens_recv, send_sem, seg_recv, recv_sem, own_send, own_recv, kz_send, kz_recv, round_sem,
):
    segs = 4
    seg = 128
    hits = angles * segs
    xpad = hits + 8
    coil = lax.axis_index("coil")
    group = lax.axis_index("kz")
    core = group % 2
    x, y, z = coil // 8, (coil // 2) % 4, coil % 2

    beside = group + 1 - 2 * core
    far = (group + 2) % 4
    sibling = (coil, beside)

    def dev(axis_x, pairing, over_z=0, over_kz=0):
        zz = 1 - z if over_z else z
        there = far if over_kz else group
        if axis_x:
            return ((flip(x, pairing) * 4 + y) * 2 + zz, there)
        return ((x * 4 + flip(y, pairing)) * 2 + zz, there)

    def zdev(over_z, over_kz):
        return ((x * 4 + y) * 2 + (1 - z if over_z else z), far if over_kz else group)

    def side_of(s):
        first_x, pairing = STREAMS[s]
        i = x if first_x else y
        return ((i + 1) // 2) % 2 if pairing == 1 else i // 2

    def part_of(s, k, mine):
        return k * 8 + s * 2 + (side_of(s) if mine else 1 - side_of(s))

    loads = [
        pltpu.make_async_copy(plane_hbm, plane, load_sem.at[0]),
        pltpu.make_async_copy(sens_hbm, sens_v, load_sem.at[1]),
    ]

    def kload(q):
        rows = pl.ds(q * (parts // 4), parts // 4)
        return pltpu.make_async_copy(kdata_hbm.at[:, rows], kd.at[:, rows], load_sem.at[2 + q])

    def iload(q):
        rows = pl.ds(q * (angles // 4), angles // 4)
        return pltpu.make_async_copy(interp_hbm.at[rows], itp.at[rows], load_sem.at[6 + q])

    for copy in loads + [kload(q) for q in range(4)] + [iload(q) for q in range(4)]:
        copy.start()

    barrier = pltpu.get_barrier_semaphore()
    turns = [(0, 0), (0, 1), (1, 0), (1, 1)]
    peers = [dev(*stream) for stream in STREAMS] + [zdev(1, 0), zdev(1, 1), sibling]
    for peer in peers:
        pl.semaphore_signal(barrier, inc=1, device_id=peer, device_id_type=MESH)

    for copy in loads:
        copy.wait()
    row = lax.broadcasted_iota(jnp.int32, (side, side), 0)
    col = lax.broadcasted_iota(jnp.int32, (side, side), 1)
    perm = jnp.where(jnp.bitwise_xor(row, col) == coil * 8, 1.0, 0.0).astype(BF16)
    for r in range(2):
        sensp[r] = jnp.dot(perm, sens_v[r], preferred_element_type=F32)

    def sens_copy(s):
        return pltpu.make_async_remote_copy(
            src_ref=sensp.at[core], dst_ref=senso.at[s, core],
            send_sem=sens_send.at[0, s], recv_sem=sens_recv.at[0, s],
            device_id=dev(*STREAMS[s]), device_id_type=MESH,
        )

    def sens_pass(s, r):
        return pltpu.make_async_remote_copy(
            src_ref=senso.at[s, r], dst_ref=senso.at[s, r],
            send_sem=sens_send.at[1, s], recv_sem=sens_recv.at[1, s],
            device_id=sibling, device_id_type=MESH,
        )

    cos_p = jnp.dot(perm, plane[0:side, 0:side], preferred_element_type=F32).astype(BF16)
    sin_p = jnp.dot(perm, plane[side : 2 * side, 0:side], preferred_element_type=F32).astype(BF16)
    blocks = jnp.concatenate([block_ref[g : g + 1, :] for g in range(segs)], axis=1)
    blocks = jnp.broadcast_to(blocks, (side, hits))
    yrow = lax.broadcasted_iota(jnp.int32, (side, hits), 0)
    for h in range(2):
        onto = jnp.where(blocks == yrow * 2 + h, 1.0, 0.0).astype(BF16)
        cos_g = jnp.dot(cos_p, onto, preferred_element_type=F32)
        sin_g = jnp.dot(sin_p, onto, preferred_element_type=F32)
        tab[h, 0:side, 0:hits] = cos_g.astype(BF16)
        tab[h, side : 2 * side, hits : 2 * hits] = cos_g.astype(BF16)
        tab[h, 0:side, hits : 2 * hits] = sin_g.astype(BF16)
        tab[h, side : 2 * side, 0:hits] = (-sin_g).astype(BF16)

    arow = lax.broadcasted_iota(jnp.int32, (angles, spokes), 0)
    scol = lax.broadcasted_iota(jnp.int32, (angles, spokes), 1)
    match = jnp.broadcast_to(angle_ref[0:1, :], (angles, spokes)) == arow
    def bin_some(q, carry):
        kload(q).wait()
        for i in range(parts // 4):
            p = q * (parts // 4) + i
            used = jnp.logical_and(match, scol < count_ref[p])
            weights = jnp.where(used, 1.0, 0.0).astype(BF16)
            for r in range(2):
                summed = jnp.dot(weights, kd[r, p], preferred_element_type=F32)
                for g in range(segs):
                    start = g * angles * BPAD + r * parts + p
                    binned[pl.ds(start, angles, stride=BPAD), :] = summed[:, g * seg : (g + 1) * seg]
        return carry

    lax.fori_loop(0, BARRIER_AT, bin_some, 0)
    pl.semaphore_wait(barrier, len(peers))
    for s in range(4):
        sens_copy(s).start()
    for peer in peers:
        pl.semaphore_signal(round_sem.at[0], inc=1, device_id=peer, device_id_type=MESH)
    lax.fori_loop(BARRIER_AT, 4, bin_some, 0)

    def spread_some(q, carry):
        iload(q).wait()
        for k in range(angles // 4):
            a = q * (angles // 4) + k
            for g in range(segs):
                start = pl.multiple_of(g * angles * BPAD + a * BPAD, 8)
                piece = binned[pl.ds(start, 2 * parts), :].astype(BF16)
                got = jnp.dot(piece, itp[a, g], preferred_element_type=F32)
                spread[pl.ds(g * angles + a, 2 * parts, stride=xpad), :] = got
        return carry

    lax.fori_loop(0, 4, spread_some, 0)

    def seg_rows(p, r):
        return pl.ds(pl.multiple_of((r * parts + p) * xpad, 8), hits)

    def seg_copy(s, k, r):
        return pltpu.make_async_remote_copy(
            src_ref=spread.at[seg_rows(part_of(s, k, False), r)], dst_ref=other.at[s, k, r],
            send_sem=send_sem.at[0, s], recv_sem=seg_recv.at[s, k, r],
            device_id=dev(*STREAMS[s]), device_id_type=MESH,
        )

    for k in range(2):
        for s in range(4):
            for r in range(2):
                seg_copy(s, k, r).start()
    pl.semaphore_wait(round_sem.at[0], len(peers))
    for peer in peers:
        pl.semaphore_signal(round_sem.at[1], inc=1, device_id=peer, device_id_type=MESH)
    for s in range(4):
        sens_copy(s).wait_recv()
        sens_pass(s, core).start()
    for s in range(4):
        sens_pass(s, 1 - core).wait_recv()
    pl.semaphore_wait(round_sem.at[1], len(peers))

    def slots(pairing):
        return (1, 0, 1, 3) if pairing == 1 else (2, 1, 0, 1)

    def lay(s):
        first_x, pairing = STREAMS[s]
        return (first_x, 3, 2, 1, 0) if pairing == 1 else (first_x, 1, 1, 0, 1)

    def make(s, k):
        first_x, pairing = STREAMS[s]
        for r in range(2):
            seg_copy(s, k, r).wait_recv()
        p = part_of(s, k, True)
        rows = []
        for r in range(2):
            own = spread[seg_rows(p, r), :].astype(BF16)
            rows.append(jnp.concatenate([own, other[s, k, r].astype(BF16)], axis=1))
        stacked = jnp.concatenate(rows, axis=0)
        for h in range(2):
            got = jnp.dot(tab[h], stacked, preferred_element_type=F32).astype(BF16)
            for n in range(2):
                for r in range(2):
                    half[n, :, r * side + h * seg : r * side + (h + 1) * seg] = got[
                        r * side : (r + 1) * side, n * seg : (n + 1) * seg
                    ]
        mine = jnp.dot(half[0], plane[...], preferred_element_type=F32)
        theirs = jnp.dot(half[1], plane[...], preferred_element_type=F32)
        for jx in range(4):
            for jy in range(4):
                here = slice((jx * 4 + jy) * 16, (jx * 4 + jy + 1) * 16)
                there = (jx ^ pairing) * 4 + jy if first_x else jx * 4 + (jy ^ pairing)
                that = slice(there * 16, (there + 1) * 16)
                a_re, a_im = sensp[0, here, :], sensp[1, here, :]
                b_re, b_im = senso[s, 0, that, :], senso[s, 1, that, :]
                o_re, o_im = mine[here, 0:side], mine[here, side : 2 * side]
                t_re, t_im = theirs[here, 0:side], theirs[here, side : 2 * side]
                parts_of = (
                    (a_re * o_re + a_im * o_im) + (b_re * t_re + b_im * t_im),
                    (a_re * o_im - a_im * o_re) + (b_re * t_im - b_im * t_re),
                )
                for r in range(2):
                    for h in range(2):
                        img[s, k * 4 + r * 2 + h, jx, jy] = parts_of[r][:, h * seg : (h + 1) * seg]

    def copies(s, stage, c):
        first_x, second, sent2, slot0, slot_t = lay(s)
        pairing = STREAMS[s][1]
        sent, keep, onward, quarter = slots(pairing)
        if stage == 2:
            if first_x:
                return img.at[s, c, pl.ds(sent2, 2)], r2x.at[s, c], dev(True, second)
            return img.at[s, c, :, pl.ds(sent2, 2)], r2y.at[s - 2, c], dev(False, second)
        if stage == 3:
            if first_x:
                return r2x.at[s, c, :, pl.ds(sent, 2)], r3.at[s, c], dev(False, pairing)
            return r2y.at[s - 2, c, pl.ds(sent, 2)], r3.at[s, c], dev(True, pairing)
        src = r3.at[s, c, :, onward] if first_x else r3.at[s, c, onward]
        return src, r4.at[s, c], dev(not first_x, second)

    def remote(s, stage, c):
        src, dst, peer = copies(s, stage, c)
        return pltpu.make_async_remote_copy(
            src_ref=src, dst_ref=dst,
            send_sem=send_sem.at[stage - 1, s], recv_sem=recv_sem.at[stage - 2, s, c],
            device_id=peer, device_id_type=MESH,
        )

    def held(s, c, pair, quarter):
        first_x, second, sent2, slot0, slot_t = lay(s)
        j = STREAMS[s][1] if pair else 0
        slot = slot_t if pair else slot0
        if first_x:
            return img[s, c, j, quarter] + r2x[s, c, slot, quarter]
        return img[s, c, quarter, j] + r2y[s - 2, c, quarter, slot]

    def held3(s, c, pair, which, quarter):
        first_x, second, sent2, slot0, slot_t = lay(s)
        slot = slot_t if pair else slot0
        got = r3[s, c, slot, which] if first_x else r3[s, c, which, slot]
        return held(s, c, pair, quarter) + got

    def step(stage, c):
        for s in range(4):
            first_x, second, sent2, slot0, slot_t = lay(s)
            sent, keep, onward, quarter = slots(STREAMS[s][1])
            remote(s, stage - 1, c).wait_recv()
            for pair in range(2):
                slot = slot_t if pair else slot0
                if stage == 3:
                    for q in (sent, sent + 1):
                        value = held(s, c, pair, q)
                        if first_x:
                            r2x[s, c, slot, q] = value
                        else:
                            r2y[s - 2, c, q, slot] = value
                else:
                    value = held3(s, c, pair, onward, quarter)
                    if first_x:
                        r3[s, c, slot, onward] = value
                    else:
                        r3[s, c, onward, slot] = value
            remote(s, stage, c).start()

    def last_copies(kr, pair, s):
        got = []
        for jz, jk in turns:
            n = pair * 4 + jz * 2 + jk
            if n == 0:
                continue
            if pair:
                src, dst, peer = xbuf.at[1, kr, jz, s], rx.at[n, kr, s], dev(*STREAMS[s], jz, jk)
            else:
                src, dst, peer = xbuf.at[0, kr, jz], rx.at[n, kr], zdev(jz, jk)
            got.append(
                pltpu.make_async_remote_copy(
                    src_ref=src, dst_ref=dst, send_sem=own_send.at[n], recv_sem=own_recv.at[n, kr],
                    device_id=peer, device_id_type=MESH,
                )
            )
        return got

    def last(kr):
        for s in range(4):
            first_x, second, sent2, slot0, slot_t = lay(s)
            keep = slots(STREAMS[s][1])[1]
            for h in range(2):
                c = kr * 2 + h
                remote(s, 4, c).wait_recv()
                for pair in range(2):
                    slot = slot_t if pair else slot0
                    value = r4[s, c, slot] + held3(s, c, pair, keep, 0)
                    for jz in range(2):
                        xbuf[pair, kr, jz, s, h] = value[jz * 8 : (jz + 1) * 8]
            for copy in last_copies(kr, 1, s):
                copy.start()
        for copy in last_copies(kr, 0, 0):
            copy.start()

    def arrived(n, kr):
        whole = rx.at[n, kr]
        return pltpu.make_async_remote_copy(
            src_ref=whole, dst_ref=whole, send_sem=own_send.at[n], recv_sem=own_recv.at[n, kr],
            device_id=sibling, device_id_type=MESH,
        )

    def gath_rows(slot, kr):
        return pl.ds(pl.multiple_of((slot * 4 + kr) * 128, 128), 128)

    def kz_remote(n, kr):
        where = gath.at[gath_rows(far if n else group, kr)]
        return pltpu.make_async_remote_copy(
            src_ref=where, dst_ref=where,
            send_sem=kz_send.at[n], recv_sem=kz_recv.at[n, kr],
            device_id=sibling, device_id_type=MESH,
        )

    def finish(kr):
        for n in range(1, 8):
            arrived(n, kr).wait_recv()
        for s in range(4):
            for h in range(2):
                for slot, mine, value in (
                    (group, True, xbuf[0, kr, 0, s, h] + rx[2, kr, s, h]),
                    (group, False, rx[4, kr, s, h] + rx[6, kr, s, h]),
                    (far, True, rx[1, kr, s, h] + rx[3, kr, s, h]),
                    (far, False, rx[5, kr, s, h] + rx[7, kr, s, h]),
                ):
                    start = (slot * 4 + kr) * 128 + h * 64 + part_of(s, 0, mine)
                    gath[pl.ds(start, 8, stride=8), :] = value
        for n in range(2):
            kz_remote(n, kr).start()

    def put(kr, first, last_one):
        for n in range(2):
            kz_remote(n, kr).wait_recv()
        for h in range(2):
            rows = []
            for g in range(4):
                base = (g * 4 + kr) * 128 + h * 64
                rows.append(jnp.concatenate([gath[base + yy * 8 : base + yy * 8 + 8, :] for yy in range(8)], axis=1))
            stacked = jnp.concatenate(rows, axis=0)
            high = stacked.astype(BF16)
            low = (stacked - high.astype(F32)).astype(BF16)
            got = jnp.dot(
                ztab_ref[group, kr], jnp.concatenate([high, high, low], axis=0), preferred_element_type=F32
            )
            if not first:
                got = got + total[h]
            if not last_one:
                total[h] = got
                continue
            for yy in range(8):
                kzout[h, pl.ds(yy, 2 * parts, stride=8), :] = got[:, yy * seg : (yy + 1) * seg]
            out_ref[:, :, :, h * seg : (h + 1) * seg] = kzout[h].reshape(2, parts, 8, seg)

    begun = [what for what, *where in PLAN].index("O")
    for n, (what, *where) in enumerate(PLAN):
        if what == "M":
            make(where[1], where[0])
        elif what == "2":
            remote(where[1], 2, where[0]).start()
        elif what == "X":
            last(*where)
        elif what == "F":
            finish(*where)
        elif what == "O":
            put(*where, n == begun, n == len(PLAN) - 1)
        else:
            step(int(what), *where)

    def sent_all(ref, sem, unused, peer):
        pltpu.make_async_remote_copy(
            src_ref=ref, dst_ref=ref, send_sem=sem, recv_sem=unused, device_id=peer, device_id_type=MESH
        ).wait_send()

    everything = pl.ds(0, 8)
    for s in range(4):
        sens_copy(s).wait_send()
        sens_pass(s, core).wait_send()
        sent_all(other.at[s], send_sem.at[0, s], seg_recv.at[s, 0, 0], sibling)
        for stage in range(2, 5):
            src, dst, peer = copies(s, stage, everything)
            sent_all(src, send_sem.at[stage - 1, s], recv_sem.at[stage - 2, s, 0], peer)
    for n in range(1, 8):
        sent_all(rx.at[n], own_send.at[n], own_recv.at[n, 0], sibling)
    for n in range(2):
        sent_all(gath.at[pl.ds(0, 512)], kz_send.at[n], kz_recv.at[n, 0], sibling)


def per_device(kdata, spoke_angle, spoke_count, block_index, interp, sens_maps):
    side = sens_maps.shape[2]
    parts = kdata.shape[1]
    spokes, samples = kdata.shape[3], kdata.shape[4]
    angles, segs, seg = interp.shape[0], interp.shape[1], interp.shape[2]
    hits = angles * segs
    any_spec = pl.BlockSpec(memory_space=pl.ANY)
    vmem_spec = pl.BlockSpec(memory_space=pltpu.VMEM)
    return pl.pallas_call(
        functools.partial(kernel, parts, angles, spokes, side),
        out_shape=jax.ShapeDtypeStruct((2, parts, 8, side), F32),
        in_specs=[pl.BlockSpec(memory_space=pltpu.SMEM)] + [vmem_spec] * 3 + [any_spec] * 4,
        out_specs=vmem_spec,
        scratch_shapes=[
            pltpu.VMEM((2, parts, spokes, samples), BF16),
            pltpu.VMEM((angles, segs, seg, seg), BF16),
            pltpu.VMEM((2, side, side), BF16),
            pltpu.VMEM((2 * side, 2 * side), BF16),
            pltpu.VMEM((2, 2 * side, 2 * hits), BF16),
            pltpu.VMEM((2, side, side), F32),
            pltpu.VMEM((4, 2, side, side), F32),
            pltpu.VMEM((segs * angles * BPAD, seg), F32),
            pltpu.VMEM((2 * parts * (hits + 8), seg), F32),
            pltpu.VMEM((4, 2, 2, hits, seg), F32),
            pltpu.VMEM((2, side, 2 * side), BF16),
            pltpu.VMEM((4, 8, 4, 4, 16, seg), F32),
            pltpu.VMEM((2, 8, 2, 4, 16, seg), F32),
            pltpu.VMEM((2, 8, 4, 2, 16, seg), F32),
            pltpu.VMEM((4, 8, 2, 2, 16, seg), F32),
            pltpu.VMEM((4, 8, 2, 16, seg), F32),
            pltpu.VMEM((2, 4, 2, 4, 2, 8, seg), F32),
            pltpu.VMEM((8, 4, 4, 2, 8, seg), F32),
            pltpu.VMEM((4 * 4 * 128, seg), F32),
            pltpu.VMEM((2, 2 * parts, 8 * seg), F32),
            pltpu.VMEM((2, 2 * parts * 8, seg), F32),
            pltpu.SemaphoreType.DMA((10,)),
            pltpu.SemaphoreType.DMA((2, 4)),
            pltpu.SemaphoreType.DMA((2, 4)),
            pltpu.SemaphoreType.DMA((4, 4)),
            pltpu.SemaphoreType.DMA((4, 2, 2)),
            pltpu.SemaphoreType.DMA((3, 4, 8)),
            pltpu.SemaphoreType.DMA((8,)),
            pltpu.SemaphoreType.DMA((8, 4)),
            pltpu.SemaphoreType.DMA((2,)),
            pltpu.SemaphoreType.DMA((2, 4)),
            pltpu.SemaphoreType.REGULAR((2,)),
        ],
        compiler_params=pltpu.CompilerParams(
            collective_id=0, has_side_effects=True, vmem_limit_bytes=56 << 20
        ),
    )(
        spoke_count,
        spoke_angle.reshape(1, spokes),
        block_index.T,
        kz_table(4, parts),
        kdata[:, :, 0],
        interp,
        sens_maps[:, 0],
        plane_table(side),
    )

def solution(mesh):
    placed = (
        P(None, "kz", "coil", None, None),
        P(),
        P("kz"),
        P(),
        P(),
        P(None, "coil", None, None),
    )
    return jax.shard_map(
        per_device,
        mesh=mesh,
        in_specs=placed,
        out_specs=P(None, "kz", "coil", None),
        check_vma=False,
    )
```

```python
import functools

import jax
import jax.numpy as jnp
import numpy as np
from jax import lax
from jax.experimental import pallas as pl
from jax.experimental.pallas import tpu as pltpu
from jax.sharding import PartitionSpec as P

F32 = jnp.float32
BF16 = jnp.bfloat16
MESH = pl.DeviceIdType.MESH

PLAN = (('M', 0, 2), ('M', 0, 1), ('2', 1, 1), ('M', 0, 3), ('2', 1, 3), ('2', 0, 3), ('2', 0, 2), ('M', 0, 0), ('2', 0, 0), ('2', 1, 0), ('2', 2, 0), ('2', 1, 2), ('2', 0, 1), ('2', 2, 1), ('2', 3, 2), ('2', 3, 3), ('M', 1, 1), ('2', 3, 1), ('2', 2, 2), ('2', 2, 3), ('2', 3, 0), ('M', 1, 0), ('M', 1, 3), ('2', 4, 0), ('3', 0), ('3', 1), ('2', 7, 1), ('M', 1, 2), ('2', 6, 2), ('2', 4, 2), ('2', 6, 0), ('2', 5, 3), ('2', 4, 3), ('3', 2), ('2', 5, 2), ('2', 4, 1), ('2', 6, 1), ('2', 6, 3), ('2', 5, 1), ('2', 5, 0), ('3', 3), ('4', 0), ('4', 1), ('2', 7, 0), ('3', 4), ('2', 7, 2), ('4', 2), ('2', 7, 3), ('3', 5), ('4', 3), ('3', 6), ('X', 0), ('4', 4), ('3', 7), ('4', 5), ('X', 1), ('4', 6), ('4', 7), ('X', 2), ('F', 0), ('X', 3), ('F', 1), ('O', 0), ('F', 2), ('O', 1), ('F', 3), ('O', 2), ('O', 3))
BARRIER_AT = 0
BPAD = 40

STREAMS = ((True, 1), (True, 3), (False, 1), (False, 3))


def dft_np(rows, cols, length):
    product = (rows[:, None] * cols[None, :]) % length
    phase = product.astype(np.float64) * (2.0 * np.pi / length)
    return np.cos(phase) / np.sqrt(length), np.sin(phase) / np.sqrt(length)


def plane_table(side):
    index = np.arange(side)
    cos_t, sin_t = dft_np(index, index, side)
    table = np.block([[cos_t, -sin_t], [sin_t, cos_t]])
    return jnp.asarray(table, dtype=BF16)


def kz_table(groups, parts):
    total = groups * parts
    index = np.arange(total)
    cos_z, sin_z = dft_np(index, index, total)
    blocks = []
    for g in range(groups):
        c = cos_z[g * parts : (g + 1) * parts].reshape(parts, groups, 1, parts)
        s = sin_z[g * parts : (g + 1) * parts].reshape(parts, groups, 1, parts)
        real = np.concatenate([c, s], axis=2).reshape(parts, -1)
        imag = np.concatenate([-s, c], axis=2).reshape(parts, -1)
        blocks.append(np.concatenate([real, imag], axis=0))
    table = np.stack(blocks).astype(np.float32).reshape(groups, 2 * parts, groups, 2, 2, parts // 2)
    table = table.transpose(0, 4, 3, 1, 2, 5).reshape(groups, 4, 2 * parts, groups * (parts // 2))
    high = table.astype(jnp.bfloat16)
    low = (table - high.astype(np.float32)).astype(jnp.bfloat16)
    return jnp.asarray(np.concatenate([high, low, high], axis=3))


def flip(i, pairing):
    return i + 1 - 2 * (i % 2) if pairing == 1 else 3 - i


def kernel(
    parts, angles, spokes, side,
    count_ref, angle_ref, block_ref, ztab_ref,
    kdata_hbm, interp_hbm, sens_hbm, plane_hbm,
    out_ref,
    kd, itp, sens_v, plane, tab, sensp, senso, binned, spread, other, half,
    img, r2x, r2y, r3, r4, xbuf, rx, gath, total, kzout,
    load_sem, sens_send, sens_recv, send_sem, seg_recv, recv_sem, own_send, own_recv, kz_send, kz_recv, round_sem,
):
    segs = 4
    seg = 128
    hits = angles * segs
    xpad = hits + 8
    coil = lax.axis_index("coil")
    group = lax.axis_index("kz")
    core = group % 2
    x, y, z = coil // 8, (coil // 2) % 4, coil % 2

    beside = group + 1 - 2 * core
    far = (group + 2) % 4
    sibling = (coil, beside)

    def dev(axis_x, pairing, over_z=0, over_kz=0):
        zz = 1 - z if over_z else z
        there = far if over_kz else group
        if axis_x:
            return ((flip(x, pairing) * 4 + y) * 2 + zz, there)
        return ((x * 4 + flip(y, pairing)) * 2 + zz, there)

    def zdev(over_z, over_kz):
        return ((x * 4 + y) * 2 + (1 - z if over_z else z), far if over_kz else group)

    def side_of(s):
        first_x, pairing = STREAMS[s]
        i = x if first_x else y
        return ((i + 1) // 2) % 2 if pairing == 1 else i // 2

    def part_of(s, k, mine):
        return k * 8 + s * 2 + (side_of(s) if mine else 1 - side_of(s))

    loads = [
        pltpu.make_async_copy(plane_hbm, plane, load_sem.at[0]),
        pltpu.make_async_copy(sens_hbm, sens_v, load_sem.at[1]),
    ]

    def kload(q):
        rows = pl.ds(q * (parts // 4), parts // 4)
        return pltpu.make_async_copy(kdata_hbm.at[:, rows], kd.at[:, rows], load_sem.at[2 + q])

    def iload(q):
        rows = pl.ds(q * (angles // 4), angles // 4)
        return pltpu.make_async_copy(interp_hbm.at[rows], itp.at[rows], load_sem.at[6 + q])

    for copy in loads + [kload(q) for q in range(4)] + [iload(q) for q in range(4)]:
        copy.start()

    barrier = pltpu.get_barrier_semaphore()
    turns = [(0, 0), (0, 1), (1, 0), (1, 1)]
    peers = [dev(*stream) for stream in STREAMS] + [zdev(1, 0), zdev(1, 1), sibling]
    for peer in peers:
        pl.semaphore_signal(barrier, inc=1, device_id=peer, device_id_type=MESH)

    for copy in loads:
        copy.wait()
    row = lax.broadcasted_iota(jnp.int32, (side, side), 0)
    col = lax.broadcasted_iota(jnp.int32, (side, side), 1)
    perm = jnp.where(jnp.bitwise_xor(row, col) == coil * 8, 1.0, 0.0).astype(BF16)
    for r in range(2):
        sensp[r] = jnp.dot(perm, sens_v[r], preferred_element_type=F32)

    def sens_copy(s):
        return pltpu.make_async_remote_copy(
            src_ref=sensp.at[core], dst_ref=senso.at[s, core],
            send_sem=sens_send.at[0, s], recv_sem=sens_recv.at[0, s],
            device_id=dev(*STREAMS[s]), device_id_type=MESH,
        )

    def sens_pass(s, r):
        return pltpu.make_async_remote_copy(
            src_ref=senso.at[s, r], dst_ref=senso.at[s, r],
            send_sem=sens_send.at[1, s], recv_sem=sens_recv.at[1, s],
            device_id=sibling, device_id_type=MESH,
        )

    cos_p = jnp.dot(perm, plane[0:side, 0:side], preferred_element_type=F32).astype(BF16)
    sin_p = jnp.dot(perm, plane[side : 2 * side, 0:side], preferred_element_type=F32).astype(BF16)
    blocks = jnp.concatenate([block_ref[g : g + 1, :] for g in range(segs)], axis=1)
    blocks = jnp.broadcast_to(blocks, (side, hits))
    yrow = lax.broadcasted_iota(jnp.int32, (side, hits), 0)
    for h in range(2):
        onto = jnp.where(blocks == yrow * 2 + h, 1.0, 0.0).astype(BF16)
        cos_g = jnp.dot(cos_p, onto, preferred_element_type=F32)
        sin_g = jnp.dot(sin_p, onto, preferred_element_type=F32)
        tab[h, 0:side, 0:hits] = cos_g.astype(BF16)
        tab[h, side : 2 * side, hits : 2 * hits] = cos_g.astype(BF16)
        tab[h, 0:side, hits : 2 * hits] = sin_g.astype(BF16)
        tab[h, side : 2 * side, 0:hits] = (-sin_g).astype(BF16)

    arow = lax.broadcasted_iota(jnp.int32, (angles, spokes), 0)
    scol = lax.broadcasted_iota(jnp.int32, (angles, spokes), 1)
    match = jnp.broadcast_to(angle_ref[0:1, :], (angles, spokes)) == arow
    def bin_some(q, carry):
        kload(q).wait()
        for i in range(parts // 4):
            p = q * (parts // 4) + i
            used = jnp.logical_and(match, scol < count_ref[p])
            weights = jnp.where(used, 1.0, 0.0).astype(BF16)
            for r in range(2):
                summed = jnp.dot(weights, kd[r, p], preferred_element_type=F32)
                for g in range(segs):
                    start = g * angles * BPAD + r * parts + p
                    binned[pl.ds(start, angles, stride=BPAD), :] = summed[:, g * seg : (g + 1) * seg]
        return carry

    lax.fori_loop(0, BARRIER_AT, bin_some, 0)
    pl.semaphore_wait(barrier, len(peers))
    for s in range(4):
        sens_copy(s).start()
    for peer in peers:
        pl.semaphore_signal(round_sem.at[0], inc=1, device_id=peer, device_id_type=MESH)
    lax.fori_loop(BARRIER_AT, 4, bin_some, 0)

    def spread_some(q, carry):
        iload(q).wait()
        for k in range(angles // 4):
            a = q * (angles // 4) + k
            for g in range(segs):
                start = pl.multiple_of(g * angles * BPAD + a * BPAD, 8)
                piece = binned[pl.ds(start, 2 * parts), :].astype(BF16)
                got = jnp.dot(piece, itp[a, g], preferred_element_type=F32)
                spread[pl.ds(g * angles + a, 2 * parts, stride=xpad), :] = got
        return carry

    lax.fori_loop(0, 4, spread_some, 0)

    def seg_rows(p, r):
        return pl.ds(pl.multiple_of((r * parts + p) * xpad, 8), hits)

    def seg_copy(s, k, r):
        return pltpu.make_async_remote_copy(
            src_ref=spread.at[seg_rows(part_of(s, k, False), r)], dst_ref=other.at[s, k, r],
            send_sem=send_sem.at[0, s], recv_sem=seg_recv.at[s, k, r],
            device_id=dev(*STREAMS[s]), device_id_type=MESH,
        )

    for k in range(2):
        for s in range(4):
            for r in range(2):
                seg_copy(s, k, r).start()
    pl.semaphore_wait(round_sem.at[0], len(peers))
    for peer in peers:
        pl.semaphore_signal(round_sem.at[1], inc=1, device_id=peer, device_id_type=MESH)
    for s in range(4):
        sens_copy(s).wait_recv()
        sens_pass(s, core).start()
    for s in range(4):
        sens_pass(s, 1 - core).wait_recv()
    pl.semaphore_wait(round_sem.at[1], len(peers))

    def slots(pairing):
        return (1, 0, 1, 3) if pairing == 1 else (2, 1, 0, 1)

    def lay(s):
        first_x, pairing = STREAMS[s]
        return (first_x, 3, 2, 1, 0) if pairing == 1 else (first_x, 1, 1, 0, 1)

    def make(s, k):
        first_x, pairing = STREAMS[s]
        for r in range(2):
            seg_copy(s, k, r).wait_recv()
        p = part_of(s, k, True)
        rows = []
        for r in range(2):
            own = spread[seg_rows(p, r), :].astype(BF16)
            rows.append(jnp.concatenate([own, other[s, k, r].astype(BF16)], axis=1))
        stacked = jnp.concatenate(rows, axis=0)
        for h in range(2):
            got = jnp.dot(tab[h], stacked, preferred_element_type=F32).astype(BF16)
            for n in range(2):
                for r in range(2):
                    half[n, :, r * side + h * seg : r * side + (h + 1) * seg] = got[
                        r * side : (r + 1) * side, n * seg : (n + 1) * seg
                    ]
        mine = jnp.dot(half[0], plane[...], preferred_element_type=F32)
        theirs = jnp.dot(half[1], plane[...], preferred_element_type=F32)
        for jx in range(4):
            for jy in range(4):
                here = slice((jx * 4 + jy) * 16, (jx * 4 + jy + 1) * 16)
                there = (jx ^ pairing) * 4 + jy if first_x else jx * 4 + (jy ^ pairing)
                that = slice(there * 16, (there + 1) * 16)
                a_re, a_im = sensp[0, here, :], sensp[1, here, :]
                b_re, b_im = senso[s, 0, that, :], senso[s, 1, that, :]
                o_re, o_im = mine[here, 0:side], mine[here, side : 2 * side]
                t_re, t_im = theirs[here, 0:side], theirs[here, side : 2 * side]
                parts_of = (
                    (a_re * o_re + a_im * o_im) + (b_re * t_re + b_im * t_im),
                    (a_re * o_im - a_im * o_re) + (b_re * t_im - b_im * t_re),
                )
                for r in range(2):
                    for h in range(2):
                        img[s, k * 4 + r * 2 + h, jx, jy] = parts_of[r][:, h * seg : (h + 1) * seg]

    def copies(s, stage, c):
        first_x, second, sent2, slot0, slot_t = lay(s)
        pairing = STREAMS[s][1]
        sent, keep, onward, quarter = slots(pairing)
        if stage == 2:
            if first_x:
                return img.at[s, c, pl.ds(sent2, 2)], r2x.at[s, c], dev(True, second)
            return img.at[s, c, :, pl.ds(sent2, 2)], r2y.at[s - 2, c], dev(False, second)
        if stage == 3:
            if first_x:
                return r2x.at[s, c, :, pl.ds(sent, 2)], r3.at[s, c], dev(False, pairing)
            return r2y.at[s - 2, c, pl.ds(sent, 2)], r3.at[s, c], dev(True, pairing)
        src = r3.at[s, c, :, onward] if first_x else r3.at[s, c, onward]
        return src, r4.at[s, c], dev(not first_x, second)

    def remote(s, stage, c):
        src, dst, peer = copies(s, stage, c)
        return pltpu.make_async_remote_copy(
            src_ref=src, dst_ref=dst,
            send_sem=send_sem.at[stage - 1, s], recv_sem=recv_sem.at[stage - 2, s, c],
            device_id=peer, device_id_type=MESH,
        )

    def held(s, c, pair, quarter):
        first_x, second, sent2, slot0, slot_t = lay(s)
        j = STREAMS[s][1] if pair else 0
        slot = slot_t if pair else slot0
        if first_x:
            return img[s, c, j, quarter] + r2x[s, c, slot, quarter]
        return img[s, c, quarter, j] + r2y[s - 2, c, quarter, slot]

    def held3(s, c, pair, which, quarter):
        first_x, second, sent2, slot0, slot_t = lay(s)
        slot = slot_t if pair else slot0
        got = r3[s, c, slot, which] if first_x else r3[s, c, which, slot]
        return held(s, c, pair, quarter) + got

    def step(stage, c):
        for s in range(4):
            first_x, second, sent2, slot0, slot_t = lay(s)
            sent, keep, onward, quarter = slots(STREAMS[s][1])
            remote(s, stage - 1, c).wait_recv()
            for pair in range(2):
                slot = slot_t if pair else slot0
                if stage == 3:
                    for q in (sent, sent + 1):
                        value = held(s, c, pair, q)
                        if first_x:
                            r2x[s, c, slot, q] = value
                        else:
                            r2y[s - 2, c, q, slot] = value
                else:
                    value = held3(s, c, pair, onward, quarter)
                    if first_x:
                        r3[s, c, slot, onward] = value
                    else:
                        r3[s, c, onward, slot] = value
            remote(s, stage, c).start()

    def last_copies(kr, pair, s):
        got = []
        for jz, jk in turns:
            n = pair * 4 + jz * 2 + jk
            if n == 0:
                continue
            if pair:
                src, dst, peer = xbuf.at[1, kr, jz, s], rx.at[n, kr, s], dev(*STREAMS[s], jz, jk)
            else:
                src, dst, peer = xbuf.at[0, kr, jz], rx.at[n, kr], zdev(jz, jk)
            got.append(
                pltpu.make_async_remote_copy(
                    src_ref=src, dst_ref=dst, send_sem=own_send.at[n], recv_sem=own_recv.at[n, kr],
                    device_id=peer, device_id_type=MESH,
                )
            )
        return got

    def last(kr):
        for s in range(4):
            first_x, second, sent2, slot0, slot_t = lay(s)
            keep = slots(STREAMS[s][1])[1]
            for h in range(2):
                c = kr * 2 + h
                remote(s, 4, c).wait_recv()
                for pair in range(2):
                    slot = slot_t if pair else slot0
                    value = r4[s, c, slot] + held3(s, c, pair, keep, 0)
                    for jz in range(2):
                        xbuf[pair, kr, jz, s, h] = value[jz * 8 : (jz + 1) * 8]
            for copy in last_copies(kr, 1, s):
                copy.start()
        for copy in last_copies(kr, 0, 0):
            copy.start()

    def arrived(n, kr):
        whole = rx.at[n, kr]
        return pltpu.make_async_remote_copy(
            src_ref=whole, dst_ref=whole, send_sem=own_send.at[n], recv_sem=own_recv.at[n, kr],
            device_id=sibling, device_id_type=MESH,
        )

    def gath_rows(slot, kr):
        return pl.ds(pl.multiple_of((slot * 4 + kr) * 128, 128), 128)

    def kz_remote(n, kr):
        where = gath.at[gath_rows(far if n else group, kr)]
        return pltpu.make_async_remote_copy(
            src_ref=where, dst_ref=where,
            send_sem=kz_send.at[n], recv_sem=kz_recv.at[n, kr],
            device_id=sibling, device_id_type=MESH,
        )

    def finish(kr):
        for n in range(1, 8):
            arrived(n, kr).wait_recv()
        for s in range(4):
            for h in range(2):
                for slot, mine, value in (
                    (group, True, xbuf[0, kr, 0, s, h] + rx[2, kr, s, h]),
                    (group, False, rx[4, kr, s, h] + rx[6, kr, s, h]),
                    (far, True, rx[1, kr, s, h] + rx[3, kr, s, h]),
                    (far, False, rx[5, kr, s, h] + rx[7, kr, s, h]),
                ):
                    start = (slot * 4 + kr) * 128 + h * 64 + part_of(s, 0, mine)
                    gath[pl.ds(start, 8, stride=8), :] = value
        for n in range(2):
            kz_remote(n, kr).start()

    def put(kr, first, last_one):
        for n in range(2):
            kz_remote(n, kr).wait_recv()
        for h in range(2):
            rows = []
            for g in range(4):
                base = (g * 4 + kr) * 128 + h * 64
                rows.append(jnp.concatenate([gath[base + yy * 8 : base + yy * 8 + 8, :] for yy in range(8)], axis=1))
            stacked = jnp.concatenate(rows, axis=0)
            high = stacked.astype(BF16)
            low = (stacked - high.astype(F32)).astype(BF16)
            got = jnp.dot(
                ztab_ref[group, kr], jnp.concatenate([high, high, low], axis=0), preferred_element_type=F32
            )
            if not first:
                got = got + total[h]
            if not last_one:
                total[h] = got
                continue
            for yy in range(8):
                kzout[h, pl.ds(yy, 2 * parts, stride=8), :] = got[:, yy * seg : (yy + 1) * seg]
            out_ref[:, :, :, h * seg : (h + 1) * seg] = kzout[h, 0 : 2 * parts * 8].reshape(2, parts, 8, seg)

    begun = [what for what, *where in PLAN].index("O")
    for n, (what, *where) in enumerate(PLAN):
        if what == "M":
            make(where[1], where[0])
        elif what == "2":
            remote(where[1], 2, where[0]).start()
        elif what == "X":
            last(*where)
        elif what == "F":
            finish(*where)
        elif what == "O":
            put(*where, n == begun, n == len(PLAN) - 1)
        else:
            step(int(what), *where)

    def sent_all(ref, sem, unused, peer):
        pltpu.make_async_remote_copy(
            src_ref=ref, dst_ref=ref, send_sem=sem, recv_sem=unused, device_id=peer, device_id_type=MESH
        ).wait_send()

    everything = pl.ds(0, 8)
    for s in range(4):
        sens_copy(s).wait_send()
        sens_pass(s, core).wait_send()
        sent_all(other.at[s], send_sem.at[0, s], seg_recv.at[s, 0, 0], sibling)
        for stage in range(2, 5):
            src, dst, peer = copies(s, stage, everything)
            sent_all(src, send_sem.at[stage - 1, s], recv_sem.at[stage - 2, s, 0], peer)
    for n in range(1, 8):
        sent_all(rx.at[n], own_send.at[n], own_recv.at[n, 0], sibling)
    for n in range(2):
        sent_all(gath.at[pl.ds(0, 512)], kz_send.at[n], kz_recv.at[n, 0], sibling)


def per_device(kdata, spoke_angle, spoke_count, block_index, interp, sens_maps):
    side = sens_maps.shape[2]
    parts = kdata.shape[1]
    spokes, samples = kdata.shape[3], kdata.shape[4]
    angles, segs, seg = interp.shape[0], interp.shape[1], interp.shape[2]
    hits = angles * segs
    any_spec = pl.BlockSpec(memory_space=pl.ANY)
    vmem_spec = pl.BlockSpec(memory_space=pltpu.VMEM)
    return pl.pallas_call(
        functools.partial(kernel, parts, angles, spokes, side),
        out_shape=jax.ShapeDtypeStruct((2, parts, 8, side), F32),
        in_specs=[pl.BlockSpec(memory_space=pltpu.SMEM)] + [vmem_spec] * 3 + [any_spec] * 4,
        out_specs=vmem_spec,
        scratch_shapes=[
            pltpu.VMEM((2, parts, spokes, samples), BF16),
            pltpu.VMEM((angles, segs, seg, seg), BF16),
            pltpu.VMEM((2, side, side), BF16),
            pltpu.VMEM((2 * side, 2 * side), BF16),
            pltpu.VMEM((2, 2 * side, 2 * hits), BF16),
            pltpu.VMEM((2, side, side), F32),
            pltpu.VMEM((4, 2, side, side), F32),
            pltpu.VMEM(((segs * angles + 1) * BPAD, seg), F32),
            pltpu.VMEM(((2 * parts + 1) * (hits + 8), seg), F32),
            pltpu.VMEM((4, 2, 2, hits, seg), F32),
            pltpu.VMEM((2, side, 2 * side), BF16),
            pltpu.VMEM((4, 8, 4, 4, 16, seg), F32),
            pltpu.VMEM((2, 8, 2, 4, 16, seg), F32),
            pltpu.VMEM((2, 8, 4, 2, 16, seg), F32),
            pltpu.VMEM((4, 8, 2, 2, 16, seg), F32),
            pltpu.VMEM((4, 8, 2, 16, seg), F32),
            pltpu.VMEM((2, 4, 2, 4, 2, 8, seg), F32),
            pltpu.VMEM((8, 4, 4, 2, 8, seg), F32),
            pltpu.VMEM((4 * 4 * 128 + 8, seg), F32),
            pltpu.VMEM((2, 2 * parts, 8 * seg), F32),
            pltpu.VMEM((2, 2 * parts * 8 + 8, seg), F32),
            pltpu.SemaphoreType.DMA((10,)),
            pltpu.SemaphoreType.DMA((2, 4)),
            pltpu.SemaphoreType.DMA((2, 4)),
            pltpu.SemaphoreType.DMA((4, 4)),
            pltpu.SemaphoreType.DMA((4, 2, 2)),
            pltpu.SemaphoreType.DMA((3, 4, 8)),
            pltpu.SemaphoreType.DMA((8,)),
            pltpu.SemaphoreType.DMA((8, 4)),
            pltpu.SemaphoreType.DMA((2,)),
            pltpu.SemaphoreType.DMA((2, 4)),
            pltpu.SemaphoreType.REGULAR((2,)),
        ],
        compiler_params=pltpu.CompilerParams(
            collective_id=0, has_side_effects=True, vmem_limit_bytes=56 << 20
        ),
    )(
        spoke_count,
        spoke_angle.reshape(1, spokes),
        block_index.T,
        kz_table(4, parts),
        kdata[:, :, 0],
        interp,
        sens_maps[:, 0],
        plane_table(side),
    )

def solution(mesh):
    placed = (
        P(None, "kz", "coil", None, None),
        P(),
        P("kz"),
        P(),
        P(),
        P(None, "coil", None, None),
    )
    return jax.shard_map(
        per_device,
        mesh=mesh,
        in_specs=placed,
        out_specs=P(None, "kz", "coil", None),
        check_vma=False,
    )
```

```python
import functools

import jax
import jax.numpy as jnp
import numpy as np
from jax import lax
from jax.experimental import pallas as pl
from jax.experimental.pallas import tpu as pltpu
from jax.sharding import PartitionSpec as P

F32 = jnp.float32
BF16 = jnp.bfloat16
MESH = pl.DeviceIdType.MESH

PLAN = (('M', 0, 2), ('M', 0, 1), ('2', 1, 1), ('M', 0, 3), ('2', 1, 3), ('2', 0, 3), ('2', 0, 2), ('M', 0, 0), ('2', 0, 0), ('2', 1, 0), ('2', 2, 0), ('2', 1, 2), ('2', 0, 1), ('2', 2, 1), ('2', 3, 2), ('2', 3, 3), ('M', 1, 1), ('2', 3, 1), ('2', 2, 2), ('2', 2, 3), ('2', 3, 0), ('M', 1, 0), ('M', 1, 3), ('2', 4, 0), ('3', 0), ('3', 1), ('2', 7, 1), ('M', 1, 2), ('2', 6, 2), ('2', 4, 2), ('2', 6, 0), ('2', 5, 3), ('2', 4, 3), ('3', 2), ('2', 5, 2), ('2', 4, 1), ('2', 6, 1), ('2', 6, 3), ('2', 5, 1), ('2', 5, 0), ('3', 3), ('4', 0), ('4', 1), ('2', 7, 0), ('3', 4), ('2', 7, 2), ('4', 2), ('2', 7, 3), ('3', 5), ('4', 3), ('3', 6), ('X', 0), ('4', 4), ('3', 7), ('4', 5), ('X', 1), ('4', 6), ('4', 7), ('X', 2), ('F', 0), ('X', 3), ('F', 1), ('O', 0), ('F', 2), ('O', 1), ('F', 3), ('O', 2), ('O', 3))
BARRIER_AT = 0
BPAD = 40

STREAMS = ((True, 1), (True, 3), (False, 1), (False, 3))


def dft_np(rows, cols, length):
    product = (rows[:, None] * cols[None, :]) % length
    phase = product.astype(np.float64) * (2.0 * np.pi / length)
    return np.cos(phase) / np.sqrt(length), np.sin(phase) / np.sqrt(length)


def plane_table(side):
    index = np.arange(side)
    cos_t, sin_t = dft_np(index, index, side)
    table = np.block([[cos_t, -sin_t], [sin_t, cos_t]])
    return jnp.asarray(table, dtype=BF16)


def kz_table(groups, parts):
    total = groups * parts
    index = np.arange(total)
    cos_z, sin_z = dft_np(index, index, total)
    blocks = []
    for g in range(groups):
        c = cos_z[g * parts : (g + 1) * parts].reshape(parts, groups, 1, parts)
        s = sin_z[g * parts : (g + 1) * parts].reshape(parts, groups, 1, parts)
        real = np.concatenate([c, s], axis=2).reshape(parts, -1)
        imag = np.concatenate([-s, c], axis=2).reshape(parts, -1)
        blocks.append(np.concatenate([real, imag], axis=0))
    table = np.stack(blocks).astype(np.float32).reshape(groups, 2 * parts, groups, 2, 2, parts // 2)
    table = table.transpose(0, 4, 3, 1, 2, 5).reshape(groups, 4, 2 * parts, groups * (parts // 2))
    high = table.astype(jnp.bfloat16)
    low = (table - high.astype(np.float32)).astype(jnp.bfloat16)
    return jnp.asarray(np.concatenate([high, low, high], axis=3))


def flip(i, pairing):
    return i + 1 - 2 * (i % 2) if pairing == 1 else 3 - i


def kernel(
    parts, angles, spokes, side,
    count_ref, angle_ref, block_ref, ztab_ref,
    kdata_hbm, interp_hbm, sens_hbm, plane_hbm,
    out_ref,
    kd, itp, sens_v, plane, tab, sensp, senso, binned, spread, other, half,
    img, r2x, r2y, r3, r4, xbuf, rx, gath, total, kzout,
    load_sem, sens_send, sens_recv, send_sem, seg_recv, recv_sem, own_send, own_recv, kz_send, kz_recv, round_sem,
):
    segs = 4
    seg = 128
    hits = angles * segs
    xpad = hits + 8
    coil = lax.axis_index("coil")
    group = lax.axis_index("kz")
    core = group % 2
    x, y, z = coil // 8, (coil // 2) % 4, coil % 2

    beside = group + 1 - 2 * core
    far = (group + 2) % 4
    sibling = (coil, beside)

    def dev(axis_x, pairing, over_z=0, over_kz=0):
        zz = 1 - z if over_z else z
        there = far if over_kz else group
        if axis_x:
            return ((flip(x, pairing) * 4 + y) * 2 + zz, there)
        return ((x * 4 + flip(y, pairing)) * 2 + zz, there)

    def zdev(over_z, over_kz):
        return ((x * 4 + y) * 2 + (1 - z if over_z else z), far if over_kz else group)

    def side_of(s):
        first_x, pairing = STREAMS[s]
        i = x if first_x else y
        return ((i + 1) // 2) % 2 if pairing == 1 else i // 2

    def part_of(s, k, mine):
        return k * 8 + s * 2 + (side_of(s) if mine else 1 - side_of(s))

    loads = [
        pltpu.make_async_copy(plane_hbm, plane, load_sem.at[0]),
        pltpu.make_async_copy(sens_hbm, sens_v, load_sem.at[1]),
    ]

    def kload(q):
        rows = pl.ds(q * (parts // 4), parts // 4)
        return pltpu.make_async_copy(kdata_hbm.at[:, rows], kd.at[:, rows], load_sem.at[2 + q])

    def iload(q):
        rows = pl.ds(q * (angles // 4), angles // 4)
        return pltpu.make_async_copy(interp_hbm.at[rows], itp.at[rows], load_sem.at[6 + q])

    for copy in loads[::-1] + [kload(q) for q in range(4)] + [iload(q) for q in range(4)]:
        copy.start()

    barrier = pltpu.get_barrier_semaphore()
    turns = [(0, 0), (0, 1), (1, 0), (1, 1)]
    peers = [dev(*stream) for stream in STREAMS] + [zdev(1, 0), zdev(1, 1), sibling]
    for peer in peers:
        pl.semaphore_signal(barrier, inc=1, device_id=peer, device_id_type=MESH)

    loads[1].wait()
    row = lax.broadcasted_iota(jnp.int32, (side, side), 0)
    col = lax.broadcasted_iota(jnp.int32, (side, side), 1)
    perm = jnp.where(jnp.bitwise_xor(row, col) == coil * 8, 1.0, 0.0).astype(BF16)
    for r in range(2):
        sensp[r] = jnp.dot(perm, sens_v[r], preferred_element_type=F32)

    def sens_copy(s):
        return pltpu.make_async_remote_copy(
            src_ref=sensp.at[core], dst_ref=senso.at[s, core],
            send_sem=sens_send.at[0, s], recv_sem=sens_recv.at[0, s],
            device_id=dev(*STREAMS[s]), device_id_type=MESH,
        )

    def sens_pass(s, r):
        return pltpu.make_async_remote_copy(
            src_ref=senso.at[s, r], dst_ref=senso.at[s, r],
            send_sem=sens_send.at[1, s], recv_sem=sens_recv.at[1, s],
            device_id=sibling, device_id_type=MESH,
        )

    loads[0].wait()
    cos_p = jnp.dot(perm, plane[0:side, 0:side], preferred_element_type=F32).astype(BF16)
    sin_p = jnp.dot(perm, plane[side : 2 * side, 0:side], preferred_element_type=F32).astype(BF16)
    blocks = jnp.concatenate([block_ref[g : g + 1, :] for g in range(segs)], axis=1)
    blocks = jnp.broadcast_to(blocks, (side, hits))
    yrow = lax.broadcasted_iota(jnp.int32, (side, hits), 0)
    for h in range(2):
        onto = jnp.where(blocks == yrow * 2 + h, 1.0, 0.0).astype(BF16)
        cos_g = jnp.dot(cos_p, onto, preferred_element_type=F32)
        sin_g = jnp.dot(sin_p, onto, preferred_element_type=F32)
        tab[h, 0:side, 0:hits] = cos_g.astype(BF16)
        tab[h, side : 2 * side, hits : 2 * hits] = cos_g.astype(BF16)
        tab[h, 0:side, hits : 2 * hits] = sin_g.astype(BF16)
        tab[h, side : 2 * side, 0:hits] = (-sin_g).astype(BF16)

    arow = lax.broadcasted_iota(jnp.int32, (angles, spokes), 0)
    scol = lax.broadcasted_iota(jnp.int32, (angles, spokes), 1)
    match = jnp.broadcast_to(angle_ref[0:1, :], (angles, spokes)) == arow
    def bin_some(q, carry):
        kload(q).wait()
        for i in range(parts // 4):
            p = q * (parts // 4) + i
            used = jnp.logical_and(match, scol < count_ref[p])
            weights = jnp.where(used, 1.0, 0.0).astype(BF16)
            for r in range(2):
                summed = jnp.dot(weights, kd[r, p], preferred_element_type=F32)
                for g in range(segs):
                    start = g * angles * BPAD + r * parts + p
                    binned[pl.ds(start, angles, stride=BPAD), :] = summed[:, g * seg : (g + 1) * seg]
        return carry

    lax.fori_loop(0, BARRIER_AT, bin_some, 0)
    pl.semaphore_wait(barrier, len(peers))
    for s in range(4):
        sens_copy(s).start()
    for peer in peers:
        pl.semaphore_signal(round_sem.at[0], inc=1, device_id=peer, device_id_type=MESH)
    lax.fori_loop(BARRIER_AT, 4, bin_some, 0)

    def spread_some(q, carry):
        iload(q).wait()
        for k in range(angles // 4):
            a = q * (angles // 4) + k
            for g in range(segs):
                start = pl.multiple_of(g * angles * BPAD + a * BPAD, 8)
                piece = binned[pl.ds(start, 2 * parts), :].astype(BF16)
                got = jnp.dot(piece, itp[a, g], preferred_element_type=F32)
                spread[pl.ds(g * angles + a, 2 * parts, stride=xpad), :] = got
        return carry

    lax.fori_loop(0, 4, spread_some, 0)

    def seg_rows(p, r):
        return pl.ds(pl.multiple_of((r * parts + p) * xpad, 8), hits)

    def seg_copy(s, k, r):
        return pltpu.make_async_remote_copy(
            src_ref=spread.at[seg_rows(part_of(s, k, False), r)], dst_ref=other.at[s, k, r],
            send_sem=send_sem.at[0, s], recv_sem=seg_recv.at[s, k, r],
            device_id=dev(*STREAMS[s]), device_id_type=MESH,
        )

    for k in range(2):
        for s in range(4):
            for r in range(2):
                seg_copy(s, k, r).start()
    pl.semaphore_wait(round_sem.at[0], len(peers))
    for peer in peers:
        pl.semaphore_signal(round_sem.at[1], inc=1, device_id=peer, device_id_type=MESH)
    for s in range(4):
        sens_copy(s).wait_recv()
        sens_pass(s, core).start()
    for s in range(4):
        sens_pass(s, 1 - core).wait_recv()
    pl.semaphore_wait(round_sem.at[1], len(peers))

    def slots(pairing):
        return (1, 0, 1, 3) if pairing == 1 else (2, 1, 0, 1)

    def lay(s):
        first_x, pairing = STREAMS[s]
        return (first_x, 3, 2, 1, 0) if pairing == 1 else (first_x, 1, 1, 0, 1)

    def make(s, k):
        first_x, pairing = STREAMS[s]
        for r in range(2):
            seg_copy(s, k, r).wait_recv()
        p = part_of(s, k, True)
        rows = []
        for r in range(2):
            own = spread[seg_rows(p, r), :].astype(BF16)
            rows.append(jnp.concatenate([own, other[s, k, r].astype(BF16)], axis=1))
        stacked = jnp.concatenate(rows, axis=0)
        for h in range(2):
            got = jnp.dot(tab[h], stacked, preferred_element_type=F32).astype(BF16)
            for n in range(2):
                for r in range(2):
                    half[n, :, r * side + h * seg : r * side + (h + 1) * seg] = got[
                        r * side : (r + 1) * side, n * seg : (n + 1) * seg
                    ]
        mine = jnp.dot(half[0], plane[...], preferred_element_type=F32)
        theirs = jnp.dot(half[1], plane[...], preferred_element_type=F32)
        for jx in range(4):
            for jy in range(4):
                here = slice((jx * 4 + jy) * 16, (jx * 4 + jy + 1) * 16)
                there = (jx ^ pairing) * 4 + jy if first_x else jx * 4 + (jy ^ pairing)
                that = slice(there * 16, (there + 1) * 16)
                a_re, a_im = sensp[0, here, :], sensp[1, here, :]
                b_re, b_im = senso[s, 0, that, :], senso[s, 1, that, :]
                o_re, o_im = mine[here, 0:side], mine[here, side : 2 * side]
                t_re, t_im = theirs[here, 0:side], theirs[here, side : 2 * side]
                parts_of = (
                    (a_re * o_re + a_im * o_im) + (b_re * t_re + b_im * t_im),
                    (a_re * o_im - a_im * o_re) + (b_re * t_im - b_im * t_re),
                )
                for r in range(2):
                    for h in range(2):
                        img[s, k * 4 + r * 2 + h, jx, jy] = parts_of[r][:, h * seg : (h + 1) * seg]

    def copies(s, stage, c):
        first_x, second, sent2, slot0, slot_t = lay(s)
        pairing = STREAMS[s][1]
        sent, keep, onward, quarter = slots(pairing)
        if stage == 2:
            if first_x:
                return img.at[s, c, pl.ds(sent2, 2)], r2x.at[s, c], dev(True, second)
            return img.at[s, c, :, pl.ds(sent2, 2)], r2y.at[s - 2, c], dev(False, second)
        if stage == 3:
            if first_x:
                return r2x.at[s, c, :, pl.ds(sent, 2)], r3.at[s, c], dev(False, pairing)
            return r2y.at[s - 2, c, pl.ds(sent, 2)], r3.at[s, c], dev(True, pairing)
        src = r3.at[s, c, :, onward] if first_x else r3.at[s, c, onward]
        return src, r4.at[s, c], dev(not first_x, second)

    def remote(s, stage, c):
        src, dst, peer = copies(s, stage, c)
        return pltpu.make_async_remote_copy(
            src_ref=src, dst_ref=dst,
            send_sem=send_sem.at[stage - 1, s], recv_sem=recv_sem.at[stage - 2, s, c],
            device_id=peer, device_id_type=MESH,
        )

    def held(s, c, pair, quarter):
        first_x, second, sent2, slot0, slot_t = lay(s)
        j = STREAMS[s][1] if pair else 0
        slot = slot_t if pair else slot0
        if first_x:
            return img[s, c, j, quarter] + r2x[s, c, slot, quarter]
        return img[s, c, quarter, j] + r2y[s - 2, c, quarter, slot]

    def held3(s, c, pair, which, quarter):
        first_x, second, sent2, slot0, slot_t = lay(s)
        slot = slot_t if pair else slot0
        got = r3[s, c, slot, which] if first_x else r3[s, c, which, slot]
        return held(s, c, pair, quarter) + got

    def step(stage, c):
        for s in range(4):
            first_x, second, sent2, slot0, slot_t = lay(s)
            sent, keep, onward, quarter = slots(STREAMS[s][1])
            remote(s, stage - 1, c).wait_recv()
            for pair in range(2):
                slot = slot_t if pair else slot0
                if stage == 3:
                    for q in (sent, sent + 1):
                        value = held(s, c, pair, q)
                        if first_x:
                            r2x[s, c, slot, q] = value
                        else:
                            r2y[s - 2, c, q, slot] = value
                else:
                    value = held3(s, c, pair, onward, quarter)
                    if first_x:
                        r3[s, c, slot, onward] = value
                    else:
                        r3[s, c, onward, slot] = value
            remote(s, stage, c).start()

    def last_copies(kr, pair, s):
        got = []
        for jz, jk in turns:
            n = pair * 4 + jz * 2 + jk
            if n == 0:
                continue
            if pair:
                src, dst, peer = xbuf.at[1, kr, jz, s], rx.at[n, kr, s], dev(*STREAMS[s], jz, jk)
            else:
                src, dst, peer = xbuf.at[0, kr, jz], rx.at[n, kr], zdev(jz, jk)
            got.append(
                pltpu.make_async_remote_copy(
                    src_ref=src, dst_ref=dst, send_sem=own_send.at[n], recv_sem=own_recv.at[n, kr],
                    device_id=peer, device_id_type=MESH,
                )
            )
        return got

    def last(kr):
        for s in range(4):
            first_x, second, sent2, slot0, slot_t = lay(s)
            keep = slots(STREAMS[s][1])[1]
            for h in range(2):
                c = kr * 2 + h
                remote(s, 4, c).wait_recv()
                for pair in range(2):
                    slot = slot_t if pair else slot0
                    value = r4[s, c, slot] + held3(s, c, pair, keep, 0)
                    for jz in range(2):
                        xbuf[pair, kr, jz, s, h] = value[jz * 8 : (jz + 1) * 8]
            for copy in last_copies(kr, 1, s):
                copy.start()
        for copy in last_copies(kr, 0, 0):
            copy.start()

    def arrived(n, kr):
        whole = rx.at[n, kr]
        return pltpu.make_async_remote_copy(
            src_ref=whole, dst_ref=whole, send_sem=own_send.at[n], recv_sem=own_recv.at[n, kr],
            device_id=sibling, device_id_type=MESH,
        )

    def gath_rows(slot, kr):
        return pl.ds(pl.multiple_of((slot * 4 + kr) * 128, 128), 128)

    def kz_remote(n, kr):
        where = gath.at[gath_rows(far if n else group, kr)]
        return pltpu.make_async_remote_copy(
            src_ref=where, dst_ref=where,
            send_sem=kz_send.at[n], recv_sem=kz_recv.at[n, kr],
            device_id=sibling, device_id_type=MESH,
        )

    def finish(kr):
        for n in range(1, 8):
            arrived(n, kr).wait_recv()
        for s in range(4):
            for h in range(2):
                for slot, mine, value in (
                    (group, True, xbuf[0, kr, 0, s, h] + rx[2, kr, s, h]),
                    (group, False, rx[4, kr, s, h] + rx[6, kr, s, h]),
                    (far, True, rx[1, kr, s, h] + rx[3, kr, s, h]),
                    (far, False, rx[5, kr, s, h] + rx[7, kr, s, h]),
                ):
                    start = (slot * 4 + kr) * 128 + h * 64 + part_of(s, 0, mine)
                    gath[pl.ds(start, 8, stride=8), :] = value
        for n in range(2):
            kz_remote(n, kr).start()

    def put(kr, first, last_one):
        for n in range(2):
            kz_remote(n, kr).wait_recv()
        for h in range(2):
            rows = []
            for g in range(4):
                base = (g * 4 + kr) * 128 + h * 64
                rows.append(jnp.concatenate([gath[base + yy * 8 : base + yy * 8 + 8, :] for yy in range(8)], axis=1))
            stacked = jnp.concatenate(rows, axis=0)
            high = stacked.astype(BF16)
            low = (stacked - high.astype(F32)).astype(BF16)
            got = jnp.dot(
                ztab_ref[group, kr], jnp.concatenate([high, high, low], axis=0), preferred_element_type=F32
            )
            if not first:
                got = got + total[h]
            if not last_one:
                total[h] = got
                continue
            for yy in range(8):
                kzout[h, pl.ds(yy, 2 * parts, stride=8), :] = got[:, yy * seg : (yy + 1) * seg]
            out_ref[:, :, :, h * seg : (h + 1) * seg] = kzout[h, 0 : 2 * parts * 8].reshape(2, parts, 8, seg)

    begun = [what for what, *where in PLAN].index("O")
    for n, (what, *where) in enumerate(PLAN):
        if what == "M":
            make(where[1], where[0])
        elif what == "2":
            remote(where[1], 2, where[0]).start()
        elif what == "X":
            last(*where)
        elif what == "F":
            finish(*where)
        elif what == "O":
            put(*where, n == begun, n == len(PLAN) - 1)
        else:
            step(int(what), *where)

    def sent_all(ref, sem, unused, peer):
        pltpu.make_async_remote_copy(
            src_ref=ref, dst_ref=ref, send_sem=sem, recv_sem=unused, device_id=peer, device_id_type=MESH
        ).wait_send()

    everything = pl.ds(0, 8)
    for s in range(4):
        sens_copy(s).wait_send()
        sens_pass(s, core).wait_send()
        sent_all(other.at[s], send_sem.at[0, s], seg_recv.at[s, 0, 0], sibling)
        for stage in range(2, 5):
            src, dst, peer = copies(s, stage, everything)
            sent_all(src, send_sem.at[stage - 1, s], recv_sem.at[stage - 2, s, 0], peer)
    for n in range(1, 8):
        sent_all(rx.at[n], own_send.at[n], own_recv.at[n, 0], sibling)
    for n in range(2):
        sent_all(gath.at[pl.ds(0, 512)], kz_send.at[n], kz_recv.at[n, 0], sibling)


def per_device(kdata, spoke_angle, spoke_count, block_index, interp, sens_maps):
    side = sens_maps.shape[2]
    parts = kdata.shape[1]
    spokes, samples = kdata.shape[3], kdata.shape[4]
    angles, segs, seg = interp.shape[0], interp.shape[1], interp.shape[2]
    hits = angles * segs
    any_spec = pl.BlockSpec(memory_space=pl.ANY)
    vmem_spec = pl.BlockSpec(memory_space=pltpu.VMEM)
    return pl.pallas_call(
        functools.partial(kernel, parts, angles, spokes, side),
        out_shape=jax.ShapeDtypeStruct((2, parts, 8, side), F32),
        in_specs=[pl.BlockSpec(memory_space=pltpu.SMEM)] + [vmem_spec] * 3 + [any_spec] * 4,
        out_specs=vmem_spec,
        scratch_shapes=[
            pltpu.VMEM((2, parts, spokes, samples), BF16),
            pltpu.VMEM((angles, segs, seg, seg), BF16),
            pltpu.VMEM((2, side, side), BF16),
            pltpu.VMEM((2 * side, 2 * side), BF16),
            pltpu.VMEM((2, 2 * side, 2 * hits), BF16),
            pltpu.VMEM((2, side, side), F32),
            pltpu.VMEM((4, 2, side, side), F32),
            pltpu.VMEM(((segs * angles + 1) * BPAD, seg), F32),
            pltpu.VMEM(((2 * parts + 1) * (hits + 8), seg), F32),
            pltpu.VMEM((4, 2, 2, hits, seg), F32),
            pltpu.VMEM((2, side, 2 * side), BF16),
            pltpu.VMEM((4, 8, 4, 4, 16, seg), F32),
            pltpu.VMEM((2, 8, 2, 4, 16, seg), F32),
            pltpu.VMEM((2, 8, 4, 2, 16, seg), F32),
            pltpu.VMEM((4, 8, 2, 2, 16, seg), F32),
            pltpu.VMEM((4, 8, 2, 16, seg), F32),
            pltpu.VMEM((2, 4, 2, 4, 2, 8, seg), F32),
            pltpu.VMEM((8, 4, 4, 2, 8, seg), F32),
            pltpu.VMEM((4 * 4 * 128 + 8, seg), F32),
            pltpu.VMEM((2, 2 * parts, 8 * seg), F32),
            pltpu.VMEM((2, 2 * parts * 8 + 8, seg), F32),
            pltpu.SemaphoreType.DMA((10,)),
            pltpu.SemaphoreType.DMA((2, 4)),
            pltpu.SemaphoreType.DMA((2, 4)),
            pltpu.SemaphoreType.DMA((4, 4)),
            pltpu.SemaphoreType.DMA((4, 2, 2)),
            pltpu.SemaphoreType.DMA((3, 4, 8)),
            pltpu.SemaphoreType.DMA((8,)),
            pltpu.SemaphoreType.DMA((8, 4)),
            pltpu.SemaphoreType.DMA((2,)),
            pltpu.SemaphoreType.DMA((2, 4)),
            pltpu.SemaphoreType.REGULAR((2,)),
        ],
        compiler_params=pltpu.CompilerParams(
            collective_id=0, has_side_effects=True, vmem_limit_bytes=56 << 20
        ),
    )(
        spoke_count,
        spoke_angle.reshape(1, spokes),
        block_index.T,
        kz_table(4, parts),
        kdata[:, :, 0],
        interp,
        sens_maps[:, 0],
        plane_table(side),
    )

def solution(mesh):
    placed = (
        P(None, "kz", "coil", None, None),
        P(),
        P("kz"),
        P(),
        P(),
        P(None, "coil", None, None),
    )
    return jax.shard_map(
        per_device,
        mesh=mesh,
        in_specs=placed,
        out_specs=P(None, "kz", "coil", None),
        check_vma=False,
    )
```
